256 devices in a mesh: tm: 16 (over z, core), rows: 16 (over y, x).
Axes of the slice: x: 4, y: 4, z: 8, core: 2. Of those that a mesh axis runs over, the one named last changes fastest.
Arguments:
- frames_in: bfloat16 [32, 64, 120, 128], P('tm', 'rows'), may hold values from -25 to 25, as said below
- norm_gain: float32 [128], replicated, may hold values from 0.25 to 1.75
- norm_bias: float32 [128], replicated, may hold values from -0.5 to 0.5
- conv_weight: bfloat16 [3, 3, 3, 128, 128], replicated, may hold values from -0.109375 to 0.109375
- cotangent: bfloat16 [32, 64, 120, 128], P('tm', 'rows'), may hold values from -6 to 6
Outputs:
- output_frames: bfloat16 [32, 64, 120, 128], P('tm', 'rows')
- input_grad: bfloat16 [32, 64, 120, 128], P('tm', 'rows')
- weight_grad: float32 [128, 3456], P('rows')
- gain_grad: float32 [128], replicated
- bias_grad: float32 [128], replicated
The draws below stay inside these ranges and needn't reach their ends.
Inputs may be any that keep to these rules, and one draw needn't show every extreme that they name: Entries of frames_in lie within 25 in magnitude.
All inputs are finite; a program needn't handle non-finite values.
Results may differ from the reference program's by a relative error of at most 0.0042.
Values may be sent and summed in bfloat16 or wider, within the bound.
A program may use at most 64 MiB of HBM per device.

```python
import math
import jax
import jax.numpy as jnp
from jax import lax

C = 128
G = 32
W = 120
NT = 32
NH = 64


def draw_frames_in(key, part):
    keys_all = jax.random.split(key, 4)
    dims_all = (NT, NH, W, C)
    base_draw = jnp.clip(jax.random.normal(keys_all[0], dims_all, jnp.float32), -6.0, 6.0)
    time_pos = jnp.arange(NT, dtype=jnp.float32) / max(NT - 1, 1)
    height_pos = jnp.arange(NH, dtype=jnp.float32) / max(NH - 1, 1)
    frame_scale = 3.0 ** time_pos * jnp.exp(jax.random.uniform(keys_all[1], (NT,), jnp.float32, -0.35, 0.35))
    row_scale = 3.0 ** height_pos * jnp.exp(jax.random.uniform(keys_all[2], (NH,), jnp.float32, -0.35, 0.35))
    chan_scale = jnp.exp(jax.random.uniform(keys_all[3], (C,), jnp.float32, -0.7, 0.7))
    scaled = 0.1 * base_draw * frame_scale[:, None, None, None] * row_scale[None, :, None, None] * chan_scale
    return scaled.astype(jnp.bfloat16)


def level_of(own_key, extent, cuts, low, high):
    def one(position, blocks):
        heights = jax.random.uniform(jax.random.fold_in(jax.random.fold_in(own_key, 6), position), (blocks,), jnp.float32, low / len(cuts), high / len(cuts))
        return jnp.repeat(jnp.exp(heights), extent[position] // blocks).reshape((-1,) + (1,) * (len(extent) - position - 1))

    level = one(*cuts[0])
    for cut in cuts[1:]:
        level = level * one(*cut)
    return level


def bell_draw(rng, extent, deviation, bound, cuts=(), held_as=jnp.bfloat16):
    drawn = jax.random.normal(rng, extent, jnp.float32) * deviation
    if len(cuts) > 0:
        drawn = level_of(rng, extent, cuts, -0.22, 0.18) * drawn
    return jnp.clip(drawn, min=-bound, max=bound).astype(held_as)


def setup_inputs(seed: int = 0) -> dict:
    seeds = jax.random.split(jax.random.key(seed), 6)
    return {
        "frames_in": draw_frames_in(jax.random.fold_in(seeds[5], 71), 0),
        "norm_gain": jnp.clip(1.0 + 0.15 * jax.random.normal(seeds[1], (C,), jnp.float32), 0.25, 1.75),
        "norm_bias": jnp.clip(jax.random.uniform(seeds[2], (C,), jnp.float32, -0.5, 0.5), -0.5, 0.5),
        "conv_weight": bell_draw(seeds[3], (3, 3, 3, C, C), (27 * C) ** -0.5, 0.109375),
        "cotangent": bell_draw(seeds[4], (NT, NH, W, C), 1.0, 6.0, ((0, 16), (1, 16))),
    }


EPSILON = 1e-06

def group_expand(per_channel):
    return jnp.repeat(per_channel.reshape(G, C // G).sum(axis=1), C // G)

def reference(frames_in, norm_gain, norm_bias, conv_weight, cotangent):
    total_cells = NT * NH * W * (C // G)
    values = frames_in.astype(jnp.float32)
    channel_sum = lax.optimization_barrier(jnp.sum(values, axis=(0, 1, 2)))
    channel_sq = lax.optimization_barrier(jnp.sum(values * values, axis=(0, 1, 2)))
    group_mean = group_expand(channel_sum) / total_cells
    variance = group_expand(channel_sq) / total_cells - group_mean * group_mean
    inverse_std = lax.rsqrt(variance + EPSILON)
    normed = (values - group_mean) * inverse_std
    preact = normed * norm_gain + norm_bias
    activated = jax.nn.silu(preact).astype(jnp.bfloat16)
    padded = jnp.pad(activated, ((2, 0), (1, 1), (1, 1), (0, 0)))
    grad_padded = jnp.pad(cotangent, ((0, 2), (1, 1), (1, 1), (0, 0)))
    grad_flat = cotangent.reshape(-1, C)
    conv_sum = jnp.zeros((NT * NH * W, C), jnp.float32)
    grad_act = jnp.zeros((NT * NH * W, C), jnp.float32)
    pieces = []
    for time_off in range(3):
        for row_off in range(3):
            for col_off in range(3):
                window = padded[time_off:time_off + NT, row_off:row_off + NH, col_off:col_off + W].reshape(-1, C)
                conv_sum = conv_sum + jnp.dot(window, conv_weight[time_off, row_off, col_off], preferred_element_type=jnp.float32)
                pieces.append(lax.dot_general(grad_flat, window, (((0,), (0,)), ((), ())), preferred_element_type=jnp.float32))
                grad_window = grad_padded[time_off:time_off + NT, row_off:row_off + NH, col_off:col_off + W].reshape(-1, C)
                flipped = conv_weight[2 - time_off, 2 - row_off, 2 - col_off].T
                grad_act = grad_act + jnp.dot(grad_window, flipped, preferred_element_type=jnp.float32)
    output_frames = (values + conv_sum.reshape(values.shape)).astype(jnp.bfloat16)
    weight_grad = jnp.concatenate(pieces, axis=1) * (1.0 / math.sqrt(NT * NH * W))
    sigmoid_v = jax.nn.sigmoid(preact)
    grad_pre = grad_act.reshape(values.shape) * sigmoid_v * (1.0 + preact * (1.0 - sigmoid_v))
    gain_grad = lax.optimization_barrier(jnp.sum(grad_pre * normed, axis=(0, 1, 2)))
    bias_grad = lax.optimization_barrier(jnp.sum(grad_pre, axis=(0, 1, 2)))
    mean_dn = group_expand(norm_gain * bias_grad) / total_cells
    mean_dnn = group_expand(norm_gain * gain_grad) / total_cells
    input_grad = inverse_std * (grad_pre * norm_gain - mean_dn - normed * mean_dnn) + cotangent.astype(jnp.float32)
    return (output_frames, input_grad.astype(jnp.bfloat16), weight_grad, gain_grad, bias_grad)
```

```python
import functools
import math

import jax
import jax.numpy as jnp
from jax import lax
from jax.experimental import pallas as pl
from jax.experimental.pallas import tpu as pltpu
from jax.sharding import Mesh
from jax.sharding import PartitionSpec as P

G = 32
EPSILON = 1e-06
TM = ("z", "c")
ROWS = ("y", "x")
MESH = pl.DeviceIdType.MESH
WP = 128
HALF = 14
CHUNKS = 2
PER = HALF // CHUNKS
F32 = jnp.float32
BF16 = jnp.bfloat16


def group_total(per_channel, size):
    lanes = lax.broadcasted_iota(jnp.int32, per_channel.shape, 1)
    within = lanes % size
    channels = per_channel.shape[1]
    total = per_channel
    for step in range(1, size):
        ahead = pltpu.roll(per_channel, channels - step, 1)
        behind = pltpu.roll(per_channel, step, 1)
        total = total + jnp.where(within + step < size, ahead, 0.0)
        total = total + jnp.where(within >= step, behind, 0.0)
    return total


def kernel(
    sizes, x_hbm, gain_ref, bias_ref, w_hbm, cot_hbm,
    of_hbm, ig_hbm, wg_hbm, gain_hbm, bias_hbm,
    xr, cr, wv, a0, a3, c3, ct, ga, wgf, dsend, drecv, bsend, brecv, crecv, fin,
    ofv, igv, wgv, gv, bv, st1, st2, gs1, gs2,
    load_sem, out_sem, xs, xq, cs, cq, s1s, s1r, s2s, s2r, g1s, g1r, g2s, g2r,
    ds, dr, bs, br, zs, zr, fs, fr,
):
    nz, nc, ny, nx = sizes
    n_tm, n_rows = nz * nc, ny * nx
    frames, band, width, chans = x_hbm.shape
    pixels = frames * band * WP
    own_o = chans // n_rows
    all_pixels = frames * n_tm * band * n_rows * width
    cells = all_pixels * (chans // G)
    z, c = lax.axis_index("z"), lax.axis_index("c")
    y, x = lax.axis_index("y"), lax.axis_index("x")
    tm, row = z * nc + c, y * nx + x

    def at(t, r):
        t, r = lax.rem(t + n_tm, n_tm), lax.rem(r + n_rows, n_rows)
        return {"z": t // nc, "c": lax.rem(t, nc), "y": r // nx, "x": lax.rem(r, nx)}

    def xy_peers():
        for k in range(1, n_rows):
            dy, dx = k // nx, k % nx
            ty, tx = lax.rem(y + dy, ny), lax.rem(x + dx, nx)
            yield k, ty * nx + tx, {"z": z, "c": c, "y": ty, "x": tx}

    def zc_peers():
        for k in range(1, n_tm):
            dz, dc = k // nc, k % nc
            tz, tc = lax.rem(z + dz, nz), lax.rem(c + dc, nc)
            yield k, tz * nc + tc, {"z": tz, "c": tc, "y": y, "x": x}

    def remote(src, dst, send_sem, recv_sem, device):
        return pltpu.make_async_remote_copy(
            src_ref=src, dst_ref=dst, send_sem=send_sem, recv_sem=recv_sem,
            device_id=device, device_id_type=MESH,
        )

    load_x = pltpu.make_async_copy(x_hbm, xr.at[frames : 2 * frames, 1 : band + 1], load_sem.at[0])
    load_c = pltpu.make_async_copy(cot_hbm, cr.at[0:frames, 1 : band + 1], load_sem.at[1])
    load_w = pltpu.make_async_copy(w_hbm, wv, load_sem.at[2])
    load_x.start()
    load_c.start()
    load_w.start()

    barrier = pltpu.get_barrier_semaphore()
    partners = 0
    for _, _, device in (*zc_peers(), *xy_peers()):
        pl.semaphore_signal(barrier, inc=1, device_id=device, device_id_type=MESH)
        partners += 1
    for dt in (-1, 1):
        for dr_ in (-1, 1):
            pl.semaphore_signal(
                barrier, inc=1, device_id=at(tm + dt, row + dr_), device_id_type=MESH
            )
            partners += 1

    load_x.wait()

    def stat_row(k, carry):
        total, square = carry
        v = xr[frames + k // band, 1 + lax.rem(k, band)].astype(F32)
        return (
            total + v.reshape(width // 8, 8, chans).sum(axis=0),
            square + (v * v).reshape(width // 8, 8, chans).sum(axis=0),
        )

    zero8 = jnp.zeros((8, chans), F32)
    total, square = lax.fori_loop(0, frames * band, stat_row, (zero8, zero8))
    st1[row, 0:1] = total.sum(axis=0, keepdims=True)
    st1[row, 1:2] = square.sum(axis=0, keepdims=True)

    pl.semaphore_wait(barrier, partners)

    def spread_xy(slots, send_sem, recv_sem):
        return [
            remote(slots.at[row], slots.at[row], send_sem.at[k], recv_sem.at[row], device)
            for k, _, device in xy_peers()
        ]

    def spread_zc(slots, send_sem, recv_sem):
        return [
            remote(slots.at[tm], slots.at[tm], send_sem.at[k], recv_sem.at[tm], device)
            for k, _, device in zc_peers()
        ]

    def arrived_xy(slots, send_sem, recv_sem):
        for k, peer, device in xy_peers():
            remote(slots.at[peer], slots.at[peer], send_sem.at[k], recv_sem.at[peer], device).wait_recv()

    def arrived_zc(slots, send_sem, recv_sem):
        for k, peer, device in zc_peers():
            remote(slots.at[peer], slots.at[peer], send_sem.at[k], recv_sem.at[peer], device).wait_recv()

    def summed(slots):
        total = slots[0]
        for k in range(1, slots.shape[0]):
            total = total + slots[k]
        return total

    sent = spread_xy(st1, s1s, s1r)
    for copy in sent:
        copy.start()

    def margins(buf, first, there, way, send_sem, recv_sem):
        mine = buf.at[first : first + frames, 1 : band + 1]
        low = buf.at[first : first + frames, 1]
        high = buf.at[first : first + frames, band]
        same = buf.at[first : first + frames]
        moved = buf.at[there : there + frames]
        up_t = (tm + way >= 0) & (tm + way < n_tm)
        from_t = (tm - way >= 0) & (tm - way < n_tm)
        up_r, down_r = row < n_rows - 1, row > 0
        plan = [
            (high, same.at[:, 0], at(tm, row + 1), up_r, down_r),
            (low, same.at[:, band + 1], at(tm, row - 1), down_r, up_r),
            (mine, moved.at[:, 1 : band + 1], at(tm + way, row), up_t, from_t),
            (high, moved.at[:, 0], at(tm + way, row + 1), up_t & up_r, from_t & down_r),
            (low, moved.at[:, band + 1], at(tm + way, row - 1), up_t & down_r, from_t & up_r),
        ]
        return [
            (remote(src, dst, send_sem.at[k], recv_sem.at[k], device), sends, gets)
            for k, (src, dst, device, sends, gets) in enumerate(plan)
        ]

    load_c.wait()
    cot_margins = margins(cr, 0, frames, -1, cs, cq)
    x_margins = margins(xr, frames, 0, 1, xs, xq)
    for copy, sends, _ in (*cot_margins, *x_margins):

        @pl.when(sends)
        def _():
            copy.start()

    zeros_pad = jnp.zeros((WP - width, chans), F32)

    def padded_row(v):
        return jnp.concatenate([v, zeros_pad], axis=0)

    def cot_row(t, h, keep):
        v = padded_row(cr[t, h].astype(F32))
        v = jnp.where(keep, v, 0.0)
        sides = (pltpu.roll(v, 1, 0), v, pltpu.roll(v, WP - 1, 0))
        for shift in range(3):
            c3[shift, t, h] = sides[shift].astype(BF16)
        return sides

    for k in range(frames * band):
        sides = cot_row(k // band, 1 + k % band, True)
        for shift in range(3):
            ct[shift * chans : (shift + 1) * chans, k * WP : (k + 1) * WP] = (
                sides[2 - shift].T.astype(BF16)
            )
    load_w.wait()

    arrived_xy(st1, s1s, s1r)
    st2[tm] = summed(st1)
    sent2 = spread_zc(st2, s2s, s2r)
    for copy in sent2:
        copy.start()

    for copy, _, gets in cot_margins:

        @pl.when(gets)
        def _():
            copy.wait_recv()

    row_low, row_high = row > 0, row < n_rows - 1

    def cot_margin_row(t, h):
        keep = True
        if t >= frames:
            keep = tm < n_tm - 1
        if h == 0:
            keep = keep & row_low
        if h == band + 1:
            keep = keep & row_high
        cot_row(t, h, keep)

    for t in range(2 * frames):
        for h in range(band + 2):
            if not (t < frames and 1 <= h <= band):
                cot_margin_row(t, h)

    def window(ref, a, b):
        return ref[pl.ds(a, frames), b : b + band].reshape(pixels, chans)

    taps = [(b, s) for b in range(3) for s in range(3)]
    for a in range(3):
        lhs = jnp.concatenate([window(c3.at[s], a, b) for b, s in taps], axis=1)
        rhs = jnp.concatenate([wv[9 * (2 - a) + 3 * (2 - b) + 2 - s] for b, s in taps], axis=1)
        part = lax.dot_general(lhs, rhs, (((1,), (1,)), ((), ())), preferred_element_type=F32)
        if a == 0:
            ga[...] = part
        else:
            ga[...] += part

    arrived_zc(st2, s2s, s2r)
    stats = summed(st2)
    wide = lambda v: jnp.broadcast_to(v, (8, chans))
    mean = group_total(wide(stats[0:1]), chans // G) / cells
    variance = group_total(wide(stats[1:2]), chans // G) / cells - mean * mean
    inverse = lax.rsqrt(variance + EPSILON)
    gain, shift_ = wide(gain_ref[...]), wide(bias_ref[...])
    mean, inverse, gain, shift_ = (v[0:1] for v in (mean, inverse, gain, shift_))

    for copy, _, gets in x_margins:

        @pl.when(gets)
        def _():
            copy.wait_recv()

    def act_row(k, carry):
        t, h = k // (band + 2), lax.rem(k, band + 2)
        v = xr[t, h].astype(F32)
        pre = (v - mean) * inverse * gain + shift_
        keep = (
            ((t >= frames) | (tm > 0))
            & ((h >= 1) | row_low)
            & ((h <= band) | row_high)
        )
        act = jnp.where(keep, pre / (1.0 + jnp.exp(-pre)), 0.0)
        a0[t, h] = padded_row(act).astype(BF16)
        return carry

    lax.fori_loop(0, 2 * frames * (band + 2), act_row, 0)

    first = c == 0
    other = {"z": z, "c": 1 - c, "y": y, "x": x}
    part0 = jnp.where(first, 5, 0)
    part1 = jnp.where(first, 0, 9)
    halves = (
        remote(dsend.at[pl.ds(part0, 9)], drecv.at[pl.ds(part0, 9)], ds.at[0], dr.at[0], other),
        remote(dsend.at[pl.ds(part1, 5)], drecv.at[pl.ds(part1, 5)], ds.at[1], dr.at[1], other),
    )
    got0, got1 = jnp.where(first, 0, 5), jnp.where(first, 9, 0)
    halves_in = (
        remote(dsend.at[pl.ds(got0, 9)], drecv.at[pl.ds(got0, 9)], ds.at[0], dr.at[0], other),
        remote(dsend.at[pl.ds(got1, 5)], drecv.at[pl.ds(got1, 5)], ds.at[1], dr.at[1], other),
    )
    for k in range(3):
        a = jnp.where(first, 2 - k, k)
        rhs = jnp.concatenate([window(a0, a, b) for b in range(3)], axis=1)
        part = jnp.dot(ct[...], rhs, preferred_element_type=F32)
        for b in range(3):
            for s in range(3):
                block = part[s * chans : (s + 1) * chans, b * chans : (b + 1) * chans]
                if k == 0:
                    dsend[part0 + 3 * b + s] = block.astype(BF16)
                else:
                    wgf[9 * a + 3 * b + s] = block
        if k == 0:
            halves[0].start()
        if k == 1:
            at1 = jnp.where(first, 13, 9)
            for j in range(5):
                dsend[part1 + j] = wgf[at1 + j].astype(BF16)
            halves[1].start()

    for copy in halves_in:
        copy.wait_recv()
    base = jnp.where(first, 0, 13)
    to_rows = []
    for ch in range(CHUNKS):
        for j in range(PER):
            value = wgf[base + ch * PER + j] + drecv[ch * PER + j].astype(F32)
            bsend[ch, :, j] = value.reshape(n_rows, own_o, chans).astype(BF16)
        brecv[ch, row] = bsend[ch, row]
        for k, peer, device in xy_peers():
            copy = remote(
                bsend.at[ch, peer], brecv.at[ch, row], bs.at[ch, k], br.at[ch, row], device
            )
            copy.start()
            to_rows.append(copy)

    def pre_row(k):
        v = xr[frames + k // band, 1 + lax.rem(k, band)].astype(F32)
        normed = (v - mean) * inverse
        return normed

    def grad_row(k, carry):
        gains, biases = carry
        normed = pre_row(k)
        pre = normed * gain + shift_
        sig = 1.0 / (1.0 + jnp.exp(-pre))
        at_k = pl.multiple_of(k * WP, WP)
        grad = ga[pl.ds(at_k, width)] * sig * (1.0 + pre * (1.0 - sig))
        ga[pl.ds(at_k, width)] = grad
        return (
            gains + (grad * normed).reshape(width // 8, 8, chans).sum(axis=0),
            biases + grad.reshape(width // 8, 8, chans).sum(axis=0),
        )

    gains, biases = lax.fori_loop(0, frames * band, grad_row, (zero8, zero8))
    gs1[row, 0:1] = gains.sum(axis=0, keepdims=True)
    gs1[row, 1:2] = biases.sum(axis=0, keepdims=True)
    sent3 = spread_xy(gs1, g1s, g1r)
    for copy in sent3:
        copy.start()

    def shift_row(k, carry):
        t, h = k // (band + 2), lax.rem(k, band + 2)
        v = a0[t, h].astype(F32)
        a3[0, t, h] = pltpu.roll(v, 1, 0).astype(BF16)
        a3[1, t, h] = pltpu.roll(v, WP - 1, 0).astype(BF16)
        return carry

    lax.fori_loop(0, 2 * frames * (band + 2), shift_row, 0)
    sides = (a3.at[0], a0, a3.at[1])
    conv = None
    for a in range(3):
        lhs = jnp.concatenate([window(sides[s], a, b) for b, s in taps], axis=1)
        rhs = jnp.concatenate([wv[9 * a + 3 * b + s] for b, s in taps], axis=0)
        part = jnp.dot(lhs, rhs, preferred_element_type=F32)
        conv = part if a == 0 else conv + part
    conv = conv.reshape(frames, band, WP, chans)
    for t in range(frames):
        for h in range(band):
            v = xr[frames + t, 1 + h].astype(F32)
            ofv[t, h] = (v + conv[t, h, :width]).astype(BF16)
    put_of = pltpu.make_async_copy(ofv, of_hbm, out_sem.at[0])
    put_of.start()

    arrived_xy(gs1, g1s, g1r)
    gs2[tm] = summed(gs1)
    sent4 = spread_zc(gs2, g2s, g2r)
    for copy in sent4:
        copy.start()

    to_z = []
    for ch in range(CHUNKS):
        for k, peer, device in xy_peers():
            remote(
                bsend.at[ch, peer], brecv.at[ch, peer], bs.at[ch, k], br.at[ch, peer], device
            ).wait_recv()
        value = brecv[ch, 0].astype(F32)
        for k in range(1, n_rows):
            value = value + brecv[ch, k].astype(F32)
        crecv[ch, z] = value.astype(BF16)
        for k in range(1, nz):
            device = {"z": lax.rem(z + k, nz), "c": c, "y": y, "x": x}
            copy = remote(crecv.at[ch, z], crecv.at[ch, z], zs.at[ch, k], zr.at[ch, z], device)
            copy.start()
            to_z.append(copy)

    arrived_zc(gs2, g2s, g2r)
    sums = summed(gs2)
    gain_grad, bias_grad = wide(sums[0:1]), wide(sums[1:2])
    gv[...] = sums[0:1]
    bv[...] = sums[1:2]
    put_g = pltpu.make_async_copy(gv, gain_hbm, out_sem.at[3])
    put_b = pltpu.make_async_copy(bv, bias_hbm, out_sem.at[4])
    put_g.start()
    put_b.start()
    mean_dn = (group_total(gain * bias_grad, chans // G) / cells)[0:1]
    mean_dnn = (group_total(gain * gain_grad, chans // G) / cells)[0:1]

    def input_row(k, carry):
        t, h = k // band, lax.rem(k, band)
        normed = pre_row(k)
        grad = ga[pl.ds(pl.multiple_of(k * WP, WP), width)]
        cot = cr[t, 1 + h].astype(F32)
        igv[t, h] = (inverse * (grad * gain - mean_dn - normed * mean_dnn) + cot).astype(BF16)
        return carry

    lax.fori_loop(0, frames * band, input_row, 0)
    put_ig = pltpu.make_async_copy(igv, ig_hbm, out_sem.at[1])
    put_ig.start()

    to_core = []
    for ch in range(CHUNKS):
        for k in range(1, nz):
            peer = lax.rem(z + k, nz)
            device = {"z": peer, "c": c, "y": y, "x": x}
            remote(
                crecv.at[ch, peer], crecv.at[ch, peer], zs.at[ch, k], zr.at[ch, peer], device
            ).wait_recv()
        value = crecv[ch, 0].astype(F32)
        for k in range(1, nz):
            value = value + crecv[ch, k].astype(F32)
        fin[c, ch] = value
        copy = remote(fin.at[c, ch], fin.at[c, ch], fs.at[ch], fr.at[ch], other)
        copy.start()
        to_core.append(copy)
    for ch in range(CHUNKS):
        remote(fin.at[1 - c, ch], fin.at[1 - c, ch], fs.at[ch], fr.at[ch], other).wait_recv()
    scale = 1.0 / math.sqrt(all_pixels)
    for j in range(27):
        if j < HALF:
            value = fin[0, j // PER, j % PER]
        else:
            value = fin[1, (j - 13) // PER, (j - 13) % PER]
        wgv[:, j * chans : (j + 1) * chans] = value * scale
    put_wg = pltpu.make_async_copy(wgv, wg_hbm, out_sem.at[2])
    put_wg.start()

    for copy in (*sent, *sent2, *sent3, *sent4, *halves, *to_rows, *to_z, *to_core):
        copy.wait_send()
    for copy, sends, _ in (*cot_margins, *x_margins):

        @pl.when(sends)
        def _():
            copy.wait_send()

    for copy in (put_of, put_ig, put_g, put_b, put_wg):
        copy.wait()


def per_device(sizes, frames_in, norm_gain, norm_bias, conv_weight, cotangent):
    nz, nc, ny, nx = sizes
    n_tm, n_rows = nz * nc, ny * nx
    frames, band, width, chans = frames_in.shape
    own_o = chans // n_rows
    rows = (2 * frames, band + 2)
    vmem, dma = pltpu.VMEM, pltpu.SemaphoreType.DMA
    scratch = [
        vmem((*rows, width, chans), BF16),
        vmem((*rows, width, chans), BF16),
        vmem((27, chans, chans), BF16),
        vmem((*rows, WP, chans), BF16),
        vmem((2, *rows, WP, chans), BF16),
        vmem((3, *rows, WP, chans), BF16),
        vmem((3 * chans, frames * band * WP), BF16),
        vmem((frames * band * WP, chans), F32),
        vmem((27, chans, chans), F32),
        vmem((HALF, chans, chans), BF16),
        vmem((HALF, chans, chans), BF16),
        vmem((CHUNKS, n_rows, PER, own_o, chans), BF16),
        vmem((CHUNKS, n_rows, PER, own_o, chans), BF16),
        vmem((CHUNKS, nz, PER, own_o, chans), BF16),
        vmem((2, CHUNKS, PER, own_o, chans), F32),
        vmem((frames, band, width, chans), BF16),
        vmem((frames, band, width, chans), BF16),
        vmem((own_o, 27 * chans), F32),
        vmem((1, chans), F32),
        vmem((1, chans), F32),
        vmem((n_rows, 2, chans), F32),
        vmem((n_tm, 2, chans), F32),
        vmem((n_rows, 2, chans), F32),
        vmem((n_tm, 2, chans), F32),
        dma((3,)), dma((5,)),
        dma((5,)), dma((5,)), dma((5,)), dma((5,)),
        dma((n_rows,)), dma((n_rows,)), dma((n_tm,)), dma((n_tm,)),
        dma((n_rows,)), dma((n_rows,)), dma((n_tm,)), dma((n_tm,)),
        dma((2,)), dma((2,)),
        dma((CHUNKS, n_rows)), dma((CHUNKS, n_rows)),
        dma((CHUNKS, nz)), dma((CHUNKS, nz)),
        dma((CHUNKS,)), dma((CHUNKS,)),
    ]
    anywhere = pl.BlockSpec(memory_space=pl.ANY)
    inside = pl.BlockSpec(memory_space=pltpu.VMEM)
    out = jax.ShapeDtypeStruct
    of, ig, wg, gg, bg = pl.pallas_call(
        functools.partial(kernel, sizes),
        out_shape=(
            out(frames_in.shape, BF16),
            out(frames_in.shape, BF16),
            out((own_o, 27 * chans), F32),
            out((1, chans), F32),
            out((1, chans), F32),
        ),
        in_specs=[anywhere, inside, inside, anywhere, anywhere],
        out_specs=(anywhere,) * 5,
        scratch_shapes=scratch,
        compiler_params=pltpu.CompilerParams(
            collective_id=0, has_side_effects=True, vmem_limit_bytes=48 << 20
        ),
        name="block",
    )(
        frames_in,
        norm_gain.reshape(1, chans),
        norm_bias.reshape(1, chans),
        conv_weight.reshape(27, chans, chans),
        cotangent,
    )
    return of, ig, wg, gg.reshape(chans), bg.reshape(chans)


def program(devices):
    torus = Mesh(devices, ("z", "c", "y", "x"))
    placed = (P(TM, ROWS, None, None), P(), P(), P(), P(TM, ROWS, None, None))
    return jax.shard_map(
        functools.partial(per_device, devices.shape),
        mesh=torus,
        in_specs=placed,
        out_specs=(P(TM, ROWS, None, None), P(TM, ROWS, None, None), P(ROWS, None), P(), P()),
        check_vma=False,
    )


def solution(mesh):
    return program(mesh.devices.reshape(8, 2, 4, 4))
```

```python
import functools
import math

import jax
import jax.numpy as jnp
from jax import lax
from jax.experimental import pallas as pl
from jax.experimental.pallas import tpu as pltpu
from jax.sharding import Mesh
from jax.sharding import PartitionSpec as P

G = 32
EPSILON = 1e-06
TM = ("z", "c")
ROWS = ("y", "x")
MESH = pl.DeviceIdType.MESH
WP = 128
CHUNKS = 3
PER = 5
F32 = jnp.float32
BF16 = jnp.bfloat16


def group_total(per_channel, size):
    lanes = lax.broadcasted_iota(jnp.int32, per_channel.shape, 1)
    within = lanes % size
    channels = per_channel.shape[1]
    total = per_channel
    for step in range(1, size):
        ahead = pltpu.roll(per_channel, channels - step, 1)
        behind = pltpu.roll(per_channel, step, 1)
        total = total + jnp.where(within + step < size, ahead, 0.0)
        total = total + jnp.where(within >= step, behind, 0.0)
    return total


def kernel(
    sizes, x_hbm, gn_hbm, sh_hbm, w_hbm, cot_hbm,
    of_hbm, ig_hbm, wg_hbm, gain_hbm, bias_hbm,
    gain_ref, bias_ref, xr, cr, wv, a0, a3, c3, ct, ga, wgf, dsend, drecv, bsend, brecv, crecv, fin,
    ofv, igv, wgv, gv, bv, st1, st2, gs1, gs2,
    load_sem, out_sem, xs, xq, cs, cq, s1s, s1r, s2s, s2r, g1s, g1r, g2s, g2r,
    ds, dr, bs, br, zs, zr, fs, fr,
):
    nz, nc, ny, nx = sizes
    n_tm, n_rows = nz * nc, ny * nx
    frames, band, width, chans = x_hbm.shape
    pixels = frames * band * WP
    own_o = chans // n_rows
    all_pixels = frames * n_tm * band * n_rows * width
    cells = all_pixels * (chans // G)
    z, c = lax.axis_index("z"), lax.axis_index("c")
    y, x = lax.axis_index("y"), lax.axis_index("x")
    tm, row = z * nc + c, y * nx + x

    def at(t, r):
        t, r = lax.rem(t + n_tm, n_tm), lax.rem(r + n_rows, n_rows)
        return {"z": t // nc, "c": lax.rem(t, nc), "y": r // nx, "x": lax.rem(r, nx)}

    def xy_peers():
        for k in range(1, n_rows):
            dy, dx = k // nx, k % nx
            ty, tx = lax.rem(y + dy, ny), lax.rem(x + dx, nx)
            yield k, ty * nx + tx, {"z": z, "c": c, "y": ty, "x": tx}

    def zc_peers():
        for k in range(1, n_tm):
            dz, dc = k // nc, k % nc
            tz, tc = lax.rem(z + dz, nz), lax.rem(c + dc, nc)
            yield k, tz * nc + tc, {"z": tz, "c": tc, "y": y, "x": x}

    def remote(src, dst, send_sem, recv_sem, device):
        return pltpu.make_async_remote_copy(
            src_ref=src, dst_ref=dst, send_sem=send_sem, recv_sem=recv_sem,
            device_id=device, device_id_type=MESH,
        )

    load_x = pltpu.make_async_copy(x_hbm, xr.at[frames : 2 * frames, 1 : band + 1], load_sem.at[0])
    load_c = pltpu.make_async_copy(cot_hbm, cr.at[0:frames, 1 : band + 1], load_sem.at[1])
    load_w = pltpu.make_async_copy(w_hbm, wv, load_sem.at[2])
    load_gn = pltpu.make_async_copy(gn_hbm, gain_ref, load_sem.at[3])
    load_sh = pltpu.make_async_copy(sh_hbm, bias_ref, load_sem.at[4])
    for copy in (load_x, load_c, load_w, load_gn, load_sh):
        copy.start()

    barrier = pltpu.get_barrier_semaphore()
    partners = 0
    for _, _, device in (*zc_peers(), *xy_peers()):
        pl.semaphore_signal(barrier, inc=1, device_id=device, device_id_type=MESH)
        partners += 1
    for dt in (-1, 1):
        for dr_ in (-1, 1):
            pl.semaphore_signal(
                barrier, inc=1, device_id=at(tm + dt, row + dr_), device_id_type=MESH
            )
            partners += 1

    load_x.wait()

    def stat_row(k, carry):
        total, square = carry
        v = xr[frames + k // band, 1 + lax.rem(k, band)].astype(F32)
        return (
            total + v.reshape(width // 8, 8, chans).sum(axis=0),
            square + (v * v).reshape(width // 8, 8, chans).sum(axis=0),
        )

    zero8 = jnp.zeros((8, chans), F32)
    total, square = lax.fori_loop(0, frames * band, stat_row, (zero8, zero8))
    st1[row, 0:1] = total.sum(axis=0, keepdims=True)
    st1[row, 1:2] = square.sum(axis=0, keepdims=True)

    pl.semaphore_wait(barrier, partners)

    def spread_xy(slots, send_sem, recv_sem):
        return [
            remote(slots.at[row], slots.at[row], send_sem.at[k], recv_sem.at[row], device)
            for k, _, device in xy_peers()
        ]

    def spread_zc(slots, send_sem, recv_sem):
        return [
            remote(slots.at[tm], slots.at[tm], send_sem.at[k], recv_sem.at[tm], device)
            for k, _, device in zc_peers()
        ]

    def arrived_xy(slots, send_sem, recv_sem):
        for k, peer, device in xy_peers():
            remote(slots.at[peer], slots.at[peer], send_sem.at[k], recv_sem.at[peer], device).wait_recv()

    def arrived_zc(slots, send_sem, recv_sem):
        for k, peer, device in zc_peers():
            remote(slots.at[peer], slots.at[peer], send_sem.at[k], recv_sem.at[peer], device).wait_recv()

    def summed(slots):
        total = slots[0]
        for k in range(1, slots.shape[0]):
            total = total + slots[k]
        return total

    sent = spread_xy(st1, s1s, s1r)
    for copy in sent:
        copy.start()

    def margins(buf, first, there, way, send_sem, recv_sem):
        mine = buf.at[first : first + frames, 1 : band + 1]
        low = buf.at[first : first + frames, 1]
        high = buf.at[first : first + frames, band]
        same = buf.at[first : first + frames]
        moved = buf.at[there : there + frames]
        up_t = (tm + way >= 0) & (tm + way < n_tm)
        from_t = (tm - way >= 0) & (tm - way < n_tm)
        up_r, down_r = row < n_rows - 1, row > 0
        plan = [
            (high, same.at[:, 0], at(tm, row + 1), up_r, down_r),
            (low, same.at[:, band + 1], at(tm, row - 1), down_r, up_r),
            (mine, moved.at[:, 1 : band + 1], at(tm + way, row), up_t, from_t),
            (high, moved.at[:, 0], at(tm + way, row + 1), up_t & up_r, from_t & down_r),
            (low, moved.at[:, band + 1], at(tm + way, row - 1), up_t & down_r, from_t & up_r),
        ]
        return [
            (remote(src, dst, send_sem.at[k], recv_sem.at[k], device), sends, gets)
            for k, (src, dst, device, sends, gets) in enumerate(plan)
        ]

    load_c.wait()
    cot_margins = margins(cr, 0, frames, -1, cs, cq)
    x_margins = margins(xr, frames, 0, 1, xs, xq)
    for copy, sends, _ in (*cot_margins, *x_margins):

        @pl.when(sends)
        def _():
            copy.start()

    zeros_pad = jnp.zeros((WP - width, chans), F32)

    def padded_row(v):
        return jnp.concatenate([v, zeros_pad], axis=0)

    def cot_row(t, h, keep):
        v = padded_row(cr[t, h].astype(F32))
        v = jnp.where(keep, v, 0.0)
        sides = (pltpu.roll(v, 1, 0), v, pltpu.roll(v, WP - 1, 0))
        for shift in range(3):
            c3[shift, t, h] = sides[shift].astype(BF16)
        return sides

    for k in range(frames * band):
        sides = cot_row(k // band, 1 + k % band, True)
        for shift in range(3):
            ct[shift * chans : (shift + 1) * chans, k * WP : (k + 1) * WP] = (
                sides[2 - shift].T.astype(BF16)
            )
    load_w.wait()
    load_gn.wait()
    load_sh.wait()

    arrived_xy(st1, s1s, s1r)
    st2[tm] = summed(st1)
    sent2 = spread_zc(st2, s2s, s2r)
    for copy in sent2:
        copy.start()

    row_low, row_high = row > 0, row < n_rows - 1
    for copy, _, gets in cot_margins[:2]:

        @pl.when(gets)
        def _():
            copy.wait_recv()

    for t in range(frames):
        cot_row(t, 0, row_low)
        cot_row(t, band + 1, row_high)

    taps = [(b, s) for b in range(3) for s in range(3)]

    def frame(refs, t):
        rows = [refs[s][t, b : b + band].reshape(band * WP, chans) for b, s in taps]
        return jnp.concatenate(rows, axis=1)

    def back_taps(a):
        return jnp.concatenate([wv[9 * (2 - a) + 3 * (2 - b) + 2 - s] for b, s in taps], axis=1)

    def back(lhs, rhs):
        return lax.dot_general(lhs, rhs, (((1,), (1,)), ((), ())), preferred_element_type=F32)

    half = band * WP
    c3s = [c3.at[s] for s in range(3)]
    both = back(frame(c3s, 1), jnp.concatenate([back_taps(1), back_taps(0)], axis=0))
    ga[0:half] = back(frame(c3s, 0), back_taps(0)) + both[:, :chans]
    ga[half:] = both[:, chans:]

    for copy, _, gets in cot_margins[2:]:

        @pl.when(gets)
        def _():
            copy.wait_recv()

    has_next = tm < n_tm - 1
    for t in range(frames, 2 * frames):
        for h in range(band + 2):
            keep = has_next
            if h == 0:
                keep = keep & row_low
            if h == band + 1:
                keep = keep & row_high
            cot_row(t, h, keep)
    both = back(frame(c3s, 2), jnp.concatenate([back_taps(2), back_taps(1)], axis=0))
    ga[0:half] += both[:, :chans]
    ga[half:] += back(frame(c3s, 3), back_taps(2)) + both[:, chans:]

    arrived_zc(st2, s2s, s2r)
    stats = summed(st2)
    wide = lambda v: jnp.broadcast_to(v, (8, chans))
    mean = group_total(wide(stats[0:1]), chans // G) / cells
    variance = group_total(wide(stats[1:2]), chans // G) / cells - mean * mean
    inverse = lax.rsqrt(variance + EPSILON)
    gain, shift_ = wide(gain_ref[...]), wide(bias_ref[...])
    mean, inverse, gain, shift_ = (v[0:1] for v in (mean, inverse, gain, shift_))

    for copy, _, gets in x_margins:

        @pl.when(gets)
        def _():
            copy.wait_recv()

    def sigmoid(v):
        return 0.5 + 0.5 * jnp.tanh(0.5 * v)

    def act_row(k, carry):
        t, h = k // (band + 2), lax.rem(k, band + 2)
        v = xr[t, h].astype(F32)
        pre = (v - mean) * inverse * gain + shift_
        keep = (
            ((t >= frames) | (tm > 0))
            & ((h >= 1) | row_low)
            & ((h <= band) | row_high)
        )
        a0[t, h] = padded_row(jnp.where(keep, pre * sigmoid(pre), 0.0)).astype(BF16)
        return carry

    def act_frames(low, high):
        lax.fori_loop(low * (band + 2), high * (band + 2), act_row, 0)

    other = {"z": z, "c": 1 - c, "y": y, "x": x}
    given, kept = 4 * (1 - c), 4 * c
    halves = [
        remote(dsend.at[a], drecv.at[a], ds.at[a], dr.at[a], other) for a in range(CHUNKS)
    ]

    def weight_blocks(a):
        rhs = jnp.concatenate(
            [a0[a : a + frames, b : b + band].reshape(pixels, chans) for b in range(3)], axis=1
        )
        part = jnp.dot(ct[...], rhs, preferred_element_type=F32)
        for b, s in taps:
            wgf[a, 3 * b + s] = part[s * chans : (s + 1) * chans, b * chans : (b + 1) * chans]
        for j in range(PER):
            dsend[a, j] = wgf[a, given + j].astype(BF16)
        halves[a].start()

    to_rows = []

    def send_rows(a):
        halves[a].wait_recv()
        for j in range(PER):
            value = wgf[a, kept + j] + drecv[a, j].astype(F32)
            bsend[a, :, j] = value.reshape(n_rows, own_o, chans).astype(BF16)
        brecv[a, row] = bsend[a, row]
        for k, peer, device in xy_peers():
            copy = remote(
                bsend.at[a, peer], brecv.at[a, row], bs.at[a, k], br.at[a, row], device
            )
            copy.start()
            to_rows.append(copy)

    act_frames(0, 2)
    weight_blocks(0)
    act_frames(2, 3)
    weight_blocks(1)

    def pre_row(k):
        v = xr[frames + k // band, 1 + lax.rem(k, band)].astype(F32)
        return (v - mean) * inverse

    def grad_row(k, carry):
        gains, biases = carry
        normed = pre_row(k)
        pre = normed * gain + shift_
        sig = sigmoid(pre)
        at_k = pl.multiple_of(k * WP, WP)
        grad = ga[pl.ds(at_k, width)] * sig * (1.0 + pre * (1.0 - sig))
        ga[pl.ds(at_k, width)] = grad
        return (
            gains + (grad * normed).reshape(width // 8, 8, chans).sum(axis=0),
            biases + grad.reshape(width // 8, 8, chans).sum(axis=0),
        )

    gains, biases = lax.fori_loop(0, frames * band, grad_row, (zero8, zero8))
    gs1[row, 0:1] = gains.sum(axis=0, keepdims=True)
    gs1[row, 1:2] = biases.sum(axis=0, keepdims=True)
    sent3 = spread_xy(gs1, g1s, g1r)
    for copy in sent3:
        copy.start()

    send_rows(0)
    act_frames(3, 4)
    weight_blocks(2)
    send_rows(1)
    send_rows(2)

    def shift_row(k, carry):
        t, h = k // (band + 2), lax.rem(k, band + 2)
        v = a0[t, h].astype(F32)
        a3[0, t, h] = pltpu.roll(v, 1, 0).astype(BF16)
        a3[1, t, h] = pltpu.roll(v, WP - 1, 0).astype(BF16)
        return carry

    lax.fori_loop(0, 2 * frames * (band + 2), shift_row, 0)
    sides = (a3.at[0], a0, a3.at[1])

    def front_taps(a):
        return jnp.concatenate([wv[9 * a + 3 * b + s] for b, s in taps], axis=0)

    def front(lhs, rhs):
        return jnp.dot(lhs, rhs, preferred_element_type=F32)

    def put_frame(t, conv):
        for h in range(band):
            v = xr[frames + t, 1 + h].astype(F32)
            ofv[t, h] = (v + conv[h * WP : h * WP + width]).astype(BF16)

    one = front(frame(sides, 1), jnp.concatenate([front_taps(1), front_taps(0)], axis=1))
    two = front(frame(sides, 2), jnp.concatenate([front_taps(2), front_taps(1)], axis=1))
    put_frame(0, front(frame(sides, 0), front_taps(0)) + one[:, :chans] + two[:, :chans])
    put_frame(1, front(frame(sides, 3), front_taps(2)) + one[:, chans:] + two[:, chans:])
    put_of = pltpu.make_async_copy(ofv, of_hbm, out_sem.at[0])
    put_of.start()

    arrived_xy(gs1, g1s, g1r)
    gs2[tm] = summed(gs1)
    sent4 = spread_zc(gs2, g2s, g2r)
    for copy in sent4:
        copy.start()

    to_z = []
    for ch in range(CHUNKS):
        for k, peer, device in xy_peers():
            remote(
                bsend.at[ch, peer], brecv.at[ch, peer], bs.at[ch, k], br.at[ch, peer], device
            ).wait_recv()
        value = brecv[ch, 0].astype(F32)
        for k in range(1, n_rows):
            value = value + brecv[ch, k].astype(F32)
        crecv[ch, z] = value.astype(BF16)
        for k in range(1, nz):
            device = {"z": lax.rem(z + k, nz), "c": c, "y": y, "x": x}
            copy = remote(crecv.at[ch, z], crecv.at[ch, z], zs.at[ch, k], zr.at[ch, z], device)
            copy.start()
            to_z.append(copy)

    arrived_zc(gs2, g2s, g2r)
    sums = summed(gs2)
    gain_grad, bias_grad = wide(sums[0:1]), wide(sums[1:2])
    gv[...] = sums[0:1]
    bv[...] = sums[1:2]
    put_g = pltpu.make_async_copy(gv, gain_hbm, out_sem.at[3])
    put_b = pltpu.make_async_copy(bv, bias_hbm, out_sem.at[4])
    put_g.start()
    put_b.start()
    mean_dn = (group_total(gain * bias_grad, chans // G) / cells)[0:1]
    mean_dnn = (group_total(gain * gain_grad, chans // G) / cells)[0:1]

    def input_row(k, carry):
        t, h = k // band, lax.rem(k, band)
        normed = pre_row(k)
        grad = ga[pl.ds(pl.multiple_of(k * WP, WP), width)]
        cot = cr[t, 1 + h].astype(F32)
        igv[t, h] = (inverse * (grad * gain - mean_dn - normed * mean_dnn) + cot).astype(BF16)
        return carry

    lax.fori_loop(0, frames * band, input_row, 0)
    put_ig = pltpu.make_async_copy(igv, ig_hbm, out_sem.at[1])
    put_ig.start()

    to_core = []
    for ch in range(CHUNKS):
        for k in range(1, nz):
            peer = lax.rem(z + k, nz)
            device = {"z": peer, "c": c, "y": y, "x": x}
            remote(
                crecv.at[ch, peer], crecv.at[ch, peer], zs.at[ch, k], zr.at[ch, peer], device
            ).wait_recv()
        value = crecv[ch, 0].astype(F32)
        for k in range(1, nz):
            value = value + crecv[ch, k].astype(F32)
        fin[c, ch] = value
        copy = remote(fin.at[c, ch], fin.at[c, ch], fs.at[ch], fr.at[ch], other)
        copy.start()
        to_core.append(copy)
    for ch in range(CHUNKS):
        remote(fin.at[1 - c, ch], fin.at[1 - c, ch], fs.at[ch], fr.at[ch], other).wait_recv()
    scale = 1.0 / math.sqrt(all_pixels)
    for j in range(27):
        a, m = j // 9, j % 9
        value = fin[0, a, m] if m < PER else fin[1, a, m - 4]
        wgv[:, j * chans : (j + 1) * chans] = value * scale
    put_wg = pltpu.make_async_copy(wgv, wg_hbm, out_sem.at[2])
    put_wg.start()

    for copy in (*sent, *sent2, *sent3, *sent4, *halves, *to_rows, *to_z, *to_core):
        copy.wait_send()
    for copy, sends, _ in (*cot_margins, *x_margins):

        @pl.when(sends)
        def _():
            copy.wait_send()

    for copy in (put_of, put_ig, put_g, put_b, put_wg):
        copy.wait()


def put_out(*refs):
    sources, places, sem = refs[:5], refs[5:10], refs[10]
    copies = [pltpu.make_async_copy(s, d, sem.at[k]) for k, (s, d) in enumerate(zip(sources, places))]
    for copy in copies:
        copy.start()
    for copy in copies:
        copy.wait()


def per_device(sizes, frames_in, norm_gain, norm_bias, conv_weight, cotangent):
    nz, nc, ny, nx = sizes
    n_tm, n_rows = nz * nc, ny * nx
    frames, band, width, chans = frames_in.shape
    own_o = chans // n_rows
    rows = (2 * frames, band + 2)
    vmem, dma = pltpu.VMEM, pltpu.SemaphoreType.DMA
    scratch = [
        vmem((1, chans), F32),
        vmem((1, chans), F32),
        vmem((*rows, width, chans), BF16),
        vmem((*rows, width, chans), BF16),
        vmem((27, chans, chans), BF16),
        vmem((*rows, WP, chans), BF16),
        vmem((2, *rows, WP, chans), BF16),
        vmem((3, *rows, WP, chans), BF16),
        vmem((3 * chans, frames * band * WP), BF16),
        vmem((frames * band * WP, chans), F32),
        vmem((3, 9, chans, chans), F32),
        vmem((CHUNKS, PER, chans, chans), BF16),
        vmem((CHUNKS, PER, chans, chans), BF16),
        vmem((CHUNKS, n_rows, PER, own_o, chans), BF16),
        vmem((CHUNKS, n_rows, PER, own_o, chans), BF16),
        vmem((CHUNKS, nz, PER, own_o, chans), BF16),
        vmem((2, CHUNKS, PER, own_o, chans), F32),
        vmem((frames, band, width, chans), BF16),
        vmem((frames, band, width, chans), BF16),
        vmem((own_o, 27 * chans), F32),
        vmem((1, chans), F32),
        vmem((1, chans), F32),
        vmem((n_rows, 2, chans), F32),
        vmem((n_tm, 2, chans), F32),
        vmem((n_rows, 2, chans), F32),
        vmem((n_tm, 2, chans), F32),
        dma((5,)), dma((5,)),
        dma((5,)), dma((5,)), dma((5,)), dma((5,)),
        dma((n_rows,)), dma((n_rows,)), dma((n_tm,)), dma((n_tm,)),
        dma((n_rows,)), dma((n_rows,)), dma((n_tm,)), dma((n_tm,)),
        dma((CHUNKS,)), dma((CHUNKS,)),
        dma((CHUNKS, n_rows)), dma((CHUNKS, n_rows)),
        dma((CHUNKS, nz)), dma((CHUNKS, nz)),
        dma((CHUNKS,)), dma((CHUNKS,)),
    ]
    anywhere = pl.BlockSpec(memory_space=pl.ANY)
    stays = pl.BlockSpec(memory_space=pltpu.HBM)
    out = jax.ShapeDtypeStruct
    made = pl.pallas_call(
        functools.partial(kernel, sizes),
        out_shape=(
            out(frames_in.shape, BF16),
            out(frames_in.shape, BF16),
            out((own_o, 27 * chans), F32),
            out((1, chans), F32),
            out((1, chans), F32),
        ),
        in_specs=[stays] * 5,
        out_specs=(anywhere,) * 5,
        scratch_shapes=scratch,
        compiler_params=pltpu.CompilerParams(
            collective_id=0, has_side_effects=True, vmem_limit_bytes=48 << 20
        ),
        name="block",
    )(
        *(
            pltpu.with_memory_space_constraint(a, pltpu.HBM)
            for a in (
                frames_in,
                norm_gain.reshape(1, chans),
                norm_bias.reshape(1, chans),
                conv_weight.reshape(27, chans, chans),
                cotangent,
            )
        )
    )
    of, ig, wg, gg, bg = pl.pallas_call(
        put_out,
        out_shape=[out(a.shape, a.dtype) for a in made],
        in_specs=[anywhere] * 5,
        out_specs=[stays] * 5,
        scratch_shapes=[dma((5,))],
        compiler_params=pltpu.CompilerParams(vmem_limit_bytes=1 << 20),
        name="put_out",
    )(*made)
    return of, ig, wg, gg.reshape(chans), bg.reshape(chans)


def program(devices):
    torus = Mesh(devices, ("z", "c", "y", "x"))
    placed = (P(TM, ROWS, None, None), P(), P(), P(), P(TM, ROWS, None, None))
    return jax.shard_map(
        functools.partial(per_device, devices.shape),
        mesh=torus,
        in_specs=placed,
        out_specs=(P(TM, ROWS, None, None), P(TM, ROWS, None, None), P(ROWS, None), P(), P()),
        check_vma=False,
    )


def solution(mesh):
    return program(mesh.devices.reshape(8, 2, 4, 4))
```

```python
import functools
import math

import jax
import jax.numpy as jnp
from jax import lax
from jax.experimental import pallas as pl
from jax.experimental.pallas import tpu as pltpu
from jax.sharding import Mesh
from jax.sharding import PartitionSpec as P

G = 32
EPSILON = 1e-06
TM = ("z", "c")
ROWS = ("y", "x")
MESH = pl.DeviceIdType.MESH
WP = 128
CHUNKS = 3
PER = 5
PIECES = ((0, 0, 5), (1, 0, 5), (2, 0, 3), (2, 3, 2))
F32 = jnp.float32
BF16 = jnp.bfloat16


def group_total(per_channel, size):
    lanes = lax.broadcasted_iota(jnp.int32, per_channel.shape, 1)
    within = lanes % size
    channels = per_channel.shape[1]
    total = per_channel
    for step in range(1, size):
        ahead = pltpu.roll(per_channel, channels - step, 1)
        behind = pltpu.roll(per_channel, step, 1)
        total = total + jnp.where(within + step < size, ahead, 0.0)
        total = total + jnp.where(within >= step, behind, 0.0)
    return total


def kernel(
    sizes, x_hbm, gn_hbm, sh_hbm, w_hbm, cot_hbm,
    ofv, igv, wgv, gv, bv,
    gain_ref, bias_ref, xr, cr, wv, a0, a3, c3, ct, ga, wgf, dsend, drecv, bsend, brecv, crecv, fin,
    st1, st2, gs1, gs2,
    load_sem, xs, xq, cs, cq, s1s, s1r, s2s, s2r, g1s, g1r, g2s, g2r,
    ds, dr, bs, br, zs, zr, fs, fr,
):
    nz, nc, ny, nx = sizes
    n_tm, n_rows = nz * nc, ny * nx
    frames, band, width, chans = x_hbm.shape
    pixels = frames * band * WP
    own_o = chans // n_rows
    all_pixels = frames * n_tm * band * n_rows * width
    cells = all_pixels * (chans // G)
    z, c = lax.axis_index("z"), lax.axis_index("c")
    y, x = lax.axis_index("y"), lax.axis_index("x")
    tm, row = z * nc + c, y * nx + x

    def at(t, r):
        t, r = lax.rem(t + n_tm, n_tm), lax.rem(r + n_rows, n_rows)
        return {"z": t // nc, "c": lax.rem(t, nc), "y": r // nx, "x": lax.rem(r, nx)}

    other = {"z": z, "c": 1 - c, "y": y, "x": x}

    def xy_peers():
        for k in range(1, n_rows):
            dy, dx = k // nx, k % nx
            ty, tx = lax.rem(y + dy, ny), lax.rem(x + dx, nx)
            yield k, ty * nx + tx, {"z": z, "c": c, "y": ty, "x": tx}

    def zc_peers():
        for k in range(1, n_tm):
            dz, dc = k // nc, k % nc
            tz, tc = lax.rem(z + dz, nz), lax.rem(c + dc, nc)
            yield k, tz * nc + tc, {"z": tz, "c": tc, "y": y, "x": x}

    def remote(src, dst, send_sem, recv_sem, device):
        return pltpu.make_async_remote_copy(
            src_ref=src, dst_ref=dst, send_sem=send_sem, recv_sem=recv_sem,
            device_id=device, device_id_type=MESH,
        )

    load_x = pltpu.make_async_copy(x_hbm, xr.at[frames : 2 * frames, 1 : band + 1], load_sem.at[0])
    load_c = pltpu.make_async_copy(cot_hbm, cr.at[0:frames, 1 : band + 1], load_sem.at[1])
    load_w = pltpu.make_async_copy(w_hbm, wv, load_sem.at[2])
    load_gn = pltpu.make_async_copy(gn_hbm, gain_ref, load_sem.at[3])
    load_sh = pltpu.make_async_copy(sh_hbm, bias_ref, load_sem.at[4])
    for copy in (load_x, load_c, load_w, load_gn, load_sh):
        copy.start()

    barrier = pltpu.get_barrier_semaphore()
    partners = 0
    for _, _, device in (*zc_peers(), *xy_peers()):
        pl.semaphore_signal(barrier, inc=1, device_id=device, device_id_type=MESH)
        partners += 1
    for dt in (-1, 1):
        for dr_ in (-1, 1):
            pl.semaphore_signal(
                barrier, inc=1, device_id=at(tm + dt, row + dr_), device_id_type=MESH
            )
            partners += 1

    load_x.wait()

    def stat_row(k, carry):
        total, square = carry
        v = xr[frames + k // band, 1 + lax.rem(k, band)].astype(F32)
        return (
            total + v.reshape(width // 8, 8, chans).sum(axis=0),
            square + (v * v).reshape(width // 8, 8, chans).sum(axis=0),
        )

    zero8 = jnp.zeros((8, chans), F32)
    total, square = lax.fori_loop(0, frames * band, stat_row, (zero8, zero8))
    st1[row, 0:1] = total.sum(axis=0, keepdims=True)
    st1[row, 1:2] = square.sum(axis=0, keepdims=True)

    pl.semaphore_wait(barrier, partners)

    def spread_xy(slots, send_sem, recv_sem):
        return [
            remote(slots.at[row], slots.at[row], send_sem, recv_sem, device)
            for _, _, device in xy_peers()
        ]

    def spread_zc(slots, send_sem, recv_sem):
        return [
            remote(slots.at[tm], slots.at[tm], send_sem, recv_sem, device)
            for _, _, device in zc_peers()
        ]

    def all_but_one(slots, send_sem, recv_sem):
        rest = slots.at[0 : slots.shape[0] - 1]
        return remote(rest, rest, send_sem, recv_sem, other)

    def summed(slots):
        total = slots[0]
        for k in range(1, slots.shape[0]):
            total = total + slots[k]
        return total

    for copy in spread_xy(st1, s1s.at[0], s1r.at[0]):
        copy.start()

    def margins(buf, first, there, way, send_sem, recv_sem):
        mine = buf.at[first : first + frames, 1 : band + 1]
        low = buf.at[first : first + frames, 1]
        high = buf.at[first : first + frames, band]
        same = buf.at[first : first + frames]
        moved = buf.at[there : there + frames]
        up_t = (tm + way >= 0) & (tm + way < n_tm)
        from_t = (tm - way >= 0) & (tm - way < n_tm)
        up_r, down_r = row < n_rows - 1, row > 0
        plan = [
            (high, same.at[:, 0], at(tm, row + 1), up_r, down_r),
            (low, same.at[:, band + 1], at(tm, row - 1), down_r, up_r),
            (mine, moved.at[:, 1 : band + 1], at(tm + way, row), up_t, from_t),
            (high, moved.at[:, 0], at(tm + way, row + 1), up_t & up_r, from_t & down_r),
            (low, moved.at[:, band + 1], at(tm + way, row - 1), up_t & down_r, from_t & up_r),
        ]
        return [
            (remote(src, dst, send_sem.at[k], recv_sem.at[k], device), sends, gets)
            for k, (src, dst, device, sends, gets) in enumerate(plan)
        ]

    load_c.wait()
    cot_margins = margins(cr, 0, frames, -1, cs, cq)
    x_margins = margins(xr, frames, 0, 1, xs, xq)
    for copy, sends, _ in (*cot_margins, *x_margins):

        @pl.when(sends)
        def _():
            copy.start()

    zeros_pad = jnp.zeros((WP - width, chans), F32)

    def padded_row(v):
        return jnp.concatenate([v, zeros_pad], axis=0)

    def cot_row(t, h, keep):
        v = padded_row(cr[t, h].astype(F32))
        v = jnp.where(keep, v, 0.0)
        sides = (pltpu.roll(v, 1, 0), v, pltpu.roll(v, WP - 1, 0))
        for shift in range(3):
            c3[shift, t, h] = sides[shift].astype(BF16)
        return sides

    for k in range(frames * band):
        sides = cot_row(k // band, 1 + k % band, True)
        for shift in range(3):
            ct[shift * chans : (shift + 1) * chans, k * WP : (k + 1) * WP] = (
                sides[2 - shift].T.astype(BF16)
            )
    load_w.wait()
    load_gn.wait()
    load_sh.wait()

    all_but_one(st1, s1s.at[0], s1r.at[0]).wait_recv()
    st2[tm] = summed(st1)
    for copy in spread_zc(st2, s2s.at[0], s2r.at[0]):
        copy.start()

    row_low, row_high = row > 0, row < n_rows - 1
    for copy, _, gets in cot_margins[:2]:

        @pl.when(gets)
        def _():
            copy.wait_recv()

    for t in range(frames):
        cot_row(t, 0, row_low)
        cot_row(t, band + 1, row_high)

    taps = [(b, s) for b in range(3) for s in range(3)]

    def frame(refs, t):
        rows = [refs[s][t, b : b + band].reshape(band * WP, chans) for b, s in taps]
        return jnp.concatenate(rows, axis=1)

    def back_taps(a):
        return jnp.concatenate([wv[9 * (2 - a) + 3 * (2 - b) + 2 - s] for b, s in taps], axis=1)

    def back(lhs, rhs):
        return lax.dot_general(lhs, rhs, (((1,), (1,)), ((), ())), preferred_element_type=F32)

    half = band * WP
    c3s = [c3.at[s] for s in range(3)]
    both = back(frame(c3s, 1), jnp.concatenate([back_taps(1), back_taps(0)], axis=0))
    ga[0:half] = back(frame(c3s, 0), back_taps(0)) + both[:, :chans]
    ga[half:] = both[:, chans:]

    for copy, _, gets in cot_margins[2:]:

        @pl.when(gets)
        def _():
            copy.wait_recv()

    has_next = tm < n_tm - 1
    for t in range(frames, 2 * frames):
        for h in range(band + 2):
            keep = has_next
            if h == 0:
                keep = keep & row_low
            if h == band + 1:
                keep = keep & row_high
            cot_row(t, h, keep)
    both = back(frame(c3s, 2), jnp.concatenate([back_taps(2), back_taps(1)], axis=0))
    ga[0:half] += both[:, :chans]
    ga[half:] += back(frame(c3s, 3), back_taps(2)) + both[:, chans:]

    all_but_one(st2, s2s.at[0], s2r.at[0]).wait_recv()
    stats = summed(st2)
    wide = lambda v: jnp.broadcast_to(v, (8, chans))
    mean = group_total(wide(stats[0:1]), chans // G) / cells
    variance = group_total(wide(stats[1:2]), chans // G) / cells - mean * mean
    inverse = lax.rsqrt(variance + EPSILON)
    gain, shift_ = wide(gain_ref[...]), wide(bias_ref[...])
    mean, inverse, gain, shift_ = (v[0:1] for v in (mean, inverse, gain, shift_))

    for copy, _, gets in x_margins:

        @pl.when(gets)
        def _():
            copy.wait_recv()

    def sigmoid(v):
        return 0.5 + 0.5 * jnp.tanh(0.5 * v)

    def act_row(k, carry):
        t, h = k // (band + 2), lax.rem(k, band + 2)
        v = xr[t, h].astype(F32)
        pre = (v - mean) * inverse * gain + shift_
        keep = (
            ((t >= frames) | (tm > 0))
            & ((h >= 1) | row_low)
            & ((h <= band) | row_high)
        )
        a0[t, h] = padded_row(jnp.where(keep, pre * sigmoid(pre), 0.0)).astype(BF16)
        return carry

    def act_frames(low, high):
        lax.fori_loop(low * (band + 2), high * (band + 2), act_row, 0, unroll=True)

    given, kept = 4 * (1 - c), 4 * c
    halves = [
        remote(dsend.at[a], drecv.at[a], ds.at[a], dr.at[a], other) for a in range(CHUNKS)
    ]

    def weight_blocks(a):
        rhs = jnp.concatenate(
            [a0[a : a + frames, b : b + band].reshape(pixels, chans) for b in range(3)], axis=1
        )
        part = jnp.dot(ct[...], rhs, preferred_element_type=F32)
        for b, s in taps:
            wgf[a, 3 * b + s] = part[s * chans : (s + 1) * chans, b * chans : (b + 1) * chans]
        for j in range(PER):
            dsend[a, j] = wgf[a, given + j].astype(BF16)
        halves[a].start()

    def send_rows(p):
        a, low, count = PIECES[p]
        for j in range(low, low + count):
            value = wgf[a, kept + j] + drecv[a, j].astype(F32)
            bsend[a, :, j] = value.reshape(n_rows, own_o, chans).astype(BF16)
        blocks = slice(low, low + count)
        brecv[a, row, blocks] = bsend[a, row, blocks]
        for k, peer, device in xy_peers():
            there = brecv.at[a, row, blocks]
            remote(bsend.at[a, peer, blocks], there, bs.at[p], br.at[p], device).start()

    act_frames(0, 2)
    weight_blocks(0)
    act_frames(2, 3)
    def pre_row(k):
        v = xr[frames + k // band, 1 + lax.rem(k, band)].astype(F32)
        return (v - mean) * inverse

    def grad_row(k, carry):
        gains, biases = carry
        normed = pre_row(k)
        pre = normed * gain + shift_
        sig = sigmoid(pre)
        at_k = pl.multiple_of(k * WP, WP)
        grad = ga[pl.ds(at_k, width)] * sig * (1.0 + pre * (1.0 - sig))
        ga[pl.ds(at_k, width)] = grad
        return (
            gains + (grad * normed).reshape(width // 8, 8, chans).sum(axis=0),
            biases + grad.reshape(width // 8, 8, chans).sum(axis=0),
        )

    gains, biases = lax.fori_loop(0, frames * band, grad_row, (zero8, zero8), unroll=True)
    gs1[row, 0:1] = gains.sum(axis=0, keepdims=True)
    gs1[row, 1:2] = biases.sum(axis=0, keepdims=True)
    for copy in spread_xy(gs1, g1s.at[0], g1r.at[0]):
        copy.start()

    weight_blocks(1)

    halves[0].wait_recv()
    send_rows(0)
    act_frames(3, 4)
    weight_blocks(2)
    halves[1].wait_recv()
    send_rows(1)
    halves[2].wait_recv()
    send_rows(2)
    send_rows(3)

    def shift_row(k, carry):
        t, h = k // (band + 2), lax.rem(k, band + 2)
        v = a0[t, h].astype(F32)
        a3[0, t, h] = pltpu.roll(v, 1, 0).astype(BF16)
        a3[1, t, h] = pltpu.roll(v, WP - 1, 0).astype(BF16)
        return carry

    lax.fori_loop(0, 2 * frames * (band + 2), shift_row, 0)
    sides = (a3.at[0], a0, a3.at[1])

    def front_taps(a):
        return jnp.concatenate([wv[9 * a + 3 * b + s] for b, s in taps], axis=0)

    def front(lhs, rhs):
        return jnp.dot(lhs, rhs, preferred_element_type=F32)

    def put_frame(t, conv):
        for h in range(band):
            v = xr[frames + t, 1 + h].astype(F32)
            ofv[t, h] = (v + conv[h * WP : h * WP + width]).astype(BF16)

    one = front(frame(sides, 1), jnp.concatenate([front_taps(1), front_taps(0)], axis=1))
    two = front(frame(sides, 2), jnp.concatenate([front_taps(2), front_taps(1)], axis=1))
    put_frame(0, front(frame(sides, 0), front_taps(0)) + one[:, :chans] + two[:, :chans])
    put_frame(1, front(frame(sides, 3), front_taps(2)) + one[:, chans:] + two[:, chans:])

    def piece(buf, p, send_sem, recv_sem):
        a, low, count = PIECES[p]
        return all_but_one(buf.at[a, :, low : low + count], send_sem.at[p], recv_sem.at[p])

    def send_z(p):
        piece(brecv, p, bs, br).wait_recv()
        a, low, count = PIECES[p]
        blocks = slice(low, low + count)
        value = brecv[a, 0, blocks].astype(F32)
        for k in range(1, n_rows):
            value = value + brecv[a, k, blocks].astype(F32)
        crecv[a, z, blocks] = value.astype(BF16)
        mine = crecv.at[a, z, blocks]
        for k in range(1, nz):
            device = {"z": lax.rem(z + k, nz), "c": c, "y": y, "x": x}
            remote(mine, mine, zs.at[p], zr.at[p], device).start()

    all_but_one(gs1, g1s.at[0], g1r.at[0]).wait_recv()
    gs2[tm] = summed(gs1)
    for copy in spread_zc(gs2, g2s.at[0], g2r.at[0]):
        copy.start()

    for p in range(len(PIECES)):
        send_z(p)

    all_but_one(gs2, g2s.at[0], g2r.at[0]).wait_recv()
    sums = summed(gs2)
    gain_grad, bias_grad = wide(sums[0:1]), wide(sums[1:2])
    gv[...] = sums[0:1]
    bv[...] = sums[1:2]
    mean_dn = (group_total(gain * bias_grad, chans // G) / cells)[0:1]
    mean_dnn = (group_total(gain * gain_grad, chans // G) / cells)[0:1]

    def input_row(k, carry):
        t, h = k // band, lax.rem(k, band)
        normed = pre_row(k)
        grad = ga[pl.ds(pl.multiple_of(k * WP, WP), width)]
        cot = cr[t, 1 + h].astype(F32)
        igv[t, h] = (inverse * (grad * gain - mean_dn - normed * mean_dnn) + cot).astype(BF16)
        return carry

    lax.fori_loop(0, frames * band, input_row, 0)

    to_core = []
    for p, (a, low, count) in enumerate(PIECES):
        piece(crecv, p, zs, zr).wait_recv()
        blocks = slice(low, low + count)
        value = crecv[a, 0, blocks].astype(F32)
        for k in range(1, nz):
            value = value + crecv[a, k, blocks].astype(F32)
        fin[c, a, blocks] = value
        mine = fin.at[c, a, blocks]
        copy = remote(mine, mine, fs.at[p], fr.at[p], other)
        copy.start()
        to_core.append(copy)
    scale = 1.0 / math.sqrt(all_pixels)
    for p, (a, low, count) in enumerate(PIECES):
        theirs = fin.at[1 - c, a, low : low + count]
        remote(theirs, theirs, fs.at[p], fr.at[p], other).wait_recv()
        for core in range(2):
            for j in range(low, low + count):
                if core == 0 or j > 0:
                    at_m = (9 * a + 4 * core + j) * chans
                    wgv[:, at_m : at_m + chans] = fin[core, a, j] * scale

    for copy in (
        all_but_one(st1, s1s.at[0], s1r.at[0]),
        all_but_one(st2, s2s.at[0], s2r.at[0]),
        all_but_one(gs1, g1s.at[0], g1r.at[0]),
        all_but_one(gs2, g2s.at[0], g2r.at[0]),
        *halves,
        *(piece(bsend, p, bs, br) for p in range(len(PIECES))),
        *(piece(crecv, p, zs, zr) for p in range(len(PIECES))),
        *to_core,
    ):
        copy.wait_send()
    for copy, sends, _ in (*cot_margins, *x_margins):

        @pl.when(sends)
        def _():
            copy.wait_send()


def put_out(*refs):
    sources, places, sem = refs[:5], refs[5:10], refs[10]
    copies = [pltpu.make_async_copy(s, d, sem.at[k]) for k, (s, d) in enumerate(zip(sources, places))]
    for copy in copies:
        copy.start()
    for copy in copies:
        copy.wait()


def per_device(sizes, frames_in, norm_gain, norm_bias, conv_weight, cotangent):
    nz, nc, ny, nx = sizes
    n_tm, n_rows = nz * nc, ny * nx
    frames, band, width, chans = frames_in.shape
    own_o = chans // n_rows
    rows = (2 * frames, band + 2)
    vmem, dma = pltpu.VMEM, pltpu.SemaphoreType.DMA
    scratch = [
        vmem((1, chans), F32),
        vmem((1, chans), F32),
        vmem((*rows, width, chans), BF16),
        vmem((*rows, width, chans), BF16),
        vmem((27, chans, chans), BF16),
        vmem((*rows, WP, chans), BF16),
        vmem((2, *rows, WP, chans), BF16),
        vmem((3, *rows, WP, chans), BF16),
        vmem((3 * chans, frames * band * WP), BF16),
        vmem((frames * band * WP, chans), F32),
        vmem((3, 9, chans, chans), F32),
        vmem((CHUNKS, PER, chans, chans), BF16),
        vmem((CHUNKS, PER, chans, chans), BF16),
        vmem((CHUNKS, n_rows, PER, own_o, chans), BF16),
        vmem((CHUNKS, n_rows, PER, own_o, chans), BF16),
        vmem((CHUNKS, nz, PER, own_o, chans), BF16),
        vmem((2, CHUNKS, PER, own_o, chans), F32),
        vmem((n_rows, 2, chans), F32),
        vmem((n_tm, 2, chans), F32),
        vmem((n_rows, 2, chans), F32),
        vmem((n_tm, 2, chans), F32),
        dma((5,)),
        dma((5,)), dma((5,)), dma((5,)), dma((5,)),
        dma((1,)), dma((1,)), dma((1,)), dma((1,)), dma((1,)), dma((1,)), dma((1,)), dma((1,)),
        dma((CHUNKS,)), dma((CHUNKS,)),
        dma((len(PIECES),)), dma((len(PIECES),)),
        dma((len(PIECES),)), dma((len(PIECES),)),
        dma((len(PIECES),)), dma((len(PIECES),)),
    ]
    anywhere = pl.BlockSpec(memory_space=pl.ANY)
    stays = pl.BlockSpec(memory_space=pltpu.HBM)
    out = jax.ShapeDtypeStruct
    made = pl.pallas_call(
        functools.partial(kernel, sizes),
        out_shape=(
            out(frames_in.shape, BF16),
            out(frames_in.shape, BF16),
            out((own_o, 27 * chans), F32),
            out((1, chans), F32),
            out((1, chans), F32),
        ),
        in_specs=[stays] * 5,
        out_specs=[pl.BlockSpec(memory_space=pltpu.VMEM)] * 5,
        scratch_shapes=scratch,
        compiler_params=pltpu.CompilerParams(
            collective_id=0, has_side_effects=True, vmem_limit_bytes=48 << 20
        ),
        name="block",
    )(
        *(
            pltpu.with_memory_space_constraint(a, pltpu.HBM)
            for a in (
                frames_in,
                norm_gain.reshape(1, chans),
                norm_bias.reshape(1, chans),
                conv_weight.reshape(27, chans, chans),
                cotangent,
            )
        )
    )
    of, ig, wg, gg, bg = pl.pallas_call(
        put_out,
        out_shape=[out(a.shape, a.dtype) for a in made],
        in_specs=[anywhere] * 5,
        out_specs=[stays] * 5,
        scratch_shapes=[dma((5,))],
        compiler_params=pltpu.CompilerParams(vmem_limit_bytes=1 << 20),
        name="put_out",
    )(*made)
    return of, ig, wg, gg.reshape(chans), bg.reshape(chans)


def program(devices):
    torus = Mesh(devices, ("z", "c", "y", "x"))
    placed = (P(TM, ROWS, None, None), P(), P(), P(), P(TM, ROWS, None, None))
    return jax.shard_map(
        functools.partial(per_device, devices.shape),
        mesh=torus,
        in_specs=placed,
        out_specs=(P(TM, ROWS, None, None), P(TM, ROWS, None, None), P(ROWS, None), P(), P()),
        check_vma=False,
    )


def solution(mesh):
    return program(mesh.devices.reshape(8, 2, 4, 4))
```

```python
import functools
import math

import jax
import jax.numpy as jnp
from jax import lax
from jax.experimental import pallas as pl
from jax.experimental.pallas import tpu as pltpu
from jax.sharding import Mesh
from jax.sharding import PartitionSpec as P

G = 32
EPSILON = 1e-06
TM = ("z", "c")
ROWS = ("y", "x")
MESH = pl.DeviceIdType.MESH
WP = 128
F32 = jnp.float32
BF16 = jnp.bfloat16
PAIRS = tuple((a, b) for a in (2, 1, 0) for b in range(3))
PIECES = ((0, 1), (1, 3), (3, 5), (5, 7), (7, 9))
N_PIECES = len(PIECES)


def group_total(per_channel, size):
    lanes = lax.broadcasted_iota(jnp.int32, per_channel.shape, 1)
    within = lanes % size
    channels = per_channel.shape[1]
    total = per_channel
    for step in range(1, size):
        ahead = pltpu.roll(per_channel, channels - step, 1)
        behind = pltpu.roll(per_channel, step, 1)
        total = total + jnp.where(within + step < size, ahead, 0.0)
        total = total + jnp.where(within >= step, behind, 0.0)
    return total


def kernel(
    sizes, x_hbm, gn_hbm, sh_hbm, w_hbm, cot_hbm,
    ofv, igv, wgv, gv, bv,
    gain_ref, bias_ref, xr, cr, cpart, wv, a0, a3, c3, c3e, ct, ga, cv, bsend, brecv, crecv, fin,
    st1, st2, gs1, gs2,
    load_sem, xs, xq, cs, cq, ps, pq, st_s, st_r, bs, br, zs, zr, fs, fr,
):
    nz, nc, ny, nx = sizes
    n_tm, n_rows = nz * nc, ny * nx
    frames, band, width, chans = x_hbm.shape
    high_rows = band + 2
    own_o = chans // n_rows
    dests = n_rows // nc
    half_o = chans // nc
    all_pixels = frames * n_tm * band * n_rows * width
    cells = all_pixels * (chans // G)
    z, c = lax.axis_index("z"), lax.axis_index("c")
    y, x = lax.axis_index("y"), lax.axis_index("x")
    tm, row = z * nc + c, y * nx + x
    own = frames + frames * c
    other = {"z": z, "c": 1 - c, "y": y, "x": x}
    lead, follow = c == 0, c == 1
    has_before = z > 0

    def at(t, r):
        t, r = lax.rem(t + n_tm, n_tm), lax.rem(r + n_rows, n_rows)
        return {"z": t // nc, "c": lax.rem(t, nc), "y": r // nx, "x": lax.rem(r, nx)}

    def farthest_first(steps):
        return sorted(steps, key=lambda pairs: -sum(min(d, n - d) for d, n in pairs))

    def xy_peers():
        for (dy, _), (dx, _) in farthest_first(
            [((k // nx, ny), (k % nx, nx)) for k in range(1, n_rows)]
        ):
            ty, tx = lax.rem(y + dy, ny), lax.rem(x + dx, nx)
            yield {"z": z, "c": c, "y": ty, "x": tx}

    def zc_peers():
        for (dz, _), (dc, _) in farthest_first(
            [((k // nc, nz), (k % nc, nc)) for k in range(1, n_tm)]
        ):
            tz, tc = lax.rem(z + dz, nz), lax.rem(c + dc, nc)
            yield {"z": tz, "c": tc, "y": y, "x": x}

    def z_peers():
        for ((dz, _),) in farthest_first([((k, nz),) for k in range(1, nz)]):
            yield {"z": lax.rem(z + dz, nz), "c": c, "y": y, "x": x}

    def remote(src, dst, send_sem, recv_sem, device):
        return pltpu.make_async_remote_copy(
            src_ref=src, dst_ref=dst, send_sem=send_sem, recv_sem=recv_sem,
            device_id=device, device_id_type=MESH,
        )

    def several(slots, count, send_sem, recv_sem):
        some = slots.at[0:count]
        return remote(some, some, send_sem, recv_sem, other)

    load_x = pltpu.make_async_copy(
        x_hbm, xr.at[pl.ds(own, frames), 1 : band + 1], load_sem.at[0]
    )
    load_c = pltpu.make_async_copy(cot_hbm, cr.at[0:frames, 1 : band + 1], load_sem.at[1])
    load_w = pltpu.make_async_copy(w_hbm, wv, load_sem.at[2])
    load_gn = pltpu.make_async_copy(gn_hbm, gain_ref, load_sem.at[3])
    load_sh = pltpu.make_async_copy(sh_hbm, bias_ref, load_sem.at[4])
    for copy in (load_x, load_c, load_w, load_gn, load_sh):
        copy.start()

    barrier = pltpu.get_barrier_semaphore()
    partners = 0
    corners = [at(tm + dt, row + dw) for dt in (-1, 1) for dw in (-1, 1)]
    for device in (*zc_peers(), *xy_peers(), *corners):
        pl.semaphore_signal(barrier, inc=1, device_id=device, device_id_type=MESH)
        partners += 1

    load_x.wait()

    def folded(v):
        return v.reshape(width // 8, 8, chans).sum(axis=0)

    def stat_row(k, carry):
        total, square = carry
        v = xr[own + k // band, 1 + lax.rem(k, band)].astype(F32)
        return total + folded(v), square + folded(v * v)

    zero8 = jnp.zeros((8, chans), F32)
    total, square = lax.fori_loop(0, frames * band, stat_row, (zero8, zero8))
    st1[row, 0:1] = total.sum(axis=0, keepdims=True)
    st1[row, 1:2] = square.sum(axis=0, keepdims=True)

    pl.semaphore_wait(barrier, partners)

    def summed(slots):
        total = slots[0]
        for k in range(1, slots.shape[0]):
            total = total + slots[k]
        return total

    def spread(slots, mine, peers, k):
        for device in peers:
            remote(slots.at[mine], slots.at[mine], st_s.at[k], st_r.at[k], device).start()

    def gathered(slots, k):
        return several(slots, slots.shape[0] - 1, st_s.at[k], st_r.at[k])

    spread(st1, row, xy_peers(), 0)

    def margins(buf, first, there, way, sends_on, gets_on, send_sem, recv_sem):
        mine = buf.at[pl.ds(first, frames)]
        moved = buf.at[pl.ds(there, frames)]
        up_t = (tm + way >= 0) & (tm + way < n_tm) & sends_on
        from_t = (tm - way >= 0) & (tm - way < n_tm) & gets_on
        up_r, down_r = row < n_rows - 1, row > 0
        low, high, body = mine.at[:, 1], mine.at[:, band], slice(1, band + 1)
        plan = [
            (high, mine.at[:, 0], at(tm, row + 1), up_r, down_r),
            (low, mine.at[:, band + 1], at(tm, row - 1), down_r, up_r),
            (mine.at[:, body], moved.at[:, body], at(tm + way, row), up_t, from_t),
            (high, moved.at[:, 0], at(tm + way, row + 1), up_t & up_r, from_t & down_r),
            (low, moved.at[:, band + 1], at(tm + way, row - 1), up_t & down_r, from_t & up_r),
        ]
        return [
            (remote(src, dst, send_sem.at[k], recv_sem.at[k], device), sends, gets)
            for k, (src, dst, device, sends, gets) in enumerate(plan)
        ]

    load_c.wait()
    cot_margins = margins(cr, 0, frames, -1, True, True, cs, cq)
    x_margins = margins(xr, own, 0, 1, follow, lead, xs, xq)
    partner_cot = remote(cr.at[0:frames, 1 : band + 1], cpart, ps.at[0], pq.at[0], other)
    mine_x = xr.at[pl.ds(own, frames), 1 : band + 1]
    swapped_x = remote(mine_x, mine_x, ps.at[1], pq.at[1], other)

    def started(copy, sends):
        @pl.when(sends)
        def _():
            copy.start()

    def received(copy, gets):
        @pl.when(gets)
        def _():
            copy.wait_recv()

    def left(copy, sends):
        @pl.when(sends)
        def _():
            copy.wait_send()

    partner_cot.start()
    swapped_x.start()
    for copy, sends, _ in (*x_margins, *cot_margins):
        started(copy, sends)

    zeros_pad = jnp.zeros((WP - width, chans), F32)

    def padded_row(v):
        return jnp.concatenate([v, zeros_pad], axis=0)

    def three_ways(v, keep=True):
        v = padded_row(v.astype(F32))
        if keep is not True:
            v = jnp.where(keep, v, 0.0)
        return pltpu.roll(v, 1, 0), v, pltpu.roll(v, WP - 1, 0)

    def cot_row(t, h, keep=True):
        sides = three_ways(cr[t, h], keep)
        for shift in range(3):
            c3[shift, t, h] = sides[shift].astype(BF16)
        return sides

    def put_turned(chip_half, k, sides):
        for shift in range(3):
            turned = sides[2 - shift].T.astype(BF16)
            for core in range(nc):
                ct[chip_half, core, shift * half_o : (shift + 1) * half_o, k * WP : (k + 1) * WP] = (
                    turned[core * half_o : (core + 1) * half_o]
                )

    for k in range(frames * band):
        put_turned(c, k, cot_row(k // band, 1 + k % band))
    for h in (0, band + 1):
        c3[:, :, h] = jnp.zeros((3, 2 * frames, WP, chans), BF16)
    load_w.wait()
    load_gn.wait()
    load_sh.wait()
    partner_cot.wait_recv()
    for k in range(frames * band):
        put_turned(1 - c, k, three_ways(cpart[k // band, k % band]))

    gathered(st1, 0).wait_recv()
    st2[tm] = summed(st1)
    spread(st2, tm, zc_peers(), 1)

    row_low, row_high = row > 0, row < n_rows - 1
    before = xr.at[0:frames]
    passed_low = remote(before.at[:, 0], before.at[:, 0], ps.at[5], pq.at[5], other)
    passed_high = remote(before.at[:, band + 1], before.at[:, band + 1], ps.at[6], pq.at[6], other)
    body_before = before.at[:, 1 : band + 1]
    passed_body = remote(body_before, body_before, ps.at[4], pq.at[4], other)
    mine_all = xr.at[pl.ds(own, frames)]
    gave_low = remote(mine_all.at[:, 0], mine_all.at[:, 0], ps.at[2], pq.at[2], other)
    gave_high = remote(mine_all.at[:, band + 1], mine_all.at[:, band + 1], ps.at[3], pq.at[3], other)
    for copy, _, gets in x_margins[:2]:
        received(copy, gets)
    started(gave_low, row_low)
    started(gave_high, row_high)

    taps = [(b, s) for b in range(3) for s in range(3)]

    def frame(refs, t):
        rows = [refs[s][t, b : b + band].reshape(band * WP, chans) for b, s in taps]
        return jnp.concatenate(rows, axis=1)

    def back_taps(a):
        return jnp.concatenate([wv[9 * (2 - a) + 3 * (2 - b) + 2 - s] for b, s in taps], axis=1)

    def back(lhs, rhs):
        return lax.dot_general(lhs, rhs, (((1,), (1,)), ((), ())), preferred_element_type=F32)

    half = band * WP
    c3s = [c3.at[s] for s in range(3)]
    both = back(frame(c3s, 1), jnp.concatenate([back_taps(1), back_taps(0)], axis=0))
    ga[0:half] = back(frame(c3s, 0), back_taps(0)) + both[:, :chans]
    ga[half:] = both[:, chans:]

    received(cot_margins[2][0], cot_margins[2][2])
    has_next = tm < n_tm - 1
    for t in range(frames, 2 * frames):
        for h in range(1, band + 1):
            cot_row(t, h, has_next)
    both = back(frame(c3s, 2), jnp.concatenate([back_taps(2), back_taps(1)], axis=0))
    ga[0:half] += both[:, :chans]
    ga[half:] += back(frame(c3s, 3), back_taps(2)) + both[:, chans:]

    gathered(st2, 1).wait_recv()
    stats = summed(st2)
    wide = lambda v: jnp.broadcast_to(v, (8, chans))
    mean = group_total(wide(stats[0:1]), chans // G) / cells
    variance = group_total(wide(stats[1:2]), chans // G) / cells - mean * mean
    inverse = lax.rsqrt(variance + EPSILON)
    gain, shift_ = wide(gain_ref[...]), wide(bias_ref[...])
    mean, inverse, gain, shift_ = (v[0:1] for v in (mean, inverse, gain, shift_))

    swapped_x.wait_recv()
    received(gave_low, row_low)
    received(gave_high, row_high)

    def sigmoid(v):
        return 0.5 + 0.5 * jnp.tanh(0.5 * v)

    def act_frames(low, high, rows=range(band + 2)):
        for t in range(low, high):
            for h in rows:
                v = xr[t, h].astype(F32)
                pre = (v - mean) * inverse * gain + shift_
                act = pre * sigmoid(pre)
                keep = True
                if t < frames:
                    keep = has_before
                if h == 0:
                    keep = keep & row_low
                if h == band + 1:
                    keep = keep & row_high
                if keep is not True:
                    act = jnp.where(keep, act, 0.0)
                a0[t, h] = padded_row(act).astype(BF16)

    chip_frames = frames * nc
    turned = lambda: jnp.concatenate([ct[h, c] for h in range(nc)], axis=1)
    active = row // dests == c
    place = lax.rem(row, dests)

    def blocks_of(p):
        low, high = PIECES[p]
        return slice(3 * low, 3 * high)

    def weight_piece(p):
        low, high = PIECES[p]
        rhs = jnp.concatenate(
            [
                a0[a : a + chip_frames, b : b + band].reshape(chip_frames * half, chans)
                for a, b in PAIRS[low:high]
            ],
            axis=1,
        )
        part = jnp.dot(turned(), rhs, preferred_element_type=F32)
        for j in range(high - low):
            for s in range(3):
                block = part[s * half_o : (s + 1) * half_o, j * chans : (j + 1) * chans]
                bsend[:, 3 * (low + j) + s] = block.reshape(dests, own_o, chans).astype(BF16)

    def send_rows(p):
        blocks = blocks_of(p)

        @pl.when(active)
        def _():
            brecv[row, blocks] = bsend[place, blocks]

        for q in range(dests):
            to = dests * c + q
            device = {"z": z, "c": c, "y": to // nx, "x": lax.rem(to, nx)}
            copy = remote(
                bsend.at[q, blocks], brecv.at[row, blocks], bs.at[p], br.at[p], device
            )
            started(copy, to != row)

    act_frames(frames, frames + chip_frames, range(band))
    for copy, _, gets in x_margins[2:]:
        received(copy, gets)
    started(passed_body, lead & has_before)
    started(passed_low, lead & has_before & row_low)
    started(passed_high, lead & has_before & row_high)

    weight_piece(0)
    send_rows(0)
    act_frames(frames, frames + chip_frames, range(band, band + 2))
    weight_piece(1)
    send_rows(1)
    received(passed_body, follow & has_before)
    received(passed_low, follow & has_before & row_low)
    received(passed_high, follow & has_before & row_high)
    act_frames(1, 2)

    weight_piece(2)
    send_rows(2)
    act_frames(0, 1)
    for k in (0, 1, 3, 4):
        received(cot_margins[k][0], cot_margins[k][2])
    for t in range(2 * frames):
        for side, exists in ((0, row_low), (1, row_high)):
            keep = exists & has_next if t >= frames else exists
            sides = three_ways(cr[t, side * (band + 1)], keep)
            for shift in range(3):
                c3e[shift, t, side] = sides[shift].astype(BF16)
    for side, b in ((0, 0), (1, 2)):
        lhs = jnp.concatenate(
            [
                jnp.concatenate(
                    [c3e[s, t + a, side] for a in range(3) for s in range(3)], axis=1
                )
                for t in range(frames)
            ],
            axis=0,
        )
        rhs = jnp.concatenate(
            [wv[9 * (2 - a) + 3 * (2 - b) + 2 - s] for a in range(3) for s in range(3)], axis=1
        )
        edge = back(lhs, rhs)
        for t in range(frames):
            at_t = t * half + side * (band - 1) * WP
            ga[at_t : at_t + WP] += edge[t * WP : (t + 1) * WP]

    def pre_row(k):
        v = xr[own + k // band, 1 + k % band].astype(F32)
        return (v - mean) * inverse

    gains, biases = zero8, zero8
    for k in range(frames * band):
        normed = pre_row(k)
        pre = normed * gain + shift_
        sig = sigmoid(pre)
        at_k = slice(k * WP, k * WP + width)
        grad = ga[at_k] * sig * (1.0 + pre * (1.0 - sig))
        ga[at_k] = grad
        gains = gains + folded(grad * normed)
        biases = biases + folded(grad)
    gs1[tm, 0:1] = gains.sum(axis=0, keepdims=True)
    gs1[tm, 1:2] = biases.sum(axis=0, keepdims=True)
    spread(gs1, tm, zc_peers(), 2)

    weight_piece(3)
    send_rows(3)
    weight_piece(4)
    send_rows(4)

    def of_piece(buf, count, p, send_sem, recv_sem):
        blocks = blocks_of(p)
        return several(buf.at[:, blocks], count, send_sem.at[p], recv_sem.at[p])

    def send_z(p):
        blocks = blocks_of(p)

        @pl.when(active)
        def _():
            of_piece(brecv, n_rows - 1, p, bs, br).wait_recv()
            value = brecv[0, blocks].astype(F32)
            for k in range(1, n_rows):
                value = value + brecv[k, blocks].astype(F32)
            crecv[z, blocks] = value.astype(BF16)
            mine = crecv.at[z, blocks]
            for device in z_peers():
                remote(mine, mine, zs.at[p], zr.at[p], device).start()

    def shift_row(k, carry):
        t, h = k // high_rows, lax.rem(k, high_rows)
        v = a0[frames * c + t, h].astype(F32)
        a3[0, t, h] = pltpu.roll(v, 1, 0).astype(BF16)
        a3[1, t, h] = pltpu.roll(v, WP - 1, 0).astype(BF16)
        return carry

    lax.fori_loop(0, 2 * frames * high_rows, shift_row, 0)
    send_z(0)
    sides = (a3.at[0], a0.at[pl.ds(frames * c, 2 * frames)], a3.at[1])

    def front_taps(a):
        return jnp.concatenate([wv[9 * a + 3 * b + s] for b, s in taps], axis=0)

    def front(lhs, rhs):
        return jnp.dot(lhs, rhs, preferred_element_type=F32)

    one = front(frame(sides, 1), jnp.concatenate([front_taps(1), front_taps(0)], axis=1))
    cv[0:half] = front(frame(sides, 0), front_taps(0)) + one[:, :chans]
    cv[half:] = one[:, chans:]
    send_z(1)
    two = front(frame(sides, 2), jnp.concatenate([front_taps(2), front_taps(1)], axis=1))
    cv[0:half] += two[:, :chans]
    cv[half:] += front(frame(sides, 3), front_taps(2)) + two[:, chans:]
    for k in range(frames * band):
        v = xr[own + k // band, 1 + k % band].astype(F32)
        ofv[k // band, k % band] = (v + cv[k * WP : k * WP + width]).astype(BF16)
    send_z(2)
    gathered(gs1, 2).wait_recv()
    gs2[row] = summed(gs1)
    spread(gs2, row, xy_peers(), 3)

    send_z(3)

    send_z(4)

    gathered(gs2, 3).wait_recv()
    sums = summed(gs2)
    gain_grad, bias_grad = wide(sums[0:1]), wide(sums[1:2])
    gv[...] = sums[0:1]
    bv[...] = sums[1:2]
    mean_dn = (group_total(gain * bias_grad, chans // G) / cells)[0:1]
    mean_dnn = (group_total(gain * gain_grad, chans // G) / cells)[0:1]
    for k in range(frames * band):
        t, h = k // band, k % band
        normed = pre_row(k)
        grad = ga[k * WP : k * WP + width]
        cot = cr[t, 1 + h].astype(F32)
        igv[t, h] = (inverse * (grad * gain - mean_dn - normed * mean_dnn) + cot).astype(BF16)

    to_core = []
    for p in range(N_PIECES):
        blocks = blocks_of(p)
        mine = fin.at[blocks]
        copy = remote(mine, mine, fs.at[p], fr.at[p], other)
        to_core.append(copy)

        @pl.when(active)
        def _():
            of_piece(crecv, nz - 1, p, zs, zr).wait_recv()
            value = crecv[0, blocks].astype(F32)
            for k in range(1, nz):
                value = value + crecv[k, blocks].astype(F32)
            fin[blocks] = value
            copy.start()

    scale = 1.0 / math.sqrt(all_pixels)
    for p in range(N_PIECES):
        blocks = blocks_of(p)
        received(to_core[p], jnp.logical_not(active))
        for m in range(blocks.start, blocks.stop):
            a, b = PAIRS[m // 3]
            at_m = (9 * a + 3 * b + m % 3) * chans
            wgv[:, at_m : at_m + chans] = fin[m] * scale

    for slots, k in ((st1, 0), (st2, 1), (gs1, 2), (gs2, 3)):
        gathered(slots, k).wait_send()
    partner_cot.wait_send()
    swapped_x.wait_send()
    for copy, sends, _ in (*cot_margins, *x_margins):
        left(copy, sends)
    left(gave_low, row_low)
    left(gave_high, row_high)
    left(passed_body, lead & has_before)
    left(passed_low, lead & has_before & row_low)
    left(passed_high, lead & has_before & row_high)

    @pl.when(active)
    def _():
        for p in range(N_PIECES):
            of_piece(bsend, dests - 1, p, bs, br).wait_send()
            of_piece(crecv, nz - 1, p, zs, zr).wait_send()
            to_core[p].wait_send()

    @pl.when(jnp.logical_not(active))
    def _():
        for p in range(N_PIECES):
            of_piece(bsend, dests, p, bs, br).wait_send()


def put_out(*refs):
    sources, places, sem = refs[:5], refs[5:10], refs[10]
    copies = [pltpu.make_async_copy(s, d, sem.at[k]) for k, (s, d) in enumerate(zip(sources, places))]
    for copy in copies:
        copy.start()
    for copy in copies:
        copy.wait()


def per_device(sizes, frames_in, norm_gain, norm_bias, conv_weight, cotangent):
    nz, nc, ny, nx = sizes
    n_tm, n_rows = nz * nc, ny * nx
    frames, band, width, chans = frames_in.shape
    own_o, dests = chans // n_rows, n_rows // nc
    rows = (2 * frames, band + 2)
    chip = (frames + frames * nc, band + 2)
    vmem, dma = pltpu.VMEM, pltpu.SemaphoreType.DMA
    scratch = [
        vmem((1, chans), F32),
        vmem((1, chans), F32),
        vmem((*chip, width, chans), BF16),
        vmem((*rows, width, chans), BF16),
        vmem((frames, band, width, chans), BF16),
        vmem((27, chans, chans), BF16),
        vmem((*chip, WP, chans), BF16),
        vmem((2, *rows, WP, chans), BF16),
        vmem((3, *rows, WP, chans), BF16),
        vmem((3, 2 * frames, 2, WP, chans), BF16),
        vmem((nc, nc, 3 * chans // nc, frames * band * WP), BF16),
        vmem((frames * band * WP, chans), F32),
        vmem((frames * band * WP, chans), F32),
        vmem((dests, 27, own_o, chans), BF16),
        vmem((n_rows, 27, own_o, chans), BF16),
        vmem((nz, 27, own_o, chans), BF16),
        vmem((27, own_o, chans), F32),
        vmem((n_rows, 2, chans), F32),
        vmem((n_tm, 2, chans), F32),
        vmem((n_tm, 2, chans), F32),
        vmem((n_rows, 2, chans), F32),
        dma((5,)),
        dma((5,)), dma((5,)), dma((5,)), dma((5,)), dma((7,)), dma((7,)), dma((4,)), dma((4,)),
        dma((N_PIECES,)), dma((N_PIECES,)), dma((N_PIECES,)), dma((N_PIECES,)),
        dma((N_PIECES,)), dma((N_PIECES,)),
    ]
    anywhere = pl.BlockSpec(memory_space=pl.ANY)
    stays = pl.BlockSpec(memory_space=pltpu.HBM)
    inside = pl.BlockSpec(memory_space=pltpu.VMEM)
    out = jax.ShapeDtypeStruct
    operands = (
        frames_in,
        norm_gain.reshape(1, chans),
        norm_bias.reshape(1, chans),
        conv_weight.reshape(27, chans, chans),
        cotangent,
    )
    made = pl.pallas_call(
        functools.partial(kernel, sizes),
        out_shape=(
            out(frames_in.shape, BF16),
            out(frames_in.shape, BF16),
            out((own_o, 27 * chans), F32),
            out((1, chans), F32),
            out((1, chans), F32),
        ),
        in_specs=[stays] * 5,
        out_specs=[inside] * 5,
        scratch_shapes=scratch,
        compiler_params=pltpu.CompilerParams(
            collective_id=0, has_side_effects=True, vmem_limit_bytes=48 << 20
        ),
        name="block",
    )(*(pltpu.with_memory_space_constraint(a, pltpu.HBM) for a in operands))
    of, ig, wg, gg, bg = pl.pallas_call(
        put_out,
        out_shape=[out(a.shape, a.dtype) for a in made],
        in_specs=[anywhere] * 5,
        out_specs=[stays] * 5,
        scratch_shapes=[dma((5,))],
        compiler_params=pltpu.CompilerParams(vmem_limit_bytes=1 << 20),
        name="put_out",
    )(*made)
    return of, ig, wg, gg.reshape(chans), bg.reshape(chans)


def program(devices):
    torus = Mesh(devices, ("z", "c", "y", "x"))
    placed = (P(TM, ROWS, None, None), P(), P(), P(), P(TM, ROWS, None, None))
    return jax.shard_map(
        functools.partial(per_device, devices.shape),
        mesh=torus,
        in_specs=placed,
        out_specs=(P(TM, ROWS, None, None), P(TM, ROWS, None, None), P(ROWS, None), P(), P()),
        check_vma=False,
    )


def solution(mesh):
    return program(mesh.devices.reshape(8, 2, 4, 4))
```

```python
import functools
import math

import jax
import jax.numpy as jnp
from jax import lax
from jax.experimental import pallas as pl
from jax.experimental.pallas import tpu as pltpu
from jax.sharding import Mesh
from jax.sharding import PartitionSpec as P

G = 32
EPSILON = 1e-06
TM = ("z", "c")
ROWS = ("y", "x")
MESH = pl.DeviceIdType.MESH
WP = 128
F32 = jnp.float32
BF16 = jnp.bfloat16
PAIRS = tuple((a, b) for a in (2, 1, 0) for b in range(3))
PIECES = ((0, 1), (1, 3), (3, 5), (5, 7), (7, 8), (8, 9))
N_PIECES = len(PIECES)


def group_total(per_channel, size):
    lanes = lax.broadcasted_iota(jnp.int32, per_channel.shape, 1)
    within = lanes % size
    channels = per_channel.shape[1]
    total = per_channel
    for step in range(1, size):
        ahead = pltpu.roll(per_channel, channels - step, 1)
        behind = pltpu.roll(per_channel, step, 1)
        total = total + jnp.where(within + step < size, ahead, 0.0)
        total = total + jnp.where(within >= step, behind, 0.0)
    return total


def kernel(
    sizes, x_hbm, gn_hbm, sh_hbm, w_hbm, cot_hbm,
    ofv, igv, wgv, gv, bv,
    gain_ref, bias_ref, xr, cr, cpart, wv, a0, a3, c3, c3e, ct, ga, cv, bsend, brecv, crecv, fin,
    st1, st2, gs1, gs2,
    load_sem, xs, xq, cs, cq, ps, pq, st_s, st_r, bs, br, zs, zr, fs, fr,
):
    nz, nc, ny, nx = sizes
    n_tm, n_rows = nz * nc, ny * nx
    frames, band, width, chans = x_hbm.shape
    high_rows = band + 2
    own_o = chans // n_rows
    dests = n_rows // nc
    half_o = chans // nc
    all_pixels = frames * n_tm * band * n_rows * width
    cells = all_pixels * (chans // G)
    z, c = lax.axis_index("z"), lax.axis_index("c")
    y, x = lax.axis_index("y"), lax.axis_index("x")
    tm, row = z * nc + c, y * nx + x
    own = frames + frames * c
    other = {"z": z, "c": 1 - c, "y": y, "x": x}
    lead, follow = c == 0, c == 1
    has_before = z > 0

    def at(t, r):
        t, r = lax.rem(t + n_tm, n_tm), lax.rem(r + n_rows, n_rows)
        return {"z": t // nc, "c": lax.rem(t, nc), "y": r // nx, "x": lax.rem(r, nx)}

    def farthest_first(steps):
        return sorted(steps, key=lambda pairs: -sum(min(d, n - d) for d, n in pairs))

    def plane(core):
        steps = [((k // nx, ny), (k % nx, nx)) for k in range(1, n_rows)]
        for (dy, _), (dx, _) in farthest_first(steps):
            yield {"z": z, "c": core, "y": lax.rem(y + dy, ny), "x": lax.rem(x + dx, nx)}

    def column(core):
        for ((dz, _),) in farthest_first([((k, nz),) for k in range(1, nz)]):
            yield {"z": lax.rem(z + dz, nz), "c": core, "y": y, "x": x}

    def remote(src, dst, send_sem, recv_sem, device):
        return pltpu.make_async_remote_copy(
            src_ref=src, dst_ref=dst, send_sem=send_sem, recv_sem=recv_sem,
            device_id=device, device_id_type=MESH,
        )

    def several(slots, count, send_sem, recv_sem):
        some = slots.at[0:count]
        return remote(some, some, send_sem, recv_sem, other)

    def started(copy, sends):
        @pl.when(sends)
        def _():
            copy.start()

    def received(copy, gets):
        @pl.when(gets)
        def _():
            copy.wait_recv()

    def left(copy, sends):
        @pl.when(sends)
        def _():
            copy.wait_send()

    load_x = pltpu.make_async_copy(
        x_hbm, xr.at[pl.ds(own, frames), 1 : band + 1], load_sem.at[0]
    )
    load_c = pltpu.make_async_copy(cot_hbm, cr.at[0:frames, 1 : band + 1], load_sem.at[1])
    load_w = pltpu.make_async_copy(w_hbm, wv, load_sem.at[2])
    load_gn = pltpu.make_async_copy(gn_hbm, gain_ref, load_sem.at[3])
    load_sh = pltpu.make_async_copy(sh_hbm, bias_ref, load_sem.at[4])
    for copy in (load_x, load_c, load_w, load_gn, load_sh):
        copy.start()

    barrier = pltpu.get_barrier_semaphore()
    def enter(devices):
        for device in devices:
            pl.semaphore_signal(barrier, inc=1, device_id=device, device_id_type=MESH)

    corners = [at(tm + dt, row + dw) for dt in (-1, 1) for dw in (-1, 1)]
    enter((*column(1), *plane(1), other, *corners))

    @pl.when(follow)
    def _():
        enter((*column(0), *plane(0)))

    @pl.when(lead)
    def _():
        enter((at(tm, row + 1), at(tm, row - 1)))

    chips = n_rows - 1 + nz - 1
    partners = jnp.where(follow, 2 * chips + 5, chips + 7)

    load_x.wait()

    def folded(v):
        return v.reshape(width // 8, 8, chans).sum(axis=0)

    def stat_row(k, carry):
        total, square = carry
        v = xr[own + k // band, 1 + lax.rem(k, band)].astype(F32)
        return total + folded(v), square + folded(v * v)

    zero8 = jnp.zeros((8, chans), F32)
    total, square = lax.fori_loop(0, frames * band, stat_row, (zero8, zero8))
    st1[nc * row + c, 0:1] = total.sum(axis=0, keepdims=True)
    st1[nc * row + c, 1:2] = square.sum(axis=0, keepdims=True)

    pl.semaphore_wait(barrier, partners)

    def summed(slots):
        total = slots[0]
        for k in range(1, slots.shape[0]):
            total = total + slots[k]
        return total

    def collect(slots, mine, peers, k):
        part = slots.at[mine]
        for device in peers:
            remote(part, part, st_s.at[k], st_r.at[k], device).start()
        started(remote(part, part, st_s.at[k], st_r.at[k], other), lead)

    def spread(slots, mine, collected, peers, k):
        @pl.when(follow)
        def _():
            several(collected, collected.shape[0] - 1, st_s.at[k - 1], st_r.at[k - 1]).wait_recv()
            slots[mine] = summed(collected)
            part = slots.at[mine]
            for device in (*peers, other):
                remote(part, part, st_s.at[k], st_r.at[k], device).start()

    def finished(slots, k):
        received(several(slots, slots.shape[0] - 1, st_s.at[k], st_r.at[k]), follow)
        received(several(slots, slots.shape[0], st_s.at[k], st_r.at[k]), lead)

    collect(st1, nc * row + c, plane(1), 0)

    def margins(buf, first, there, way, body_from, corners_from, send_sem, recv_sem):
        mine = buf.at[pl.ds(first, frames)]
        moved = buf.at[pl.ds(there, frames)]
        up_t = (tm + way >= 0) & (tm + way < n_tm)
        from_t = (tm - way >= 0) & (tm - way < n_tm)
        up_c, from_c = up_t & (c == corners_from), from_t & (c != corners_from)
        if body_from is not None:
            up_t, from_t = up_t & (c == body_from), from_t & (c != body_from)
        up_r, down_r = row < n_rows - 1, row > 0
        low, high, body = mine.at[:, 1], mine.at[:, band], slice(1, band + 1)
        plan = [
            (high, mine.at[:, 0], at(tm, row + 1), up_r, down_r),
            (low, mine.at[:, band + 1], at(tm, row - 1), down_r, up_r),
            (mine.at[:, body], moved.at[:, body], at(tm + way, row), up_t, from_t),
            (high, moved.at[:, 0], at(tm + way, row + 1), up_c & up_r, from_c & down_r),
            (low, moved.at[:, band + 1], at(tm + way, row - 1), up_c & down_r, from_c & up_r),
        ]
        return [
            (remote(src, dst, send_sem.at[k], recv_sem.at[k], device), sends, gets)
            for k, (src, dst, device, sends, gets) in enumerate(plan)
        ]

    load_c.wait()
    cot_margins = margins(cr, 0, frames, -1, None, 0, cs, cq)
    x_margins = margins(xr, own, 0, 1, 1, 1, xs, xq)
    partner_cot = remote(cr.at[0:frames, 1 : band + 1], cpart, ps.at[0], pq.at[0], other)
    mine_x = xr.at[pl.ds(own, frames), 1 : band + 1]
    swapped_x = remote(mine_x, mine_x, ps.at[1], pq.at[1], other)

    partner_cot.start()
    swapped_x.start()
    for copy, sends, _ in (*x_margins, *cot_margins):
        started(copy, sends)

    zeros_pad = jnp.zeros((WP - width, chans), F32)

    def padded_row(v):
        return jnp.concatenate([v, zeros_pad], axis=0)

    def three_ways(v, keep=True):
        v = padded_row(v.astype(F32))
        if keep is not True:
            v = jnp.where(keep, v, 0.0)
        return pltpu.roll(v, 1, 0), v, pltpu.roll(v, WP - 1, 0)

    def cot_row(t, h, keep=True):
        sides = three_ways(cr[t, h], keep)
        for shift in range(3):
            c3[shift, t, h] = sides[shift].astype(BF16)
        return sides

    def put_turned(chip_half, k, sides):
        for shift in range(3):
            turned = sides[2 - shift].T.astype(BF16)
            for core in range(nc):
                ct[chip_half, core, shift * half_o : (shift + 1) * half_o, k * WP : (k + 1) * WP] = (
                    turned[core * half_o : (core + 1) * half_o]
                )

    for k in range(frames * band):
        put_turned(c, k, cot_row(k // band, 1 + k % band))
    for h in (0, band + 1):
        c3[:, :, h] = jnp.zeros((3, 2 * frames, WP, chans), BF16)
    load_w.wait()
    load_gn.wait()
    load_sh.wait()
    partner_cot.wait_recv()
    for k in range(frames * band):
        put_turned(1 - c, k, three_ways(cpart[k // band, k % band]))

    spread(st2, z, st1, (*column(1), *column(0)), 1)

    row_low, row_high = row > 0, row < n_rows - 1
    before = xr.at[0:frames]
    passed_low = remote(before.at[:, 0], before.at[:, 0], ps.at[5], pq.at[5], other)
    passed_high = remote(before.at[:, band + 1], before.at[:, band + 1], ps.at[6], pq.at[6], other)
    body_before = before.at[:, 1 : band + 1]
    passed_body = remote(body_before, body_before, ps.at[4], pq.at[4], other)
    mine_all = xr.at[pl.ds(own, frames)]
    gave_low = remote(mine_all.at[:, 0], mine_all.at[:, 0], ps.at[2], pq.at[2], other)
    gave_high = remote(mine_all.at[:, band + 1], mine_all.at[:, band + 1], ps.at[3], pq.at[3], other)
    for copy, _, gets in x_margins[:2]:
        received(copy, gets)
    started(gave_low, row_low)
    started(gave_high, row_high)

    taps = [(b, s) for b in range(3) for s in range(3)]

    def frame(refs, t):
        rows = [refs[s][t, b : b + band].reshape(band * WP, chans) for b, s in taps]
        return jnp.concatenate(rows, axis=1)

    def back_taps(a):
        return jnp.concatenate([wv[9 * (2 - a) + 3 * (2 - b) + 2 - s] for b, s in taps], axis=1)

    def back(lhs, rhs):
        return lax.dot_general(lhs, rhs, (((1,), (1,)), ((), ())), preferred_element_type=F32)

    half = band * WP
    c3s = [c3.at[s] for s in range(3)]
    both = back(frame(c3s, 1), jnp.concatenate([back_taps(1), back_taps(0)], axis=0))
    ga[0:half] = back(frame(c3s, 0), back_taps(0)) + both[:, :chans]
    ga[half:] = both[:, chans:]

    def cot_corner(h, k):
        landing = cr.at[frames : 2 * frames, h]
        return remote(cr.at[0:frames, h], landing, ps.at[k], pq.at[k], other)

    cot_low, cot_high = cot_corner(0, 7), cot_corner(band + 1, 8)
    for copy, _, gets in cot_margins[:2]:
        received(copy, gets)
    started(cot_low, follow & row_low)
    started(cot_high, follow & row_high)

    received(cot_margins[2][0], cot_margins[2][2])
    has_next = tm < n_tm - 1
    for t in range(frames, 2 * frames):
        for h in range(1, band + 1):
            cot_row(t, h, has_next)
    both = back(frame(c3s, 2), jnp.concatenate([back_taps(2), back_taps(1)], axis=0))
    ga[0:half] += both[:, :chans]
    ga[half:] += back(frame(c3s, 3), back_taps(2)) + both[:, chans:]

    finished(st2, 1)
    stats = summed(st2)
    wide = lambda v: jnp.broadcast_to(v, (8, chans))
    mean = group_total(wide(stats[0:1]), chans // G) / cells
    variance = group_total(wide(stats[1:2]), chans // G) / cells - mean * mean
    inverse = lax.rsqrt(variance + EPSILON)
    gain, shift_ = wide(gain_ref[...]), wide(bias_ref[...])
    mean, inverse, gain, shift_ = (v[0:1] for v in (mean, inverse, gain, shift_))

    swapped_x.wait_recv()
    received(gave_low, row_low)
    received(gave_high, row_high)

    def sigmoid(v):
        return 0.5 + 0.5 * jnp.tanh(0.5 * v)

    def act_frames(low, high, rows=range(band + 2)):
        for t in range(low, high):
            for h in rows:
                v = xr[t, h].astype(F32)
                pre = (v - mean) * inverse * gain + shift_
                act = pre * sigmoid(pre)
                keep = True
                if t < frames:
                    keep = has_before
                if h == 0:
                    keep = keep & row_low
                if h == band + 1:
                    keep = keep & row_high
                if keep is not True:
                    act = jnp.where(keep, act, 0.0)
                a0[t, h] = padded_row(act).astype(BF16)

    chip_frames = frames * nc
    turned = lambda: jnp.concatenate([ct[h, c] for h in range(nc)], axis=1)
    in_first_half = row // dests == 0
    place = lax.rem(row, dests)

    def blocks_of(p):
        low, high = PIECES[p]
        return slice(3 * low, 3 * high)

    def weight_piece(p):
        low, high = PIECES[p]
        rhs = jnp.concatenate(
            [
                a0[a : a + chip_frames, b : b + band].reshape(chip_frames * half, chans)
                for a, b in PAIRS[low:high]
            ],
            axis=1,
        )
        part = jnp.dot(turned(), rhs, preferred_element_type=F32)
        for j in range(high - low):
            for s in range(3):
                block = part[s * half_o : (s + 1) * half_o, j * chans : (j + 1) * chans]
                bsend[:, 3 * (low + j) + s] = block.reshape(dests, own_o, chans).astype(BF16)

    ys = dests // nx
    from_first = lax.rem(y - ys * c + ny, ny)

    def band_dests():
        near_first = (from_first == 0) | (from_first == ny - 1)
        start = jnp.where(near_first, ys - 1, 0)
        for ((dx, _),) in farthest_first([((k, nx),) for k in range(nx)]):
            for j in range(ys):
                yield ys * c + lax.rem(start + j, ys), lax.rem(x + dx, nx), dx != 0

    def send_rows(p):
        blocks = blocks_of(p)

        @pl.when(follow & jnp.logical_not(in_first_half))
        def _():
            brecv[row, blocks] = bsend[place, blocks]

        for ty, tx, is_other in band_dests():
            q = (ty - ys * c) * nx + tx
            device = {"z": z, "c": 1, "y": ty, "x": tx}
            copy = remote(
                bsend.at[q, blocks], brecv.at[row, blocks], bs.at[p], br.at[p], device
            )
            if is_other:
                copy.start()
            else:
                started(copy, lead | (ty != y))

    act_frames(frames, frames + chip_frames, range(band))
    for copy, _, gets in x_margins[2:]:
        received(copy, gets)
    started(passed_body, lead & has_before)
    started(passed_low, lead & has_before & row_low)
    started(passed_high, lead & has_before & row_high)

    weight_piece(0)
    send_rows(0)
    act_frames(frames, frames + chip_frames, range(band, band + 2))
    weight_piece(1)
    send_rows(1)
    received(passed_body, follow & has_before)
    received(passed_low, follow & has_before & row_low)
    received(passed_high, follow & has_before & row_high)
    act_frames(1, 2)

    weight_piece(2)
    send_rows(2)
    act_frames(0, 1)
    weight_piece(3)
    send_rows(3)
    weight_piece(4)
    send_rows(4)
    weight_piece(5)
    send_rows(5)

    for copy, _, gets in cot_margins[3:]:
        received(copy, gets)
    received(cot_low, lead & row_low)
    received(cot_high, lead & row_high)
    for t in range(2 * frames):
        for side, exists in ((0, row_low), (1, row_high)):
            keep = exists & has_next if t >= frames else exists
            sides = three_ways(cr[t, side * (band + 1)], keep)
            for shift in range(3):
                c3e[shift, t, side] = sides[shift].astype(BF16)
    for side, b in ((0, 0), (1, 2)):
        lhs = jnp.concatenate(
            [
                jnp.concatenate(
                    [c3e[s, t + a, side] for a in range(3) for s in range(3)], axis=1
                )
                for t in range(frames)
            ],
            axis=0,
        )
        rhs = jnp.concatenate(
            [wv[9 * (2 - a) + 3 * (2 - b) + 2 - s] for a in range(3) for s in range(3)], axis=1
        )
        edge = back(lhs, rhs)
        for t in range(frames):
            at_t = t * half + side * (band - 1) * WP
            ga[at_t : at_t + WP] += edge[t * WP : (t + 1) * WP]

    def pre_row(k):
        v = xr[own + k // band, 1 + k % band].astype(F32)
        return (v - mean) * inverse

    gains, biases = zero8, zero8
    for k in range(frames * band):
        normed = pre_row(k)
        pre = normed * gain + shift_
        sig = sigmoid(pre)
        at_k = slice(k * WP, k * WP + width)
        grad = ga[at_k] * sig * (1.0 + pre * (1.0 - sig))
        ga[at_k] = grad
        gains = gains + folded(grad * normed)
        biases = biases + folded(grad)
    gs1[tm, 0:1] = gains.sum(axis=0, keepdims=True)
    gs1[tm, 1:2] = biases.sum(axis=0, keepdims=True)
    collect(gs1, tm, column(1), 2)

    def of_piece(buf, count, p, send_sem, recv_sem):
        blocks = blocks_of(p)
        return several(buf.at[:, blocks], count, send_sem.at[p], recv_sem.at[p])

    def send_z(p):
        blocks = blocks_of(p)

        @pl.when(follow)
        def _():
            received(of_piece(brecv, n_rows, p, bs, br), in_first_half)
            received(of_piece(brecv, n_rows - 1, p, bs, br), jnp.logical_not(in_first_half))
            value = brecv[0, blocks].astype(F32)
            for k in range(1, n_rows):
                value = value + brecv[k, blocks].astype(F32)
            crecv[z, blocks] = value.astype(BF16)
            mine = crecv.at[z, blocks]
            for device in column(1):
                remote(mine, mine, zs.at[p], zr.at[p], device).start()

    send_z(0)

    def shift_row(k, carry):
        t, h = k // high_rows, lax.rem(k, high_rows)
        v = a0[frames * c + t, h].astype(F32)
        a3[0, t, h] = pltpu.roll(v, 1, 0).astype(BF16)
        a3[1, t, h] = pltpu.roll(v, WP - 1, 0).astype(BF16)
        return carry

    lax.fori_loop(0, 2 * frames * high_rows, shift_row, 0)
    send_z(1)
    sides = (a3.at[0], a0.at[pl.ds(frames * c, 2 * frames)], a3.at[1])

    def front_taps(a):
        return jnp.concatenate([wv[9 * a + 3 * b + s] for b, s in taps], axis=0)

    def front(lhs, rhs):
        return jnp.dot(lhs, rhs, preferred_element_type=F32)

    one = front(frame(sides, 1), jnp.concatenate([front_taps(1), front_taps(0)], axis=1))
    cv[0:half] = front(frame(sides, 0), front_taps(0)) + one[:, :chans]
    cv[half:] = one[:, chans:]
    send_z(2)
    two = front(frame(sides, 2), jnp.concatenate([front_taps(2), front_taps(1)], axis=1))
    cv[0:half] += two[:, :chans]
    cv[half:] += front(frame(sides, 3), front_taps(2)) + two[:, chans:]
    for k in range(frames * band):
        v = xr[own + k // band, 1 + k % band].astype(F32)
        ofv[k // band, k % band] = (v + cv[k * WP : k * WP + width]).astype(BF16)
    send_z(3)

    send_z(4)
    spread(gs2, row, gs1, (*plane(1), *plane(0)), 3)
    send_z(5)

    finished(gs2, 3)
    sums = summed(gs2)
    gain_grad, bias_grad = wide(sums[0:1]), wide(sums[1:2])
    gv[...] = sums[0:1]
    bv[...] = sums[1:2]
    mean_dn = (group_total(gain * bias_grad, chans // G) / cells)[0:1]
    mean_dnn = (group_total(gain * gain_grad, chans // G) / cells)[0:1]
    for k in range(frames * band):
        t, h = k // band, k % band
        normed = pre_row(k)
        grad = ga[k * WP : k * WP + width]
        cot = cr[t, 1 + h].astype(F32)
        igv[t, h] = (inverse * (grad * gain - mean_dn - normed * mean_dnn) + cot).astype(BF16)

    to_core = []
    for p in range(N_PIECES):
        blocks = blocks_of(p)
        mine = fin.at[blocks]
        copy = remote(mine, mine, fs.at[p], fr.at[p], other)
        to_core.append(copy)

        @pl.when(follow)
        def _():
            of_piece(crecv, nz - 1, p, zs, zr).wait_recv()
            value = crecv[0, blocks].astype(F32)
            for k in range(1, nz):
                value = value + crecv[k, blocks].astype(F32)
            fin[blocks] = value
            copy.start()

    scale = 1.0 / math.sqrt(all_pixels)
    for p in range(N_PIECES):
        blocks = blocks_of(p)
        received(to_core[p], lead)
        for m in range(blocks.start, blocks.stop):
            a, b = PAIRS[m // 3]
            at_m = (9 * a + 3 * b + m % 3) * chans
            wgv[:, at_m : at_m + chans] = fin[m] * scale

    def parts_left(count, k, sends):
        left(several(st1, count, st_s.at[k], st_r.at[k]), sends)

    for k, chips in ((0, n_rows), (2, nz)):
        parts_left(chips, k, lead)
        parts_left(chips - 1, k, follow)
    parts_left(2 * nz - 1, 1, follow)
    parts_left(2 * n_rows - 1, 3, follow)
    partner_cot.wait_send()
    swapped_x.wait_send()
    for copy, sends, _ in (*cot_margins, *x_margins):
        left(copy, sends)
    left(gave_low, row_low)
    left(gave_high, row_high)
    left(cot_low, follow & row_low)
    left(cot_high, follow & row_high)
    left(passed_body, lead & has_before)
    left(passed_low, lead & has_before & row_low)
    left(passed_high, lead & has_before & row_high)

    own_half = follow & jnp.logical_not(in_first_half)
    for p in range(N_PIECES):
        left(of_piece(bsend, dests - 1, p, bs, br), own_half)
        left(of_piece(bsend, dests, p, bs, br), jnp.logical_not(own_half))
        left(of_piece(crecv, nz - 1, p, zs, zr), follow)
        left(to_core[p], follow)


def put_out(*refs):
    sources, places, sem = refs[:5], refs[5:10], refs[10]
    copies = [pltpu.make_async_copy(s, d, sem.at[k]) for k, (s, d) in enumerate(zip(sources, places))]
    for copy in copies:
        copy.start()
    for copy in copies:
        copy.wait()


def per_device(sizes, frames_in, norm_gain, norm_bias, conv_weight, cotangent):
    nz, nc, ny, nx = sizes
    n_tm, n_rows = nz * nc, ny * nx
    frames, band, width, chans = frames_in.shape
    own_o, dests = chans // n_rows, n_rows // nc
    rows = (2 * frames, band + 2)
    chip = (frames + frames * nc, band + 2)
    vmem, dma = pltpu.VMEM, pltpu.SemaphoreType.DMA
    scratch = [
        vmem((1, chans), F32),
        vmem((1, chans), F32),
        vmem((*chip, width, chans), BF16),
        vmem((*rows, width, chans), BF16),
        vmem((frames, band, width, chans), BF16),
        vmem((27, chans, chans), BF16),
        vmem((*chip, WP, chans), BF16),
        vmem((2, *rows, WP, chans), BF16),
        vmem((3, *rows, WP, chans), BF16),
        vmem((3, 2 * frames, 2, WP, chans), BF16),
        vmem((nc, nc, 3 * chans // nc, frames * band * WP), BF16),
        vmem((frames * band * WP, chans), F32),
        vmem((frames * band * WP, chans), F32),
        vmem((dests, 27, own_o, chans), BF16),
        vmem((n_rows, 27, own_o, chans), BF16),
        vmem((nz, 27, own_o, chans), BF16),
        vmem((27, own_o, chans), F32),
        vmem((n_rows * nc, 2, chans), F32),
        vmem((nz, 2, chans), F32),
        vmem((n_tm, 2, chans), F32),
        vmem((n_rows, 2, chans), F32),
        dma((5,)),
        dma((5,)), dma((5,)), dma((5,)), dma((5,)), dma((9,)), dma((9,)), dma((4,)), dma((4,)),
        dma((N_PIECES,)), dma((N_PIECES,)), dma((N_PIECES,)), dma((N_PIECES,)),
        dma((N_PIECES,)), dma((N_PIECES,)),
    ]
    anywhere = pl.BlockSpec(memory_space=pl.ANY)
    stays = pl.BlockSpec(memory_space=pltpu.HBM)
    inside = pl.BlockSpec(memory_space=pltpu.VMEM)
    out = jax.ShapeDtypeStruct
    operands = (
        frames_in,
        norm_gain.reshape(1, chans),
        norm_bias.reshape(1, chans),
        conv_weight.reshape(27, chans, chans),
        cotangent,
    )
    made = pl.pallas_call(
        functools.partial(kernel, sizes),
        out_shape=(
            out(frames_in.shape, BF16),
            out(frames_in.shape, BF16),
            out((own_o, 27 * chans), F32),
            out((1, chans), F32),
            out((1, chans), F32),
        ),
        in_specs=[stays] * 5,
        out_specs=[inside] * 5,
        scratch_shapes=scratch,
        compiler_params=pltpu.CompilerParams(
            collective_id=0, has_side_effects=True, vmem_limit_bytes=48 << 20
        ),
        name="block",
    )(*(pltpu.with_memory_space_constraint(a, pltpu.HBM) for a in operands))
    of, ig, wg, gg, bg = pl.pallas_call(
        put_out,
        out_shape=[out(a.shape, a.dtype) for a in made],
        in_specs=[anywhere] * 5,
        out_specs=[stays] * 5,
        scratch_shapes=[dma((5,))],
        compiler_params=pltpu.CompilerParams(vmem_limit_bytes=1 << 20),
        name="put_out",
    )(*made)
    return of, ig, wg, gg.reshape(chans), bg.reshape(chans)


def program(devices):
    torus = Mesh(devices, ("z", "c", "y", "x"))
    placed = (P(TM, ROWS, None, None), P(), P(), P(), P(TM, ROWS, None, None))
    return jax.shard_map(
        functools.partial(per_device, devices.shape),
        mesh=torus,
        in_specs=placed,
        out_specs=(P(TM, ROWS, None, None), P(TM, ROWS, None, None), P(ROWS, None), P(), P()),
        check_vma=False,
    )


def solution(mesh):
    return program(mesh.devices.reshape(8, 2, 4, 4))
```

```python
import functools
import math

import jax
import jax.numpy as jnp
from jax import lax
from jax.experimental import pallas as pl
from jax.experimental.pallas import tpu as pltpu
from jax.sharding import Mesh
from jax.sharding import PartitionSpec as P

G = 32
EPSILON = 1e-06
TM = ("z", "c")
ROWS = ("y", "x")
MESH = pl.DeviceIdType.MESH
WP = 128
F32 = jnp.float32
BF16 = jnp.bfloat16
PAIRS = tuple((a, b) for a in (2, 1, 0) for b in range(3))
PIECES = ((0, 1), (1, 3), (3, 5), (5, 7), (7, 8), (8, 9))
N_PIECES = len(PIECES)


def group_total(per_channel, size):
    lanes = lax.broadcasted_iota(jnp.int32, per_channel.shape, 1)
    within = lanes % size
    channels = per_channel.shape[1]
    total = per_channel
    for step in range(1, size):
        ahead = pltpu.roll(per_channel, channels - step, 1)
        behind = pltpu.roll(per_channel, step, 1)
        total = total + jnp.where(within + step < size, ahead, 0.0)
        total = total + jnp.where(within >= step, behind, 0.0)
    return total


def kernel(
    sizes, x_hbm, gn_hbm, sh_hbm, w_hbm, cot_hbm,
    ofv, igv, wgv, gv, bv,
    gain_ref, bias_ref, xr, cr, cpart, wv, a0, a3, c3, ct, ga, cv, bsend, brecv, crecv, fin,
    st1, st2, gs1, gs2,
    load_sem, xs, xq, cs, cq, ps, pq, st_s, st_r, bs, br, zs, zr, fs, fr,
):
    nz, nc, ny, nx = sizes
    n_tm, n_rows = nz * nc, ny * nx
    frames, band, width, chans = x_hbm.shape
    high_rows = band + 2
    own_o = chans // n_rows
    dests = n_rows // nc
    half_o = chans // nc
    all_pixels = frames * n_tm * band * n_rows * width
    cells = all_pixels * (chans // G)
    z, c = lax.axis_index("z"), lax.axis_index("c")
    y, x = lax.axis_index("y"), lax.axis_index("x")
    tm, row = z * nc + c, y * nx + x
    own = frames + frames * c
    other = {"z": z, "c": 1 - c, "y": y, "x": x}
    lead, follow = c == 0, c == 1
    has_before = z > 0

    def at(t, r):
        t, r = lax.rem(t + n_tm, n_tm), lax.rem(r + n_rows, n_rows)
        return {"z": t // nc, "c": lax.rem(t, nc), "y": r // nx, "x": lax.rem(r, nx)}

    def farthest_first(steps):
        return sorted(steps, key=lambda pairs: -sum(min(d, n - d) for d, n in pairs))

    def plane(core):
        steps = [((k // nx, ny), (k % nx, nx)) for k in range(1, n_rows)]
        for (dy, _), (dx, _) in farthest_first(steps):
            yield {"z": z, "c": core, "y": lax.rem(y + dy, ny), "x": lax.rem(x + dx, nx)}

    def column(core):
        for ((dz, _),) in farthest_first([((k, nz),) for k in range(1, nz)]):
            yield {"z": lax.rem(z + dz, nz), "c": core, "y": y, "x": x}

    def remote(src, dst, send_sem, recv_sem, device):
        return pltpu.make_async_remote_copy(
            src_ref=src, dst_ref=dst, send_sem=send_sem, recv_sem=recv_sem,
            device_id=device, device_id_type=MESH,
        )

    def several(slots, count, send_sem, recv_sem):
        some = slots.at[0:count]
        return remote(some, some, send_sem, recv_sem, other)

    def started(copy, sends):
        @pl.when(sends)
        def _():
            copy.start()

    def received(copy, gets):
        @pl.when(gets)
        def _():
            copy.wait_recv()

    def left(copy, sends):
        @pl.when(sends)
        def _():
            copy.wait_send()

    load_x = pltpu.make_async_copy(
        x_hbm, xr.at[pl.ds(own, frames), 1 : band + 1], load_sem.at[0]
    )
    load_c = pltpu.make_async_copy(cot_hbm, cr.at[0:frames, 1 : band + 1], load_sem.at[1])
    load_w = pltpu.make_async_copy(w_hbm, wv, load_sem.at[2])
    load_gn = pltpu.make_async_copy(gn_hbm, gain_ref, load_sem.at[3])
    load_sh = pltpu.make_async_copy(sh_hbm, bias_ref, load_sem.at[4])
    for copy in (load_x, load_c, load_w, load_gn, load_sh):
        copy.start()

    barrier = pltpu.get_barrier_semaphore()
    def enter(devices):
        for device in devices:
            pl.semaphore_signal(barrier, inc=1, device_id=device, device_id_type=MESH)

    corners = [at(tm + dt, row + dw) for dt in (-1, 1) for dw in (-1, 1)]
    enter((*column(1), *plane(1), other, *corners))

    @pl.when(follow)
    def _():
        enter((*column(0), *plane(0)))

    @pl.when(lead)
    def _():
        enter((at(tm, row + 1), at(tm, row - 1)))

    chips = n_rows - 1 + nz - 1
    partners = jnp.where(follow, 2 * chips + 5, chips + 7)

    load_x.wait()

    def folded(v):
        return v.reshape(width // 8, 8, chans).sum(axis=0)

    def stat_row(k, carry):
        total, square = carry
        v = xr[own + k // band, 1 + lax.rem(k, band)].astype(F32)
        return total + folded(v), square + folded(v * v)

    zero8 = jnp.zeros((8, chans), F32)
    total, square = lax.fori_loop(0, frames * band, stat_row, (zero8, zero8))
    st1[nc * row + c, 0:1] = total.sum(axis=0, keepdims=True)
    st1[nc * row + c, 1:2] = square.sum(axis=0, keepdims=True)

    pl.semaphore_wait(barrier, partners)

    def summed(slots):
        total = slots[0]
        for k in range(1, slots.shape[0]):
            total = total + slots[k]
        return total

    def collect(slots, mine, peers, k):
        part = slots.at[mine]
        for device in peers:
            remote(part, part, st_s.at[k], st_r.at[k], device).start()
        started(remote(part, part, st_s.at[k], st_r.at[k], other), lead)

    def spread(slots, mine, collected, peers, k):
        @pl.when(follow)
        def _():
            several(collected, collected.shape[0] - 1, st_s.at[k - 1], st_r.at[k - 1]).wait_recv()
            slots[mine] = summed(collected)
            part = slots.at[mine]
            for device in (*peers, other):
                remote(part, part, st_s.at[k], st_r.at[k], device).start()

    def finished(slots, k):
        received(several(slots, slots.shape[0] - 1, st_s.at[k], st_r.at[k]), follow)
        received(several(slots, slots.shape[0], st_s.at[k], st_r.at[k]), lead)

    collect(st1, nc * row + c, plane(1), 0)

    def margins(buf, first, there, way, body_from, corners_from, send_sem, recv_sem):
        mine = buf.at[pl.ds(first, frames)]
        moved = buf.at[pl.ds(there, frames)]
        up_t = (tm + way >= 0) & (tm + way < n_tm)
        from_t = (tm - way >= 0) & (tm - way < n_tm)
        up_c, from_c = up_t & (c == corners_from), from_t & (c != corners_from)
        if body_from is not None:
            up_t, from_t = up_t & (c == body_from), from_t & (c != body_from)
        up_r, down_r = row < n_rows - 1, row > 0
        low, high, body = mine.at[:, 1], mine.at[:, band], slice(1, band + 1)
        plan = [
            (high, mine.at[:, 0], at(tm, row + 1), up_r, down_r),
            (low, mine.at[:, band + 1], at(tm, row - 1), down_r, up_r),
            (mine.at[:, body], moved.at[:, body], at(tm + way, row), up_t, from_t),
            (high, moved.at[:, 0], at(tm + way, row + 1), up_c & up_r, from_c & down_r),
            (low, moved.at[:, band + 1], at(tm + way, row - 1), up_c & down_r, from_c & up_r),
        ]
        return [
            (remote(src, dst, send_sem.at[k], recv_sem.at[k], device), sends, gets)
            for k, (src, dst, device, sends, gets) in enumerate(plan)
        ]

    load_c.wait()
    cot_margins = margins(cr, 0, frames, -1, None, 0, cs, cq)
    x_margins = margins(xr, own, 0, 1, 1, 1, xs, xq)
    partner_cot = remote(cr.at[0:frames, 1 : band + 1], cpart, ps.at[0], pq.at[0], other)
    mine_x = xr.at[pl.ds(own, frames), 1 : band + 1]
    swapped_x = remote(mine_x, mine_x, ps.at[1], pq.at[1], other)

    partner_cot.start()
    swapped_x.start()
    for copy, sends, _ in (*x_margins[:3], *cot_margins, *x_margins[3:]):
        started(copy, sends)

    zeros_pad = jnp.zeros((WP - width, chans), F32)

    def padded_row(v):
        return jnp.concatenate([v, zeros_pad], axis=0)

    def three_ways(v, keep=True):
        v = padded_row(v.astype(F32))
        if keep is not True:
            v = jnp.where(keep, v, 0.0)
        return pltpu.roll(v, 1, 0), v, pltpu.roll(v, WP - 1, 0)

    def cot_row(t, h, keep=True):
        sides = three_ways(cr[t, h], keep)
        for shift in range(3):
            c3[shift, t, h] = sides[shift].astype(BF16)
        return sides

    def put_turned(chip_half, k, sides):
        for shift in range(3):
            turned = sides[2 - shift].T.astype(BF16)
            for core in range(nc):
                ct[chip_half, core, shift * half_o : (shift + 1) * half_o, k * WP : (k + 1) * WP] = (
                    turned[core * half_o : (core + 1) * half_o]
                )

    for k in range(frames * band):
        put_turned(c, k, cot_row(k // band, 1 + k % band))
    for h in (0, band + 1):
        c3[:, :, h] = jnp.zeros((3, 2 * frames, WP, chans), BF16)
    load_w.wait()
    load_gn.wait()
    load_sh.wait()
    partner_cot.wait_recv()
    for k in range(frames * band):
        put_turned(1 - c, k, three_ways(cpart[k // band, k % band]))

    spread(st2, z, st1, (*column(1), *column(0)), 1)

    row_low, row_high = row > 0, row < n_rows - 1
    before = xr.at[0:frames]
    passed_low = remote(before.at[:, 0], before.at[:, 0], ps.at[5], pq.at[5], other)
    passed_high = remote(before.at[:, band + 1], before.at[:, band + 1], ps.at[6], pq.at[6], other)
    body_before = before.at[:, 1 : band + 1]
    passed_body = remote(body_before, body_before, ps.at[4], pq.at[4], other)
    mine_all = xr.at[pl.ds(own, frames)]
    gave_low = remote(mine_all.at[:, 0], mine_all.at[:, 0], ps.at[2], pq.at[2], other)
    gave_high = remote(mine_all.at[:, band + 1], mine_all.at[:, band + 1], ps.at[3], pq.at[3], other)
    for copy, _, gets in x_margins[:2]:
        received(copy, gets)
    started(gave_low, row_low)
    started(gave_high, row_high)

    taps = [(b, s) for b in range(3) for s in range(3)]

    def frame(refs, t):
        rows = [refs[s][t, b : b + band].reshape(band * WP, chans) for b, s in taps]
        return jnp.concatenate(rows, axis=1)

    def back_taps(a):
        return jnp.concatenate([wv[9 * (2 - a) + 3 * (2 - b) + 2 - s] for b, s in taps], axis=1)

    def back(lhs, rhs):
        return lax.dot_general(lhs, rhs, (((1,), (1,)), ((), ())), preferred_element_type=F32)

    half = band * WP
    c3s = [c3.at[s] for s in range(3)]
    both = back(frame(c3s, 1), jnp.concatenate([back_taps(1), back_taps(0)], axis=0))
    ga[0:half] = back(frame(c3s, 0), back_taps(0)) + both[:, :chans]
    ga[half:] = both[:, chans:]

    def cot_corner(h, k):
        landing = cr.at[frames : 2 * frames, h]
        return remote(cr.at[0:frames, h], landing, ps.at[k], pq.at[k], other)

    cot_low, cot_high = cot_corner(0, 5), cot_corner(band + 1, 6)
    for copy, _, gets in cot_margins[:2]:
        received(copy, gets)
    started(cot_low, follow & row_low)
    started(cot_high, follow & row_high)

    received(cot_margins[2][0], cot_margins[2][2])
    has_next = tm < n_tm - 1
    for t in range(frames, 2 * frames):
        for h in range(1, band + 1):
            cot_row(t, h, has_next)
    both = back(frame(c3s, 2), jnp.concatenate([back_taps(2), back_taps(1)], axis=0))
    ga[0:half] += both[:, :chans]
    ga[half:] += back(frame(c3s, 3), back_taps(2)) + both[:, chans:]

    def edge(t_in):
        keep = has_next if t_in >= frames else True
        for side, b, exists in ((0, 0, row_low), (1, 2, row_high)):
            sides = three_ways(cr[t_in, side * (band + 1)], exists & keep)
            lhs = jnp.concatenate([v.astype(BF16) for v in sides], axis=1)
            gets = [(t, t_in - t) for t in range(frames) if 0 <= t_in - t < 3]
            rhs = jnp.concatenate(
                [
                    jnp.concatenate(
                        [wv[9 * (2 - a) + 3 * (2 - b) + 2 - s] for s in range(3)], axis=1
                    )
                    for _, a in gets
                ],
                axis=0,
            )
            given = back(lhs, rhs)
            for j, (t, _) in enumerate(gets):
                at_t = t * half + side * (band - 1) * WP
                ga[at_t : at_t + WP] += given[:, j * chans : (j + 1) * chans]

    for t in range(frames):
        edge(t)

    finished(st2, 1)
    stats = summed(st2)
    wide = lambda v: jnp.broadcast_to(v, (8, chans))
    mean = group_total(wide(stats[0:1]), chans // G) / cells
    variance = group_total(wide(stats[1:2]), chans // G) / cells - mean * mean
    inverse = lax.rsqrt(variance + EPSILON)
    gain, shift_ = wide(gain_ref[...]), wide(bias_ref[...])
    mean, inverse, gain, shift_ = (v[0:1] for v in (mean, inverse, gain, shift_))

    swapped_x.wait_recv()
    received(gave_low, row_low)
    received(gave_high, row_high)

    for copy, _, gets in x_margins[2:]:
        received(copy, gets)
    started(passed_body, lead & has_before)
    started(passed_low, lead & has_before & row_low)
    started(passed_high, lead & has_before & row_high)


    def sigmoid(v):
        return 0.5 + 0.5 * jnp.tanh(0.5 * v)

    def act_frames(low, high, rows=range(band + 2)):
        for t in range(low, high):
            for h in rows:
                v = xr[t, h].astype(F32)
                pre = (v - mean) * inverse * gain + shift_
                act = pre * sigmoid(pre)
                keep = True
                if t < frames:
                    keep = has_before
                if h == 0:
                    keep = keep & row_low
                if h == band + 1:
                    keep = keep & row_high
                if keep is not True:
                    act = jnp.where(keep, act, 0.0)
                a0[t, h] = padded_row(act).astype(BF16)

    chip_frames = frames * nc
    turned = lambda: jnp.concatenate([ct[h, c] for h in range(nc)], axis=1)
    in_first_half = row // dests == 0
    place = lax.rem(row, dests)

    def blocks_of(p):
        low, high = PIECES[p]
        return slice(3 * low, 3 * high)

    def weight_piece(p):
        low, high = PIECES[p]
        rhs = jnp.concatenate(
            [
                a0[a : a + chip_frames, b : b + band].reshape(chip_frames * half, chans)
                for a, b in PAIRS[low:high]
            ],
            axis=1,
        )
        part = jnp.dot(turned(), rhs, preferred_element_type=F32)
        for j in range(high - low):
            for s in range(3):
                block = part[s * half_o : (s + 1) * half_o, j * chans : (j + 1) * chans]
                bsend[:, 3 * (low + j) + s] = block.reshape(dests, own_o, chans).astype(BF16)

    ys = dests // nx
    from_first = lax.rem(y - ys * c + ny, ny)

    def band_dests():
        near_first = (from_first == 0) | (from_first == ny - 1)
        start = jnp.where(near_first, ys - 1, 0)
        for ((dx, _),) in farthest_first([((k, nx),) for k in range(nx)]):
            for j in range(ys):
                yield ys * c + lax.rem(start + j, ys), lax.rem(x + dx, nx), dx != 0

    def send_rows(p):
        blocks = blocks_of(p)

        @pl.when(follow & jnp.logical_not(in_first_half))
        def _():
            brecv[row, blocks] = bsend[place, blocks]

        for ty, tx, is_other in band_dests():
            q = (ty - ys * c) * nx + tx
            device = {"z": z, "c": 1, "y": ty, "x": tx}
            copy = remote(
                bsend.at[q, blocks], brecv.at[row, blocks], bs.at[0], br.at[p], device
            )
            if is_other:
                copy.start()
            else:
                started(copy, lead | (ty != y))

    act_frames(frames, frames + chip_frames, range(band))
    weight_piece(0)
    send_rows(0)
    act_frames(frames, frames + chip_frames, range(band, band + 2))
    weight_piece(1)
    send_rows(1)
    received(passed_body, follow & has_before)
    received(passed_low, follow & has_before & row_low)
    received(passed_high, follow & has_before & row_high)
    act_frames(1, 2)

    weight_piece(2)
    send_rows(2)
    act_frames(0, 1)
    weight_piece(3)
    send_rows(3)
    for copy, _, gets in cot_margins[3:]:
        received(copy, gets)
    received(cot_low, lead & row_low)
    received(cot_high, lead & row_high)
    for t in range(frames, 2 * frames):
        edge(t)

    def pre_row(k):
        v = xr[own + k // band, 1 + k % band].astype(F32)
        return (v - mean) * inverse

    gains, biases = zero8, zero8
    for k in range(frames * band):
        normed = pre_row(k)
        pre = normed * gain + shift_
        sig = sigmoid(pre)
        at_k = slice(k * WP, k * WP + width)
        grad = ga[at_k] * sig * (1.0 + pre * (1.0 - sig))
        ga[at_k] = grad
        gains = gains + folded(grad * normed)
        biases = biases + folded(grad)
    gs1[tm, 0:1] = gains.sum(axis=0, keepdims=True)
    gs1[tm, 1:2] = biases.sum(axis=0, keepdims=True)
    collect(gs1, tm, column(1), 2)

    weight_piece(4)
    send_rows(4)
    weight_piece(5)
    send_rows(5)

    def of_piece(buf, count, p, recv_sem):
        return several(buf.at[:, blocks_of(p)], count, bs.at[0], recv_sem.at[p])

    def send_z(p):
        blocks = blocks_of(p)

        @pl.when(follow)
        def _():
            received(of_piece(brecv, n_rows, p, br), in_first_half)
            received(of_piece(brecv, n_rows - 1, p, br), jnp.logical_not(in_first_half))
            value = brecv[0, blocks].astype(F32)
            for k in range(1, n_rows):
                value = value + brecv[k, blocks].astype(F32)
            crecv[z, blocks] = value.astype(BF16)
            mine = crecv.at[z, blocks]
            for device in column(1):
                remote(mine, mine, zs.at[0], zr.at[p], device).start()

    send_z(0)

    def shift_row(k, carry):
        t, h = k // high_rows, lax.rem(k, high_rows)
        v = a0[frames * c + t, h].astype(F32)
        a3[0, t, h] = pltpu.roll(v, 1, 0).astype(BF16)
        a3[1, t, h] = pltpu.roll(v, WP - 1, 0).astype(BF16)
        return carry

    lax.fori_loop(0, 2 * frames * high_rows, shift_row, 0)
    send_z(1)
    sides = (a3.at[0], a0.at[pl.ds(frames * c, 2 * frames)], a3.at[1])

    def front_taps(a):
        return jnp.concatenate([wv[9 * a + 3 * b + s] for b, s in taps], axis=0)

    def front(lhs, rhs):
        return jnp.dot(lhs, rhs, preferred_element_type=F32)

    one = front(frame(sides, 1), jnp.concatenate([front_taps(1), front_taps(0)], axis=1))
    cv[0:half] = front(frame(sides, 0), front_taps(0)) + one[:, :chans]
    cv[half:] = one[:, chans:]
    send_z(2)
    two = front(frame(sides, 2), jnp.concatenate([front_taps(2), front_taps(1)], axis=1))
    cv[0:half] += two[:, :chans]
    cv[half:] += front(frame(sides, 3), front_taps(2)) + two[:, chans:]
    for k in range(frames * band):
        v = xr[own + k // band, 1 + k % band].astype(F32)
        ofv[k // band, k % band] = (v + cv[k * WP : k * WP + width]).astype(BF16)
    spread(gs2, row, gs1, (*plane(1), *plane(0)), 3)
    send_z(3)

    send_z(4)
    send_z(5)

    finished(gs2, 3)
    sums = summed(gs2)
    gain_grad, bias_grad = wide(sums[0:1]), wide(sums[1:2])
    gv[...] = sums[0:1]
    bv[...] = sums[1:2]
    mean_dn = (group_total(gain * bias_grad, chans // G) / cells)[0:1]
    mean_dnn = (group_total(gain * gain_grad, chans // G) / cells)[0:1]
    for k in range(frames * band):
        t, h = k // band, k % band
        normed = pre_row(k)
        grad = ga[k * WP : k * WP + width]
        cot = cr[t, 1 + h].astype(F32)
        igv[t, h] = (inverse * (grad * gain - mean_dn - normed * mean_dnn) + cot).astype(BF16)

    for p in range(N_PIECES):
        blocks = blocks_of(p)

        @pl.when(follow)
        def _():
            of_piece(crecv, nz - 1, p, zr).wait_recv()
            value = crecv[0, blocks].astype(F32)
            for k in range(1, nz):
                value = value + crecv[k, blocks].astype(F32)
            fin[blocks] = value
            remote(fin.at[blocks], fin.at[blocks], fs.at[0], fr.at[0], other).start()

    whole = remote(fin, fin, fs.at[0], fr.at[0], other)
    received(whole, lead)
    scale = 1.0 / math.sqrt(all_pixels)
    for m in range(27):
        a, b = PAIRS[m // 3]
        at_m = (9 * a + 3 * b + m % 3) * chans
        wgv[:, at_m : at_m + chans] = fin[m] * scale

    def parts_left(count, k, sends):
        left(several(st1, count, st_s.at[k], st_r.at[k]), sends)

    for k, chips in ((0, n_rows), (2, nz)):
        parts_left(chips, k, lead)
        parts_left(chips - 1, k, follow)
    parts_left(2 * nz - 1, 1, follow)
    parts_left(2 * n_rows - 1, 3, follow)
    partner_cot.wait_send()
    swapped_x.wait_send()
    for copy, sends, _ in (*cot_margins, *x_margins):
        left(copy, sends)
    left(gave_low, row_low)
    left(gave_high, row_high)
    left(cot_low, follow & row_low)
    left(cot_high, follow & row_high)
    left(passed_body, lead & has_before)
    left(passed_low, lead & has_before & row_low)
    left(passed_high, lead & has_before & row_high)

    own_half = follow & jnp.logical_not(in_first_half)
    left(several(bsend, dests - 1, bs.at[0], br.at[0]), own_half)
    left(several(bsend, dests, bs.at[0], br.at[0]), jnp.logical_not(own_half))
    left(several(crecv, nz - 1, zs.at[0], zr.at[0]), follow)
    left(whole, follow)


def put_out(*refs):
    sources, places, sem = refs[:5], refs[5:10], refs[10]
    copies = [pltpu.make_async_copy(s, d, sem.at[k]) for k, (s, d) in enumerate(zip(sources, places))]
    for copy in copies:
        copy.start()
    for copy in copies:
        copy.wait()


def per_device(sizes, frames_in, norm_gain, norm_bias, conv_weight, cotangent):
    nz, nc, ny, nx = sizes
    n_tm, n_rows = nz * nc, ny * nx
    frames, band, width, chans = frames_in.shape
    own_o, dests = chans // n_rows, n_rows // nc
    rows = (2 * frames, band + 2)
    chip = (frames + frames * nc, band + 2)
    vmem, dma = pltpu.VMEM, pltpu.SemaphoreType.DMA
    scratch = [
        vmem((1, chans), F32),
        vmem((1, chans), F32),
        vmem((*chip, width, chans), BF16),
        vmem((*rows, width, chans), BF16),
        vmem((frames, band, width, chans), BF16),
        vmem((27, chans, chans), BF16),
        vmem((*chip, WP, chans), BF16),
        vmem((2, *rows, WP, chans), BF16),
        vmem((3, *rows, WP, chans), BF16),
        vmem((nc, nc, 3 * chans // nc, frames * band * WP), BF16),
        vmem((frames * band * WP, chans), F32),
        vmem((frames * band * WP, chans), F32),
        vmem((dests, 27, own_o, chans), BF16),
        vmem((n_rows, 27, own_o, chans), BF16),
        vmem((nz, 27, own_o, chans), BF16),
        vmem((27, own_o, chans), F32),
        vmem((n_rows * nc, 2, chans), F32),
        vmem((nz, 2, chans), F32),
        vmem((n_tm, 2, chans), F32),
        vmem((n_rows, 2, chans), F32),
        dma((5,)),
        dma((5,)), dma((5,)), dma((5,)), dma((5,)), dma((7,)), dma((7,)), dma((4,)), dma((4,)),
        dma((1,)), dma((N_PIECES,)), dma((1,)), dma((N_PIECES,)), dma((1,)), dma((1,)),
    ]
    anywhere = pl.BlockSpec(memory_space=pl.ANY)
    stays = pl.BlockSpec(memory_space=pltpu.HBM)
    inside = pl.BlockSpec(memory_space=pltpu.VMEM)
    out = jax.ShapeDtypeStruct
    operands = (
        frames_in,
        norm_gain.reshape(1, chans),
        norm_bias.reshape(1, chans),
        conv_weight.reshape(27, chans, chans),
        cotangent,
    )
    made = pl.pallas_call(
        functools.partial(kernel, sizes),
        out_shape=(
            out(frames_in.shape, BF16),
            out(frames_in.shape, BF16),
            out((own_o, 27 * chans), F32),
            out((1, chans), F32),
            out((1, chans), F32),
        ),
        in_specs=[stays] * 5,
        out_specs=[inside] * 5,
        scratch_shapes=scratch,
        compiler_params=pltpu.CompilerParams(
            collective_id=0, has_side_effects=True, vmem_limit_bytes=48 << 20
        ),
        name="block",
    )(*(pltpu.with_memory_space_constraint(a, pltpu.HBM) for a in operands))
    of, ig, wg, gg, bg = pl.pallas_call(
        put_out,
        out_shape=[out(a.shape, a.dtype) for a in made],
        in_specs=[anywhere] * 5,
        out_specs=[stays] * 5,
        scratch_shapes=[dma((5,))],
        compiler_params=pltpu.CompilerParams(vmem_limit_bytes=1 << 20),
        name="put_out",
    )(*made)
    return of, ig, wg, gg.reshape(chans), bg.reshape(chans)


def program(devices):
    torus = Mesh(devices, ("z", "c", "y", "x"))
    placed = (P(TM, ROWS, None, None), P(), P(), P(), P(TM, ROWS, None, None))
    return jax.shard_map(
        functools.partial(per_device, devices.shape),
        mesh=torus,
        in_specs=placed,
        out_specs=(P(TM, ROWS, None, None), P(TM, ROWS, None, None), P(ROWS, None), P(), P()),
        check_vma=False,
    )


def solution(mesh):
    return program(mesh.devices.reshape(8, 2, 4, 4))
```

```python
import functools
import math

import jax
import jax.numpy as jnp
from jax import lax
from jax.experimental import pallas as pl
from jax.experimental.pallas import tpu as pltpu
from jax.sharding import Mesh
from jax.sharding import PartitionSpec as P

G = 32
EPSILON = 1e-06
TM = ("z", "c")
ROWS = ("y", "x")
MESH = pl.DeviceIdType.MESH
WP = 128
F32 = jnp.float32
BF16 = jnp.bfloat16
PAIRS = tuple((a, b) for a in (2, 1, 0) for b in range(3))
PIECES = ((0, 1), (1, 3), (3, 5), (5, 7), (7, 9))
N_PIECES = len(PIECES)


def group_total(per_channel, size):
    lanes = lax.broadcasted_iota(jnp.int32, per_channel.shape, 1)
    within = lanes % size
    channels = per_channel.shape[1]
    total = per_channel
    for step in range(1, size):
        ahead = pltpu.roll(per_channel, channels - step, 1)
        behind = pltpu.roll(per_channel, step, 1)
        total = total + jnp.where(within + step < size, ahead, 0.0)
        total = total + jnp.where(within >= step, behind, 0.0)
    return total


def kernel(
    sizes, x_hbm, gn_hbm, sh_hbm, w_hbm, cot_hbm,
    ofv, igv, wgv, gv, bv,
    gain_ref, bias_ref, xr, cr, cpart, wv, a0, a3, c3, ct, ga, cv, bsend, brecv, crecv, fin,
    st1, st2, gs1, gs2,
    load_sem, xs, xq, cs, cq, corner_s, corner_r, ps, pq, st_s, st_r, bs, br, zs, zr, fs, fr,
):
    nz, nc, ny, nx = sizes
    n_tm, n_rows = nz * nc, ny * nx
    frames, band, width, chans = x_hbm.shape
    high_rows = band + 2
    own_o = chans // n_rows
    dests = n_rows // nc
    half_o = chans // nc
    all_pixels = frames * n_tm * band * n_rows * width
    cells = all_pixels * (chans // G)
    z, c = lax.axis_index("z"), lax.axis_index("c")
    y, x = lax.axis_index("y"), lax.axis_index("x")
    tm, row = z * nc + c, y * nx + x
    own = frames + frames * c
    other = {"z": z, "c": 1 - c, "y": y, "x": x}
    lead, follow = c == 0, c == 1
    has_before = z > 0

    def at(t, r):
        t, r = lax.rem(t + n_tm, n_tm), lax.rem(r + n_rows, n_rows)
        return {"z": t // nc, "c": lax.rem(t, nc), "y": r // nx, "x": lax.rem(r, nx)}

    def farthest_first(steps):
        return sorted(steps, key=lambda pairs: -sum(min(d, n - d) for d, n in pairs))

    def plane(core):
        steps = [((k // nx, ny), (k % nx, nx)) for k in range(1, n_rows)]
        for (dy, _), (dx, _) in farthest_first(steps):
            yield {"z": z, "c": core, "y": lax.rem(y + dy, ny), "x": lax.rem(x + dx, nx)}

    def column(core):
        for ((dz, _),) in farthest_first([((k, nz),) for k in range(1, nz)]):
            yield {"z": lax.rem(z + dz, nz), "c": core, "y": y, "x": x}

    def remote(src, dst, send_sem, recv_sem, device):
        return pltpu.make_async_remote_copy(
            src_ref=src, dst_ref=dst, send_sem=send_sem, recv_sem=recv_sem,
            device_id=device, device_id_type=MESH,
        )

    def several(slots, count, send_sem, recv_sem):
        some = slots.at[0:count]
        return remote(some, some, send_sem, recv_sem, other)

    def started(copy, sends):
        @pl.when(sends)
        def _():
            copy.start()

    def received(copy, gets):
        @pl.when(gets)
        def _():
            copy.wait_recv()

    def left(copy, sends):
        @pl.when(sends)
        def _():
            copy.wait_send()

    load_x = pltpu.make_async_copy(
        x_hbm, xr.at[pl.ds(own, frames), 1 : band + 1], load_sem.at[0]
    )
    load_c = pltpu.make_async_copy(cot_hbm, cr.at[0:frames, 1 : band + 1], load_sem.at[1])
    load_w = pltpu.make_async_copy(w_hbm, wv, load_sem.at[2])
    load_gn = pltpu.make_async_copy(gn_hbm, gain_ref, load_sem.at[3])
    load_sh = pltpu.make_async_copy(sh_hbm, bias_ref, load_sem.at[4])
    for copy in (load_x, load_c, load_w, load_gn, load_sh):
        copy.start()

    barrier = pltpu.get_barrier_semaphore()
    def enter(devices):
        for device in devices:
            pl.semaphore_signal(barrier, inc=1, device_id=device, device_id_type=MESH)

    corners = [at(tm + dt, row + dw) for dt in (-1, 1) for dw in (-1, 1)]
    enter((*column(1), *plane(1), other, *corners))

    @pl.when(follow)
    def _():
        enter((*column(0), *plane(0)))

    @pl.when(lead)
    def _():
        enter((at(tm, row + 1), at(tm, row - 1)))

    chips = n_rows - 1 + nz - 1
    partners = jnp.where(follow, 2 * chips + 5, chips + 7)

    load_x.wait()

    def folded(v):
        return v.reshape(width // 8, 8, chans).sum(axis=0)

    def stat_row(k, carry):
        total, square = carry
        v = xr[own + k // band, 1 + lax.rem(k, band)].astype(F32)
        return total + folded(v), square + folded(v * v)

    zero8 = jnp.zeros((8, chans), F32)
    total, square = lax.fori_loop(0, frames * band, stat_row, (zero8, zero8))
    st1[nc * row + c, 0:1] = total.sum(axis=0, keepdims=True)
    st1[nc * row + c, 1:2] = square.sum(axis=0, keepdims=True)

    pl.semaphore_wait(barrier, partners)

    def summed(slots):
        total = slots[0]
        for k in range(1, slots.shape[0]):
            total = total + slots[k]
        return total

    def collect(slots, mine, peers, k):
        part = slots.at[mine]
        for device in peers:
            remote(part, part, st_s.at[k], st_r.at[k], device).start()
        started(remote(part, part, st_s.at[k], st_r.at[k], other), lead)

    def spread(slots, mine, collected, peers, k):
        @pl.when(follow)
        def _():
            several(collected, collected.shape[0] - 1, st_s.at[k - 1], st_r.at[k - 1]).wait_recv()
            slots[mine] = summed(collected)
            part = slots.at[mine]
            for device in (*peers, other):
                remote(part, part, st_s.at[k], st_r.at[k], device).start()

    def finished(slots, k):
        received(several(slots, slots.shape[0] - 1, st_s.at[k], st_r.at[k]), follow)
        received(several(slots, slots.shape[0], st_s.at[k], st_r.at[k]), lead)

    collect(st1, nc * row + c, plane(1), 0)

    def margins(buf, first, there, way, body_from, corners_from, send_sem, recv_sem):
        mine = buf.at[pl.ds(first, frames)]
        moved = buf.at[pl.ds(there, frames)]
        up_t = (tm + way >= 0) & (tm + way < n_tm)
        from_t = (tm - way >= 0) & (tm - way < n_tm)
        up_c, from_c = up_t & (c == corners_from), from_t & (c != corners_from)
        if body_from is not None:
            up_t, from_t = up_t & (c == body_from), from_t & (c != body_from)
        up_r, down_r = row < n_rows - 1, row > 0
        low, high, body = mine.at[:, 1], mine.at[:, band], slice(1, band + 1)
        plan = [
            (high, mine.at[:, 0], at(tm, row + 1), up_r, down_r),
            (low, mine.at[:, band + 1], at(tm, row - 1), down_r, up_r),
            (mine.at[:, body], moved.at[:, body], at(tm + way, row), up_t, from_t),
            (high, moved.at[:, 0], at(tm + way, row + 1), up_c & up_r, from_c & down_r),
            (low, moved.at[:, band + 1], at(tm + way, row - 1), up_c & down_r, from_c & up_r),
        ]
        sems = [(send_sem.at[k], recv_sem.at[k]) for k in range(3)]
        sems += [(corner_s.at[k], corner_r.at[k]) for k in range(2)]
        return [
            (remote(src, dst, *sem, device), sends, gets)
            for (src, dst, device, sends, gets), sem in zip(plan, sems)
        ]

    load_c.wait()
    cot_margins = margins(cr, 0, frames, -1, None, 0, cs, cq)
    x_margins = margins(xr, own, 0, 1, 1, 1, xs, xq)
    partner_cot = remote(cr.at[0:frames, 1 : band + 1], cpart, ps.at[0], pq.at[0], other)
    mine_x = xr.at[pl.ds(own, frames), 1 : band + 1]
    swapped_x = remote(mine_x, mine_x, ps.at[1], pq.at[1], other)

    partner_cot.start()
    swapped_x.start()
    for copy, sends, _ in (*x_margins[:3], *cot_margins, *x_margins[3:]):
        started(copy, sends)

    zeros_pad = jnp.zeros((WP - width, chans), F32)

    def padded_row(v):
        return jnp.concatenate([v, zeros_pad], axis=0)

    def three_ways(v, keep=True):
        v = padded_row(v.astype(F32))
        if keep is not True:
            v = jnp.where(keep, v, 0.0)
        return pltpu.roll(v, 1, 0), v, pltpu.roll(v, WP - 1, 0)

    def cot_row(t, h, keep=True):
        sides = three_ways(cr[t, h], keep)
        for shift in range(3):
            c3[shift, t, h] = sides[shift].astype(BF16)
        return sides

    def put_turned(chip_half, k, sides):
        for shift in range(3):
            turned = sides[2 - shift].T.astype(BF16)
            for core in range(nc):
                ct[chip_half, core, shift * half_o : (shift + 1) * half_o, k * WP : (k + 1) * WP] = (
                    turned[core * half_o : (core + 1) * half_o]
                )

    for k in range(frames * band):
        put_turned(c, k, cot_row(k // band, 1 + k % band))
    for h in (0, band + 1):
        c3[:, :, h] = jnp.zeros((3, 2 * frames, WP, chans), BF16)
    load_w.wait()
    load_gn.wait()
    load_sh.wait()
    partner_cot.wait_recv()
    for k in range(frames * band):
        put_turned(1 - c, k, three_ways(cpart[k // band, k % band]))

    spread(st2, z, st1, (*column(1), *column(0)), 1)

    row_low, row_high = row > 0, row < n_rows - 1
    before = xr.at[0:frames]
    passed_low = remote(before.at[:, 0], before.at[:, 0], ps.at[5], pq.at[5], other)
    passed_high = remote(before.at[:, band + 1], before.at[:, band + 1], ps.at[6], pq.at[6], other)
    body_before = before.at[:, 1 : band + 1]
    passed_body = remote(body_before, body_before, ps.at[4], pq.at[4], other)
    mine_all = xr.at[pl.ds(own, frames)]
    gave_low = remote(mine_all.at[:, 0], mine_all.at[:, 0], ps.at[2], pq.at[2], other)
    gave_high = remote(mine_all.at[:, band + 1], mine_all.at[:, band + 1], ps.at[3], pq.at[3], other)
    for copy, _, gets in x_margins[:2]:
        received(copy, gets)
    started(gave_low, row_low)
    started(gave_high, row_high)

    taps = [(b, s) for b in range(3) for s in range(3)]

    def frame(refs, t):
        rows = [refs[s][t, b : b + band].reshape(band * WP, chans) for b, s in taps]
        return jnp.concatenate(rows, axis=1)

    def back_taps(a):
        return jnp.concatenate([wv[9 * (2 - a) + 3 * (2 - b) + 2 - s] for b, s in taps], axis=1)

    def back(lhs, rhs):
        return lax.dot_general(lhs, rhs, (((1,), (1,)), ((), ())), preferred_element_type=F32)

    half = band * WP
    c3s = [c3.at[s] for s in range(3)]
    both = back(frame(c3s, 1), jnp.concatenate([back_taps(1), back_taps(0)], axis=0))
    ga[0:half] = back(frame(c3s, 0), back_taps(0)) + both[:, :chans]
    ga[half:] = both[:, chans:]

    def cot_corner(h, k):
        landing = cr.at[frames : 2 * frames, h]
        return remote(cr.at[0:frames, h], landing, ps.at[k], pq.at[k], other)

    cot_low, cot_high = cot_corner(0, 5), cot_corner(band + 1, 6)
    for copy, _, gets in cot_margins[:2]:
        received(copy, gets)
    started(cot_low, follow & row_low)
    started(cot_high, follow & row_high)

    received(cot_margins[2][0], cot_margins[2][2])
    has_next = tm < n_tm - 1
    for t in range(frames, 2 * frames):
        for h in range(1, band + 1):
            cot_row(t, h, has_next)
    both = back(frame(c3s, 2), jnp.concatenate([back_taps(2), back_taps(1)], axis=0))
    ga[0:half] += both[:, :chans]
    ga[half:] += back(frame(c3s, 3), back_taps(2)) + both[:, chans:]

    def edge(t_in):
        keep = has_next if t_in >= frames else True
        for side, b, exists in ((0, 0, row_low), (1, 2, row_high)):
            sides = three_ways(cr[t_in, side * (band + 1)], exists & keep)
            lhs = jnp.concatenate([v.astype(BF16) for v in sides], axis=1)
            gets = [(t, t_in - t) for t in range(frames) if 0 <= t_in - t < 3]
            rhs = jnp.concatenate(
                [
                    jnp.concatenate(
                        [wv[9 * (2 - a) + 3 * (2 - b) + 2 - s] for s in range(3)], axis=1
                    )
                    for _, a in gets
                ],
                axis=0,
            )
            given = back(lhs, rhs)
            for j, (t, _) in enumerate(gets):
                at_t = t * half + side * (band - 1) * WP
                ga[at_t : at_t + WP] += given[:, j * chans : (j + 1) * chans]

    for t in range(frames):
        edge(t)

    finished(st2, 1)
    stats = summed(st2)
    wide = lambda v: jnp.broadcast_to(v, (8, chans))
    mean = group_total(wide(stats[0:1]), chans // G) / cells
    variance = group_total(wide(stats[1:2]), chans // G) / cells - mean * mean
    inverse = lax.rsqrt(variance + EPSILON)
    gain, shift_ = wide(gain_ref[...]), wide(bias_ref[...])
    mean, inverse, gain, shift_ = (v[0:1] for v in (mean, inverse, gain, shift_))

    swapped_x.wait_recv()
    received(gave_low, row_low)
    received(gave_high, row_high)

    for copy, _, gets in x_margins[2:]:
        received(copy, gets)
    started(passed_body, lead & has_before)
    started(passed_low, lead & has_before & row_low)
    started(passed_high, lead & has_before & row_high)


    def sigmoid(v):
        return 0.5 + 0.5 * jnp.tanh(0.5 * v)

    def act_frames(low, high, rows=range(band + 2)):
        for t in range(low, high):
            for h in rows:
                v = xr[t, h].astype(F32)
                pre = (v - mean) * inverse * gain + shift_
                act = pre * sigmoid(pre)
                keep = True
                if t < frames:
                    keep = has_before
                if h == 0:
                    keep = keep & row_low
                if h == band + 1:
                    keep = keep & row_high
                if keep is not True:
                    act = jnp.where(keep, act, 0.0)
                a0[t, h] = padded_row(act).astype(BF16)

    chip_frames = frames * nc
    turned = lambda: jnp.concatenate([ct[h, c] for h in range(nc)], axis=1)
    in_first_half = row // dests == 0
    place = lax.rem(row, dests)

    def blocks_of(p):
        low, high = PIECES[p]
        return slice(3 * low, 3 * high)

    def weight_piece(p):
        low, high = PIECES[p]
        rhs = jnp.concatenate(
            [
                a0[a : a + chip_frames, b : b + band].reshape(chip_frames * half, chans)
                for a, b in PAIRS[low:high]
            ],
            axis=1,
        )
        part = jnp.dot(turned(), rhs, preferred_element_type=F32)
        for j in range(high - low):
            for s in range(3):
                block = part[s * half_o : (s + 1) * half_o, j * chans : (j + 1) * chans]
                bsend[:, 3 * (low + j) + s] = block.reshape(dests, own_o, chans).astype(BF16)

    ys = dests // nx
    from_first = lax.rem(y - ys * c + ny, ny)

    def band_dests():
        near_first = (from_first == 0) | (from_first == ny - 1)
        start = jnp.where(near_first, ys - 1, 0)
        for ((dx, _),) in farthest_first([((k, nx),) for k in range(nx)]):
            for j in range(ys):
                yield ys * c + lax.rem(start + j, ys), lax.rem(x + dx, nx), dx != 0

    def send_rows(p):
        blocks = blocks_of(p)

        @pl.when(follow & jnp.logical_not(in_first_half))
        def _():
            brecv[row, blocks] = bsend[place, blocks]

        for ty, tx, is_other in band_dests():
            q = (ty - ys * c) * nx + tx
            device = {"z": z, "c": 1, "y": ty, "x": tx}
            copy = remote(
                bsend.at[q, blocks], brecv.at[row, blocks], bs.at[0], br.at[p], device
            )
            if is_other:
                copy.start()
            else:
                started(copy, lead | (ty != y))

    act_frames(frames, frames + chip_frames, range(band))
    weight_piece(0)
    send_rows(0)
    act_frames(frames, frames + chip_frames, range(band, band + 2))
    weight_piece(1)
    send_rows(1)
    received(passed_body, follow & has_before)
    received(passed_low, follow & has_before & row_low)
    received(passed_high, follow & has_before & row_high)
    act_frames(1, 2)

    weight_piece(2)
    send_rows(2)
    act_frames(0, 1)
    weight_piece(3)
    send_rows(3)
    for copy, _, gets in cot_margins[3:]:
        received(copy, gets)
    received(cot_low, lead & row_low)
    received(cot_high, lead & row_high)
    for t in range(frames, 2 * frames):
        edge(t)

    def pre_row(k):
        v = xr[own + k // band, 1 + k % band].astype(F32)
        return (v - mean) * inverse

    gains, biases = zero8, zero8
    for k in range(frames * band):
        normed = pre_row(k)
        pre = normed * gain + shift_
        sig = sigmoid(pre)
        at_k = slice(k * WP, k * WP + width)
        grad = ga[at_k] * sig * (1.0 + pre * (1.0 - sig))
        ga[at_k] = grad
        gains = gains + folded(grad * normed)
        biases = biases + folded(grad)
    gs1[tm, 0:1] = gains.sum(axis=0, keepdims=True)
    gs1[tm, 1:2] = biases.sum(axis=0, keepdims=True)
    collect(gs1, tm, column(1), 2)

    weight_piece(4)
    send_rows(4)

    def of_piece(buf, count, p, recv_sem):
        return several(buf.at[:, blocks_of(p)], count, bs.at[0], recv_sem.at[p])

    def send_z(p):
        blocks = blocks_of(p)

        @pl.when(follow)
        def _():
            received(of_piece(brecv, n_rows, p, br), in_first_half)
            received(of_piece(brecv, n_rows - 1, p, br), jnp.logical_not(in_first_half))
            value = brecv[0, blocks].astype(F32)
            for k in range(1, n_rows):
                value = value + brecv[k, blocks].astype(F32)
            crecv[z, blocks] = value.astype(BF16)
            mine = crecv.at[z, blocks]
            for device in column(1):
                remote(mine, mine, zs.at[0], zr.at[p], device).start()

    send_z(0)

    def shift_row(k, carry):
        t, h = k // high_rows, lax.rem(k, high_rows)
        v = a0[frames * c + t, h].astype(F32)
        a3[0, t, h] = pltpu.roll(v, 1, 0).astype(BF16)
        a3[1, t, h] = pltpu.roll(v, WP - 1, 0).astype(BF16)
        return carry

    lax.fori_loop(0, 2 * frames * high_rows, shift_row, 0)
    send_z(1)
    sides = (a3.at[0], a0.at[pl.ds(frames * c, 2 * frames)], a3.at[1])

    def front_taps(a):
        return jnp.concatenate([wv[9 * a + 3 * b + s] for b, s in taps], axis=0)

    def front(lhs, rhs):
        return jnp.dot(lhs, rhs, preferred_element_type=F32)

    one = front(frame(sides, 1), jnp.concatenate([front_taps(1), front_taps(0)], axis=1))
    cv[0:half] = front(frame(sides, 0), front_taps(0)) + one[:, :chans]
    cv[half:] = one[:, chans:]
    send_z(2)
    two = front(frame(sides, 2), jnp.concatenate([front_taps(2), front_taps(1)], axis=1))
    cv[0:half] += two[:, :chans]
    cv[half:] += front(frame(sides, 3), front_taps(2)) + two[:, chans:]
    for k in range(frames * band):
        v = xr[own + k // band, 1 + k % band].astype(F32)
        ofv[k // band, k % band] = (v + cv[k * WP : k * WP + width]).astype(BF16)
    spread(gs2, row, gs1, (*plane(1), *plane(0)), 3)
    send_z(3)

    send_z(4)

    finished(gs2, 3)
    sums = summed(gs2)
    gain_grad, bias_grad = wide(sums[0:1]), wide(sums[1:2])
    gv[...] = sums[0:1]
    bv[...] = sums[1:2]
    mean_dn = (group_total(gain * bias_grad, chans // G) / cells)[0:1]
    mean_dnn = (group_total(gain * gain_grad, chans // G) / cells)[0:1]
    for k in range(frames * band):
        t, h = k // band, k % band
        normed = pre_row(k)
        grad = ga[k * WP : k * WP + width]
        cot = cr[t, 1 + h].astype(F32)
        igv[t, h] = (inverse * (grad * gain - mean_dn - normed * mean_dnn) + cot).astype(BF16)

    for p in range(N_PIECES):
        blocks = blocks_of(p)

        @pl.when(follow)
        def _():
            of_piece(crecv, nz - 1, p, zr).wait_recv()
            value = crecv[0, blocks].astype(F32)
            for k in range(1, nz):
                value = value + crecv[k, blocks].astype(F32)
            fin[blocks] = value
            remote(fin.at[blocks], fin.at[blocks], fs.at[0], fr.at[0], other).start()

    whole = remote(fin, fin, fs.at[0], fr.at[0], other)
    received(whole, lead)
    scale = 1.0 / math.sqrt(all_pixels)
    for m in range(27):
        a, b = PAIRS[m // 3]
        at_m = (9 * a + 3 * b + m % 3) * chans
        wgv[:, at_m : at_m + chans] = fin[m] * scale

    def parts_left(count, k, sends):
        left(several(st1, count, st_s.at[k], st_r.at[k]), sends)

    for k, chips in ((0, n_rows), (2, nz)):
        parts_left(chips, k, lead)
        parts_left(chips - 1, k, follow)
    parts_left(2 * nz - 1, 1, follow)
    parts_left(2 * n_rows - 1, 3, follow)
    partner_cot.wait_send()
    swapped_x.wait_send()
    for copy, sends, _ in (*cot_margins, *x_margins):
        left(copy, sends)
    left(gave_low, row_low)
    left(gave_high, row_high)
    left(cot_low, follow & row_low)
    left(cot_high, follow & row_high)
    left(passed_body, lead & has_before)
    left(passed_low, lead & has_before & row_low)
    left(passed_high, lead & has_before & row_high)

    own_half = follow & jnp.logical_not(in_first_half)
    left(several(bsend, dests - 1, bs.at[0], br.at[0]), own_half)
    left(several(bsend, dests, bs.at[0], br.at[0]), jnp.logical_not(own_half))
    left(several(crecv, nz - 1, zs.at[0], zr.at[0]), follow)
    left(whole, follow)


def put_out(*refs):
    sources, places, sem = refs[:5], refs[5:10], refs[10]
    copies = [pltpu.make_async_copy(s, d, sem.at[k]) for k, (s, d) in enumerate(zip(sources, places))]
    for copy in copies:
        copy.start()
    for copy in copies:
        copy.wait()


def per_device(sizes, frames_in, norm_gain, norm_bias, conv_weight, cotangent):
    nz, nc, ny, nx = sizes
    n_tm, n_rows = nz * nc, ny * nx
    frames, band, width, chans = frames_in.shape
    own_o, dests = chans // n_rows, n_rows // nc
    rows = (2 * frames, band + 2)
    chip = (frames + frames * nc, band + 2)
    vmem, dma = pltpu.VMEM, pltpu.SemaphoreType.DMA
    scratch = [
        vmem((1, chans), F32),
        vmem((1, chans), F32),
        vmem((*chip, width, chans), BF16),
        vmem((*rows, width, chans), BF16),
        vmem((frames, band, width, chans), BF16),
        vmem((27, chans, chans), BF16),
        vmem((*chip, WP, chans), BF16),
        vmem((2, *rows, WP, chans), BF16),
        vmem((3, *rows, WP, chans), BF16),
        vmem((nc, nc, 3 * chans // nc, frames * band * WP), BF16),
        vmem((frames * band * WP, chans), F32),
        vmem((frames * band * WP, chans), F32),
        vmem((dests, 27, own_o, chans), BF16),
        vmem((n_rows, 27, own_o, chans), BF16),
        vmem((nz, 27, own_o, chans), BF16),
        vmem((27, own_o, chans), F32),
        vmem((n_rows * nc, 2, chans), F32),
        vmem((nz, 2, chans), F32),
        vmem((n_tm, 2, chans), F32),
        vmem((n_rows, 2, chans), F32),
        dma((5,)),
        dma((3,)), dma((3,)), dma((3,)), dma((3,)), dma((2,)), dma((2,)), dma((7,)), dma((7,)), dma((4,)), dma((4,)),
        dma((1,)), dma((N_PIECES,)), dma((1,)), dma((N_PIECES,)), dma((1,)), dma((1,)),
    ]
    anywhere = pl.BlockSpec(memory_space=pl.ANY)
    stays = pl.BlockSpec(memory_space=pltpu.HBM)
    inside = pl.BlockSpec(memory_space=pltpu.VMEM)
    out = jax.ShapeDtypeStruct
    operands = (
        frames_in,
        norm_gain.reshape(1, chans),
        norm_bias.reshape(1, chans),
        conv_weight.reshape(27, chans, chans),
        cotangent,
    )
    made = pl.pallas_call(
        functools.partial(kernel, sizes),
        out_shape=(
            out(frames_in.shape, BF16),
            out(frames_in.shape, BF16),
            out((own_o, 27 * chans), F32),
            out((1, chans), F32),
            out((1, chans), F32),
        ),
        in_specs=[stays] * 5,
        out_specs=[inside] * 5,
        scratch_shapes=scratch,
        compiler_params=pltpu.CompilerParams(
            collective_id=0, has_side_effects=True, vmem_limit_bytes=48 << 20
        ),
        name="block",
    )(*(pltpu.with_memory_space_constraint(a, pltpu.HBM) for a in operands))
    of, ig, wg, gg, bg = pl.pallas_call(
        put_out,
        out_shape=[out(a.shape, a.dtype) for a in made],
        in_specs=[anywhere] * 5,
        out_specs=[stays] * 5,
        scratch_shapes=[dma((5,))],
        compiler_params=pltpu.CompilerParams(vmem_limit_bytes=1 << 20),
        name="put_out",
    )(*made)
    return of, ig, wg, gg.reshape(chans), bg.reshape(chans)


def program(devices):
    torus = Mesh(devices, ("z", "c", "y", "x"))
    placed = (P(TM, ROWS, None, None), P(), P(), P(), P(TM, ROWS, None, None))
    return jax.shard_map(
        functools.partial(per_device, devices.shape),
        mesh=torus,
        in_specs=placed,
        out_specs=(P(TM, ROWS, None, None), P(TM, ROWS, None, None), P(ROWS, None), P(), P()),
        check_vma=False,
    )


def solution(mesh):
    return program(mesh.devices.reshape(8, 2, 4, 4))
```

```python
import functools
import math

import jax
import jax.numpy as jnp
from jax import lax
from jax.experimental import pallas as pl
from jax.experimental.pallas import tpu as pltpu
from jax.sharding import Mesh
from jax.sharding import PartitionSpec as P

G = 32
EPSILON = 1e-06
TM = ("z", "c")
ROWS = ("y", "x")
MESH = pl.DeviceIdType.MESH
WP = 128
F32 = jnp.float32
BF16 = jnp.bfloat16
PAIRS = tuple((a, b) for a in (2, 1, 0) for b in range(3))
PIECES = ((0, 1), (1, 3), (3, 5), (5, 7), (7, 9))
N_PIECES = len(PIECES)


def group_total(per_channel, size):
    lanes = lax.broadcasted_iota(jnp.int32, per_channel.shape, 1)
    within = lanes % size
    channels = per_channel.shape[1]
    total = per_channel
    for step in range(1, size):
        ahead = pltpu.roll(per_channel, channels - step, 1)
        behind = pltpu.roll(per_channel, step, 1)
        total = total + jnp.where(within + step < size, ahead, 0.0)
        total = total + jnp.where(within >= step, behind, 0.0)
    return total


def kernel(
    sizes, x_hbm, gn_hbm, sh_hbm, w_hbm, cot_hbm,
    ofv, igv, wgv, gv, bv,
    gain_ref, bias_ref, xr, cr, cpart, wv, a0, a3, c3, ct, ga, cv, bsend, brecv, crecv, fin,
    st1, st2, gs1, gs2,
    load_sem, xs, xq, cs, cq, corner_s, corner_r, ps, pq, st_s, st_r, bs, br, zs, zr, fs, fr,
):
    nz, nc, ny, nx = sizes
    n_tm, n_rows = nz * nc, ny * nx
    frames, band, width, chans = x_hbm.shape
    high_rows = band + 2
    own_o = chans // n_rows
    dests = n_rows // nc
    half_o = chans // nc
    all_pixels = frames * n_tm * band * n_rows * width
    cells = all_pixels * (chans // G)
    z, c = lax.axis_index("z"), lax.axis_index("c")
    y, x = lax.axis_index("y"), lax.axis_index("x")
    tm, row = z * nc + c, y * nx + x
    own = frames + frames * c
    other = {"z": z, "c": 1 - c, "y": y, "x": x}
    lead, follow = c == 0, c == 1
    has_before = z > 0

    def at(t, r):
        t, r = lax.rem(t + n_tm, n_tm), lax.rem(r + n_rows, n_rows)
        return {"z": t // nc, "c": lax.rem(t, nc), "y": r // nx, "x": lax.rem(r, nx)}

    def farthest_first(steps):
        return sorted(steps, key=lambda pairs: -sum(min(d, n - d) for d, n in pairs))

    def plane(core):
        steps = [((k // nx, ny), (k % nx, nx)) for k in range(1, n_rows)]
        for (dy, _), (dx, _) in farthest_first(steps):
            yield {"z": z, "c": core, "y": lax.rem(y + dy, ny), "x": lax.rem(x + dx, nx)}

    def column(core):
        for ((dz, _),) in farthest_first([((k, nz),) for k in range(1, nz)]):
            yield {"z": lax.rem(z + dz, nz), "c": core, "y": y, "x": x}

    def remote(src, dst, send_sem, recv_sem, device):
        return pltpu.make_async_remote_copy(
            src_ref=src, dst_ref=dst, send_sem=send_sem, recv_sem=recv_sem,
            device_id=device, device_id_type=MESH,
        )

    def several(slots, count, send_sem, recv_sem):
        some = slots.at[0:count]
        return remote(some, some, send_sem, recv_sem, other)

    def started(copy, sends):
        @pl.when(sends)
        def _():
            copy.start()

    def received(copy, gets):
        @pl.when(gets)
        def _():
            copy.wait_recv()

    def left(copy, sends):
        @pl.when(sends)
        def _():
            copy.wait_send()

    load_x = pltpu.make_async_copy(
        x_hbm, xr.at[pl.ds(own, frames), 1 : band + 1], load_sem.at[0]
    )
    load_c = pltpu.make_async_copy(cot_hbm, cr.at[0:frames, 1 : band + 1], load_sem.at[1])
    load_w = pltpu.make_async_copy(w_hbm, wv, load_sem.at[2])
    load_gn = pltpu.make_async_copy(gn_hbm, gain_ref, load_sem.at[3])
    load_sh = pltpu.make_async_copy(sh_hbm, bias_ref, load_sem.at[4])
    for copy in (load_x, load_c, load_w, load_gn, load_sh):
        copy.start()

    barrier = pltpu.get_barrier_semaphore()
    def enter(devices):
        for device in devices:
            pl.semaphore_signal(barrier, inc=1, device_id=device, device_id_type=MESH)

    corners = [at(tm + dt, row + dw) for dt in (-1, 1) for dw in (-1, 1)]
    enter((*column(1), *plane(1), other, *corners))

    @pl.when(follow)
    def _():
        enter((*column(0), *plane(0)))

    @pl.when(lead)
    def _():
        enter((at(tm, row + 1), at(tm, row - 1)))

    chips = n_rows - 1 + nz - 1
    partners = jnp.where(follow, 2 * chips + 5, chips + 7)

    load_x.wait()

    def folded(v):
        return v.reshape(width // 8, 8, chans).sum(axis=0)

    def stat_row(k, carry):
        total, square = carry
        v = xr[own + k // band, 1 + lax.rem(k, band)].astype(F32)
        return total + folded(v), square + folded(v * v)

    zero8 = jnp.zeros((8, chans), F32)
    total, square = lax.fori_loop(0, frames * band, stat_row, (zero8, zero8))
    st1[nc * row + c, 0:1] = total.sum(axis=0, keepdims=True)
    st1[nc * row + c, 1:2] = square.sum(axis=0, keepdims=True)

    pl.semaphore_wait(barrier, partners)

    def summed(slots):
        total = slots[0]
        for k in range(1, slots.shape[0]):
            total = total + slots[k]
        return total

    def collect(slots, mine, peers, k):
        part = slots.at[mine]
        for device in peers:
            remote(part, part, st_s.at[k], st_r.at[k], device).start()
        started(remote(part, part, st_s.at[k], st_r.at[k], other), lead)

    def spread(slots, mine, collected, peers, k):
        @pl.when(follow)
        def _():
            several(collected, collected.shape[0] - 1, st_s.at[k - 1], st_r.at[k - 1]).wait_recv()
            slots[mine] = summed(collected)
            part = slots.at[mine]
            for device in (*peers, other):
                remote(part, part, st_s.at[k], st_r.at[k], device).start()

    def finished(slots, k):
        received(several(slots, slots.shape[0] - 1, st_s.at[k], st_r.at[k]), follow)
        received(several(slots, slots.shape[0], st_s.at[k], st_r.at[k]), lead)

    collect(st1, nc * row + c, plane(1), 0)

    def margins(buf, first, there, way, body_from, corners_from, send_sem, recv_sem):
        mine = buf.at[pl.ds(first, frames)]
        moved = buf.at[pl.ds(there, frames)]
        up_t = (tm + way >= 0) & (tm + way < n_tm)
        from_t = (tm - way >= 0) & (tm - way < n_tm)
        up_c, from_c = up_t & (c == corners_from), from_t & (c != corners_from)
        if body_from is not None:
            up_t, from_t = up_t & (c == body_from), from_t & (c != body_from)
        up_r, down_r = row < n_rows - 1, row > 0
        low, high, body = mine.at[:, 1], mine.at[:, band], slice(1, band + 1)
        plan = [
            (high, mine.at[:, 0], at(tm, row + 1), up_r, down_r),
            (low, mine.at[:, band + 1], at(tm, row - 1), down_r, up_r),
            (mine.at[:, body], moved.at[:, body], at(tm + way, row), up_t, from_t),
            (high, moved.at[:, 0], at(tm + way, row + 1), up_c & up_r, from_c & down_r),
            (low, moved.at[:, band + 1], at(tm + way, row - 1), up_c & down_r, from_c & up_r),
        ]
        sems = [(send_sem.at[k], recv_sem.at[k]) for k in range(3)]
        sems += [(corner_s.at[k], corner_r.at[k]) for k in range(2)]
        return [
            (remote(src, dst, *sem, device), sends, gets)
            for (src, dst, device, sends, gets), sem in zip(plan, sems)
        ]

    load_c.wait()
    cot_margins = margins(cr, 0, frames, -1, None, 0, cs, cq)
    x_margins = margins(xr, own, 0, 1, 1, 1, xs, xq)
    partner_cot = remote(cr.at[0:frames, 1 : band + 1], cpart, ps.at[0], pq.at[0], other)
    mine_x = xr.at[pl.ds(own, frames), 1 : band + 1]
    swapped_x = remote(mine_x, mine_x, ps.at[1], pq.at[1], other)

    partner_cot.start()
    swapped_x.start()
    for copy, sends, _ in (*x_margins[:3], *cot_margins, *x_margins[3:]):
        started(copy, sends)

    zeros_pad = jnp.zeros((WP - width, chans), F32)

    def padded_row(v):
        return jnp.concatenate([v, zeros_pad], axis=0)

    def three_ways(v, keep=True):
        v = padded_row(v.astype(F32))
        if keep is not True:
            v = jnp.where(keep, v, 0.0)
        return pltpu.roll(v, 1, 0), v, pltpu.roll(v, WP - 1, 0)

    def cot_row(t, h, keep=True):
        sides = three_ways(cr[t, h], keep)
        for shift in range(3):
            c3[shift, t, h] = sides[shift].astype(BF16)
        return sides

    def put_turned(chip_half, k, sides):
        for shift in range(3):
            turned = sides[2 - shift].T.astype(BF16)
            for core in range(nc):
                ct[chip_half, core, shift * half_o : (shift + 1) * half_o, k * WP : (k + 1) * WP] = (
                    turned[core * half_o : (core + 1) * half_o]
                )

    for k in range(frames * band):
        put_turned(c, k, cot_row(k // band, 1 + k % band))
    for h in (0, band + 1):
        c3[:, :, h] = jnp.zeros((3, 2 * frames, WP, chans), BF16)
    load_w.wait()
    load_gn.wait()
    load_sh.wait()
    partner_cot.wait_recv()
    for k in range(frames * band):
        put_turned(1 - c, k, three_ways(cpart[k // band, k % band]))

    spread(st2, z, st1, (*column(1), *column(0)), 1)

    row_low, row_high = row > 0, row < n_rows - 1
    before = xr.at[0:frames]
    passed_low = remote(before.at[:, 0], before.at[:, 0], ps.at[5], pq.at[5], other)
    passed_high = remote(before.at[:, band + 1], before.at[:, band + 1], ps.at[6], pq.at[6], other)
    body_before = before.at[:, 1 : band + 1]
    passed_body = remote(body_before, body_before, ps.at[4], pq.at[4], other)
    mine_all = xr.at[pl.ds(own, frames)]
    gave_low = remote(mine_all.at[:, 0], mine_all.at[:, 0], ps.at[2], pq.at[2], other)
    gave_high = remote(mine_all.at[:, band + 1], mine_all.at[:, band + 1], ps.at[3], pq.at[3], other)
    for copy, _, gets in x_margins[:2]:
        received(copy, gets)
    started(gave_low, row_low)
    started(gave_high, row_high)

    taps = [(b, s) for b in range(3) for s in range(3)]

    def frame(refs, t):
        rows = [refs[s][t, b : b + band].reshape(band * WP, chans) for b, s in taps]
        return jnp.concatenate(rows, axis=1)

    def back_taps(a):
        return jnp.concatenate([wv[9 * (2 - a) + 3 * (2 - b) + 2 - s] for b, s in taps], axis=1)

    def back(lhs, rhs):
        return lax.dot_general(lhs, rhs, (((1,), (1,)), ((), ())), preferred_element_type=F32)

    half = band * WP
    c3s = [c3.at[s] for s in range(3)]
    both = back(frame(c3s, 1), jnp.concatenate([back_taps(1), back_taps(0)], axis=0))
    ga[0:half] = back(frame(c3s, 0), back_taps(0)) + both[:, :chans]
    ga[half:] = both[:, chans:]

    def cot_corner(h, k):
        landing = cr.at[frames : 2 * frames, h]
        return remote(cr.at[0:frames, h], landing, ps.at[k], pq.at[k], other)

    cot_low, cot_high = cot_corner(0, 5), cot_corner(band + 1, 6)
    for copy, _, gets in cot_margins[:2]:
        received(copy, gets)
    started(cot_low, follow & row_low)
    started(cot_high, follow & row_high)

    received(cot_margins[2][0], cot_margins[2][2])
    has_next = tm < n_tm - 1
    for t in range(frames, 2 * frames):
        for h in range(1, band + 1):
            cot_row(t, h, has_next)
    both = back(frame(c3s, 2), jnp.concatenate([back_taps(2), back_taps(1)], axis=0))
    ga[0:half] += both[:, :chans]
    ga[half:] += back(frame(c3s, 3), back_taps(2)) + both[:, chans:]

    def edge(t_in):
        keep = has_next if t_in >= frames else True
        for side, b, exists in ((0, 0, row_low), (1, 2, row_high)):
            sides = three_ways(cr[t_in, side * (band + 1)], exists & keep)
            lhs = jnp.concatenate([v.astype(BF16) for v in sides], axis=1)
            gets = [(t, t_in - t) for t in range(frames) if 0 <= t_in - t < 3]
            rhs = jnp.concatenate(
                [
                    jnp.concatenate(
                        [wv[9 * (2 - a) + 3 * (2 - b) + 2 - s] for s in range(3)], axis=1
                    )
                    for _, a in gets
                ],
                axis=0,
            )
            given = back(lhs, rhs)
            for j, (t, _) in enumerate(gets):
                at_t = t * half + side * (band - 1) * WP
                ga[at_t : at_t + WP] += given[:, j * chans : (j + 1) * chans]

    for t in range(frames):
        edge(t)

    finished(st2, 1)
    stats = summed(st2)
    wide = lambda v: jnp.broadcast_to(v, (8, chans))
    mean = group_total(wide(stats[0:1]), chans // G) / cells
    variance = group_total(wide(stats[1:2]), chans // G) / cells - mean * mean
    inverse = lax.rsqrt(variance + EPSILON)
    gain, shift_ = wide(gain_ref[...]), wide(bias_ref[...])
    mean, inverse, gain, shift_ = (v[0:1] for v in (mean, inverse, gain, shift_))

    swapped_x.wait_recv()
    received(gave_low, row_low)
    received(gave_high, row_high)

    for copy, _, gets in x_margins[2:]:
        received(copy, gets)
    started(passed_body, lead & has_before)
    started(passed_low, lead & has_before & row_low)
    started(passed_high, lead & has_before & row_high)


    def sigmoid(v):
        return 0.5 + 0.5 * jnp.tanh(0.5 * v)

    def act_frames(low, high, rows=range(band + 2)):
        for t in range(low, high):
            for h in rows:
                v = xr[t, h].astype(F32)
                pre = (v - mean) * inverse * gain + shift_
                act = pre * sigmoid(pre)
                keep = True
                if t < frames:
                    keep = has_before
                if h == 0:
                    keep = keep & row_low
                if h == band + 1:
                    keep = keep & row_high
                if keep is not True:
                    act = jnp.where(keep, act, 0.0)
                a0[t, h] = padded_row(act).astype(BF16)

    chip_frames = frames * nc
    turned = lambda: jnp.concatenate([ct[h, c] for h in range(nc)], axis=1)
    in_first_half = row // dests == 0
    place = lax.rem(row, dests)

    def blocks_of(p):
        low, high = PIECES[p]
        return slice(3 * low, 3 * high)

    def weight_piece(p):
        low, high = PIECES[p]
        rhs = jnp.concatenate(
            [
                a0[a : a + chip_frames, b : b + band].reshape(chip_frames * half, chans)
                for a, b in PAIRS[low:high]
            ],
            axis=1,
        )
        part = jnp.dot(turned(), rhs, preferred_element_type=F32)
        for j in range(high - low):
            for s in range(3):
                block = part[s * half_o : (s + 1) * half_o, j * chans : (j + 1) * chans]
                bsend[:, 3 * (low + j) + s] = block.reshape(dests, own_o, chans).astype(BF16)

    ys = dests // nx
    from_first = lax.rem(y - ys * c + ny, ny)

    def band_dests():
        near_first = (from_first == 0) | (from_first == ny - 1)
        start = jnp.where(near_first, ys - 1, 0)
        for ((dx, _),) in farthest_first([((k, nx),) for k in range(nx)]):
            for j in range(ys):
                yield ys * c + lax.rem(start + j, ys), lax.rem(x + dx, nx), dx != 0

    def send_rows(p):
        blocks = blocks_of(p)

        @pl.when(follow & jnp.logical_not(in_first_half))
        def _():
            brecv[row, blocks] = bsend[place, blocks]

        for ty, tx, is_other in band_dests():
            q = (ty - ys * c) * nx + tx
            device = {"z": z, "c": 1, "y": ty, "x": tx}
            copy = remote(
                bsend.at[q, blocks], brecv.at[row, blocks], bs.at[0], br.at[p], device
            )
            if is_other:
                copy.start()
            else:
                started(copy, lead | (ty != y))

    act_frames(frames, frames + chip_frames, range(band))
    weight_piece(0)
    send_rows(0)
    act_frames(frames, frames + chip_frames, range(band, band + 2))
    weight_piece(1)
    send_rows(1)
    received(passed_body, follow & has_before)
    received(passed_low, follow & has_before & row_low)
    received(passed_high, follow & has_before & row_high)
    act_frames(1, 2)

    weight_piece(2)
    send_rows(2)
    act_frames(0, 1)
    weight_piece(3)
    send_rows(3)
    weight_piece(4)
    send_rows(4)

    for copy, _, gets in cot_margins[3:]:
        received(copy, gets)
    received(cot_low, lead & row_low)
    received(cot_high, lead & row_high)
    for t in range(frames, 2 * frames):
        edge(t)

    def pre_row(k):
        v = xr[own + k // band, 1 + k % band].astype(F32)
        return (v - mean) * inverse

    gains, biases = zero8, zero8
    for k in range(frames * band):
        normed = pre_row(k)
        pre = normed * gain + shift_
        sig = sigmoid(pre)
        at_k = slice(k * WP, k * WP + width)
        grad = ga[at_k] * sig * (1.0 + pre * (1.0 - sig))
        ga[at_k] = grad
        gains = gains + folded(grad * normed)
        biases = biases + folded(grad)
    gs1[tm, 0:1] = gains.sum(axis=0, keepdims=True)
    gs1[tm, 1:2] = biases.sum(axis=0, keepdims=True)
    collect(gs1, tm, column(1), 2)

    def of_piece(buf, count, p, recv_sem):
        return several(buf.at[:, blocks_of(p)], count, bs.at[0], recv_sem.at[p])

    def send_z(p):
        blocks = blocks_of(p)

        @pl.when(follow)
        def _():
            received(of_piece(brecv, n_rows, p, br), in_first_half)
            received(of_piece(brecv, n_rows - 1, p, br), jnp.logical_not(in_first_half))
            value = brecv[0, blocks].astype(F32)
            for k in range(1, n_rows):
                value = value + brecv[k, blocks].astype(F32)
            crecv[z, blocks] = value.astype(BF16)
            mine = crecv.at[z, blocks]
            for device in column(1):
                remote(mine, mine, zs.at[0], zr.at[p], device).start()

    send_z(0)

    def shift_row(k, carry):
        t, h = k // high_rows, lax.rem(k, high_rows)
        v = a0[frames * c + t, h].astype(F32)
        a3[0, t, h] = pltpu.roll(v, 1, 0).astype(BF16)
        a3[1, t, h] = pltpu.roll(v, WP - 1, 0).astype(BF16)
        return carry

    lax.fori_loop(0, 2 * frames * high_rows, shift_row, 0)
    send_z(1)
    sides = (a3.at[0], a0.at[pl.ds(frames * c, 2 * frames)], a3.at[1])

    def front_taps(a):
        return jnp.concatenate([wv[9 * a + 3 * b + s] for b, s in taps], axis=0)

    def front(lhs, rhs):
        return jnp.dot(lhs, rhs, preferred_element_type=F32)

    one = front(frame(sides, 1), jnp.concatenate([front_taps(1), front_taps(0)], axis=1))
    cv[0:half] = front(frame(sides, 0), front_taps(0)) + one[:, :chans]
    cv[half:] = one[:, chans:]
    send_z(2)
    two = front(frame(sides, 2), jnp.concatenate([front_taps(2), front_taps(1)], axis=1))
    cv[0:half] += two[:, :chans]
    cv[half:] += front(frame(sides, 3), front_taps(2)) + two[:, chans:]
    for k in range(frames * band):
        v = xr[own + k // band, 1 + k % band].astype(F32)
        ofv[k // band, k % band] = (v + cv[k * WP : k * WP + width]).astype(BF16)
    send_z(3)

    send_z(4)
    spread(gs2, row, gs1, (*plane(1), *plane(0)), 3)

    finished(gs2, 3)
    sums = summed(gs2)
    gain_grad, bias_grad = wide(sums[0:1]), wide(sums[1:2])
    gv[...] = sums[0:1]
    bv[...] = sums[1:2]
    mean_dn = (group_total(gain * bias_grad, chans // G) / cells)[0:1]
    mean_dnn = (group_total(gain * gain_grad, chans // G) / cells)[0:1]
    for k in range(frames * band):
        t, h = k // band, k % band
        normed = pre_row(k)
        grad = ga[k * WP : k * WP + width]
        cot = cr[t, 1 + h].astype(F32)
        igv[t, h] = (inverse * (grad * gain - mean_dn - normed * mean_dnn) + cot).astype(BF16)

    for p in range(N_PIECES):
        blocks = blocks_of(p)

        @pl.when(follow)
        def _():
            of_piece(crecv, nz - 1, p, zr).wait_recv()
            value = crecv[0, blocks].astype(F32)
            for k in range(1, nz):
                value = value + crecv[k, blocks].astype(F32)
            fin[blocks] = value
            remote(fin.at[blocks], fin.at[blocks], fs.at[0], fr.at[0], other).start()

    whole = remote(fin, fin, fs.at[0], fr.at[0], other)
    received(whole, lead)
    scale = 1.0 / math.sqrt(all_pixels)
    for m in range(27):
        a, b = PAIRS[m // 3]
        at_m = (9 * a + 3 * b + m % 3) * chans
        wgv[:, at_m : at_m + chans] = fin[m] * scale

    def parts_left(count, k, sends):
        left(several(st1, count, st_s.at[k], st_r.at[k]), sends)

    for k, chips in ((0, n_rows), (2, nz)):
        parts_left(chips, k, lead)
        parts_left(chips - 1, k, follow)
    parts_left(2 * nz - 1, 1, follow)
    parts_left(2 * n_rows - 1, 3, follow)
    partner_cot.wait_send()
    swapped_x.wait_send()
    for copy, sends, _ in (*cot_margins, *x_margins):
        left(copy, sends)
    left(gave_low, row_low)
    left(gave_high, row_high)
    left(cot_low, follow & row_low)
    left(cot_high, follow & row_high)
    left(passed_body, lead & has_before)
    left(passed_low, lead & has_before & row_low)
    left(passed_high, lead & has_before & row_high)

    own_half = follow & jnp.logical_not(in_first_half)
    left(several(bsend, dests - 1, bs.at[0], br.at[0]), own_half)
    left(several(bsend, dests, bs.at[0], br.at[0]), jnp.logical_not(own_half))
    left(several(crecv, nz - 1, zs.at[0], zr.at[0]), follow)
    left(whole, follow)


def put_out(*refs):
    sources, places, sem = refs[:5], refs[5:10], refs[10]
    copies = [pltpu.make_async_copy(s, d, sem.at[k]) for k, (s, d) in enumerate(zip(sources, places))]
    for copy in copies:
        copy.start()
    for copy in copies:
        copy.wait()


def per_device(sizes, frames_in, norm_gain, norm_bias, conv_weight, cotangent):
    nz, nc, ny, nx = sizes
    n_tm, n_rows = nz * nc, ny * nx
    frames, band, width, chans = frames_in.shape
    own_o, dests = chans // n_rows, n_rows // nc
    rows = (2 * frames, band + 2)
    chip = (frames + frames * nc, band + 2)
    vmem, dma = pltpu.VMEM, pltpu.SemaphoreType.DMA
    scratch = [
        vmem((1, chans), F32),
        vmem((1, chans), F32),
        vmem((*chip, width, chans), BF16),
        vmem((*rows, width, chans), BF16),
        vmem((frames, band, width, chans), BF16),
        vmem((27, chans, chans), BF16),
        vmem((*chip, WP, chans), BF16),
        vmem((2, *rows, WP, chans), BF16),
        vmem((3, *rows, WP, chans), BF16),
        vmem((nc, nc, 3 * chans // nc, frames * band * WP), BF16),
        vmem((frames * band * WP, chans), F32),
        vmem((frames * band * WP, chans), F32),
        vmem((dests, 27, own_o, chans), BF16),
        vmem((n_rows, 27, own_o, chans), BF16),
        vmem((nz, 27, own_o, chans), BF16),
        vmem((27, own_o, chans), F32),
        vmem((n_rows * nc, 2, chans), F32),
        vmem((nz, 2, chans), F32),
        vmem((n_tm, 2, chans), F32),
        vmem((n_rows, 2, chans), F32),
        dma((5,)),
        dma((3,)), dma((3,)), dma((3,)), dma((3,)), dma((2,)), dma((2,)), dma((7,)), dma((7,)), dma((4,)), dma((4,)),
        dma((1,)), dma((N_PIECES,)), dma((1,)), dma((N_PIECES,)), dma((1,)), dma((1,)),
    ]
    anywhere = pl.BlockSpec(memory_space=pl.ANY)
    stays = pl.BlockSpec(memory_space=pltpu.HBM)
    inside = pl.BlockSpec(memory_space=pltpu.VMEM)
    out = jax.ShapeDtypeStruct
    operands = (
        frames_in,
        norm_gain.reshape(1, chans),
        norm_bias.reshape(1, chans),
        conv_weight.reshape(27, chans, chans),
        cotangent,
    )
    made = pl.pallas_call(
        functools.partial(kernel, sizes),
        out_shape=(
            out(frames_in.shape, BF16),
            out(frames_in.shape, BF16),
            out((own_o, 27 * chans), F32),
            out((1, chans), F32),
            out((1, chans), F32),
        ),
        in_specs=[stays] * 5,
        out_specs=[inside] * 5,
        scratch_shapes=scratch,
        compiler_params=pltpu.CompilerParams(
            collective_id=0, has_side_effects=True, vmem_limit_bytes=48 << 20
        ),
        name="block",
    )(*(pltpu.with_memory_space_constraint(a, pltpu.HBM) for a in operands))
    of, ig, wg, gg, bg = pl.pallas_call(
        put_out,
        out_shape=[out(a.shape, a.dtype) for a in made],
        in_specs=[anywhere] * 5,
        out_specs=[stays] * 5,
        scratch_shapes=[dma((5,))],
        compiler_params=pltpu.CompilerParams(vmem_limit_bytes=1 << 20),
        name="put_out",
    )(*made)
    return of, ig, wg, gg.reshape(chans), bg.reshape(chans)


def program(devices):
    torus = Mesh(devices, ("z", "c", "y", "x"))
    placed = (P(TM, ROWS, None, None), P(), P(), P(), P(TM, ROWS, None, None))
    return jax.shard_map(
        functools.partial(per_device, devices.shape),
        mesh=torus,
        in_specs=placed,
        out_specs=(P(TM, ROWS, None, None), P(TM, ROWS, None, None), P(ROWS, None), P(), P()),
        check_vma=False,
    )


def solution(mesh):
    return program(mesh.devices.reshape(8, 2, 4, 4))
```

```python
import functools
import math

import jax
import jax.numpy as jnp
from jax import lax
from jax.experimental import pallas as pl
from jax.experimental.pallas import tpu as pltpu
from jax.sharding import Mesh
from jax.sharding import PartitionSpec as P

G = 32
EPSILON = 1e-06
TM = ("z", "c")
ROWS = ("y", "x")
MESH = pl.DeviceIdType.MESH
WP = 128
F32 = jnp.float32
BF16 = jnp.bfloat16
PAIRS = tuple((a, b) for a in (2, 1, 0) for b in range(3))
PIECES = ((0, 1), (1, 3), (3, 5), (5, 7), (7, 9))
N_PIECES = len(PIECES)


def group_total(per_channel, size):
    lanes = lax.broadcasted_iota(jnp.int32, per_channel.shape, 1)
    within = lanes % size
    channels = per_channel.shape[1]
    total = per_channel
    for step in range(1, size):
        ahead = pltpu.roll(per_channel, channels - step, 1)
        behind = pltpu.roll(per_channel, step, 1)
        total = total + jnp.where(within + step < size, ahead, 0.0)
        total = total + jnp.where(within >= step, behind, 0.0)
    return total


def kernel(
    sizes, x_hbm, gn_hbm, sh_hbm, w_hbm, cot_hbm,
    ofv, igv, wgv, gv, bv,
    gain_ref, bias_ref, xr, cr, cpart, wv, a0, a3, c3, ct, ga, cv, bsend, brecv, crecv, fin,
    st1, st2, gs1, gs2,
    load_sem, xs, xq, cs, cq, corner_s, corner_r, ps, pq, st_s, st_r, bs, br, zs, zr, fs, fr,
):
    nz, nc, ny, nx = sizes
    n_tm, n_rows = nz * nc, ny * nx
    frames, band, width, chans = x_hbm.shape
    high_rows = band + 2
    own_o = chans // n_rows
    dests = n_rows // nc
    half_o = chans // nc
    all_pixels = frames * n_tm * band * n_rows * width
    cells = all_pixels * (chans // G)
    z, c = lax.axis_index("z"), lax.axis_index("c")
    y, x = lax.axis_index("y"), lax.axis_index("x")
    tm, row = z * nc + c, y * nx + x
    own = frames + frames * c
    other = {"z": z, "c": 1 - c, "y": y, "x": x}
    lead, follow = c == 0, c == 1
    has_before = z > 0

    def at(t, r):
        t, r = lax.rem(t + n_tm, n_tm), lax.rem(r + n_rows, n_rows)
        return {"z": t // nc, "c": lax.rem(t, nc), "y": r // nx, "x": lax.rem(r, nx)}

    def farthest_first(steps):
        return sorted(steps, key=lambda pairs: -sum(min(d, n - d) for d, n in pairs))

    def plane(core):
        steps = [((k // nx, ny), (k % nx, nx)) for k in range(1, n_rows)]
        for (dy, _), (dx, _) in farthest_first(steps):
            yield {"z": z, "c": core, "y": lax.rem(y + dy, ny), "x": lax.rem(x + dx, nx)}

    def column(core):
        for ((dz, _),) in farthest_first([((k, nz),) for k in range(1, nz)]):
            yield {"z": lax.rem(z + dz, nz), "c": core, "y": y, "x": x}

    def remote(src, dst, send_sem, recv_sem, device):
        return pltpu.make_async_remote_copy(
            src_ref=src, dst_ref=dst, send_sem=send_sem, recv_sem=recv_sem,
            device_id=device, device_id_type=MESH,
        )

    def several(slots, count, send_sem, recv_sem):
        some = slots.at[0:count]
        return remote(some, some, send_sem, recv_sem, other)

    def started(copy, sends):
        @pl.when(sends)
        def _():
            copy.start()

    def received(copy, gets):
        @pl.when(gets)
        def _():
            copy.wait_recv()

    def left(copy, sends):
        @pl.when(sends)
        def _():
            copy.wait_send()

    load_x = pltpu.make_async_copy(
        x_hbm, xr.at[pl.ds(own, frames), 1 : band + 1], load_sem.at[0]
    )
    load_c = pltpu.make_async_copy(cot_hbm, cr.at[0:frames, 1 : band + 1], load_sem.at[1])
    load_w = pltpu.make_async_copy(w_hbm, wv, load_sem.at[2])
    load_gn = pltpu.make_async_copy(gn_hbm, gain_ref, load_sem.at[3])
    load_sh = pltpu.make_async_copy(sh_hbm, bias_ref, load_sem.at[4])
    for copy in (load_x, load_c, load_w, load_gn, load_sh):
        copy.start()

    barrier = pltpu.get_barrier_semaphore()
    def enter(devices):
        for device in devices:
            pl.semaphore_signal(barrier, inc=1, device_id=device, device_id_type=MESH)

    corners = [at(tm + dt, row + dw) for dt in (-1, 1) for dw in (-1, 1)]
    enter((*column(1), *plane(1), other, *corners))

    @pl.when(follow)
    def _():
        enter((*column(0), *plane(0)))

    @pl.when(lead)
    def _():
        enter((at(tm, row + 1), at(tm, row - 1)))

    chips = n_rows - 1 + nz - 1
    partners = jnp.where(follow, 2 * chips + 5, chips + 7)

    load_x.wait()

    def folded(v):
        return v.reshape(width // 8, 8, chans).sum(axis=0)

    def stat_row(k, carry):
        total, square = carry
        v = xr[own + k // band, 1 + lax.rem(k, band)].astype(F32)
        return total + folded(v), square + folded(v * v)

    zero8 = jnp.zeros((8, chans), F32)
    total, square = lax.fori_loop(0, frames * band, stat_row, (zero8, zero8))
    st1[nc * row + c, 0:1] = total.sum(axis=0, keepdims=True)
    st1[nc * row + c, 1:2] = square.sum(axis=0, keepdims=True)

    pl.semaphore_wait(barrier, partners)

    def summed(slots):
        parts = [slots[k] for k in range(slots.shape[0])]
        while len(parts) > 1:
            parts = [low + high for low, high in zip(parts[::2], parts[1::2])]
        return parts[0]

    def collect(slots, mine, peers, k):
        part = slots.at[mine]
        for device in peers:
            remote(part, part, st_s.at[k], st_r.at[k], device).start()
        started(remote(part, part, st_s.at[k], st_r.at[k], other), lead)

    def spread(slots, mine, collected, peers, k):
        @pl.when(follow)
        def _():
            several(collected, collected.shape[0] - 1, st_s.at[k - 1], st_r.at[k - 1]).wait_recv()
            slots[mine] = summed(collected)
            part = slots.at[mine]
            for device in (*peers, other):
                remote(part, part, st_s.at[k], st_r.at[k], device).start()

    def finished(slots, k):
        received(several(slots, slots.shape[0] - 1, st_s.at[k], st_r.at[k]), follow)
        received(several(slots, slots.shape[0], st_s.at[k], st_r.at[k]), lead)

    collect(st1, nc * row + c, plane(1), 0)

    def margins(buf, first, there, way, body_from, corners_from, send_sem, recv_sem):
        mine = buf.at[pl.ds(first, frames)]
        moved = buf.at[pl.ds(there, frames)]
        up_t = (tm + way >= 0) & (tm + way < n_tm)
        from_t = (tm - way >= 0) & (tm - way < n_tm)
        up_c, from_c = up_t & (c == corners_from), from_t & (c != corners_from)
        if body_from is not None:
            up_t, from_t = up_t & (c == body_from), from_t & (c != body_from)
        up_r, down_r = row < n_rows - 1, row > 0
        low, high, body = mine.at[:, 1], mine.at[:, band], slice(1, band + 1)
        plan = [
            (high, mine.at[:, 0], at(tm, row + 1), up_r, down_r),
            (low, mine.at[:, band + 1], at(tm, row - 1), down_r, up_r),
            (mine.at[:, body], moved.at[:, body], at(tm + way, row), up_t, from_t),
            (high, moved.at[:, 0], at(tm + way, row + 1), up_c & up_r, from_c & down_r),
            (low, moved.at[:, band + 1], at(tm + way, row - 1), up_c & down_r, from_c & up_r),
        ]
        sems = [(send_sem.at[k], recv_sem.at[k]) for k in range(3)]
        sems += [(corner_s.at[k], corner_r.at[k]) for k in range(2)]
        return [
            (remote(src, dst, *sem, device), sends, gets)
            for (src, dst, device, sends, gets), sem in zip(plan, sems)
        ]

    load_c.wait()
    cot_margins = margins(cr, 0, frames, -1, None, 0, cs, cq)
    x_margins = margins(xr, own, 0, 1, 1, 1, xs, xq)
    partner_cot = remote(cr.at[0:frames, 1 : band + 1], cpart, ps.at[0], pq.at[0], other)
    mine_x = xr.at[pl.ds(own, frames), 1 : band + 1]
    swapped_x = remote(mine_x, mine_x, ps.at[1], pq.at[1], other)

    partner_cot.start()
    swapped_x.start()
    for copy, sends, _ in (*x_margins[:3], *cot_margins, *x_margins[3:]):
        started(copy, sends)

    zeros_pad = jnp.zeros((WP - width, chans), F32)

    def padded_row(v):
        return jnp.concatenate([v, zeros_pad], axis=0)

    def three_ways(v, keep=True):
        v = padded_row(v.astype(F32))
        if keep is not True:
            v = jnp.where(keep, v, 0.0)
        return pltpu.roll(v, 1, 0), v, pltpu.roll(v, WP - 1, 0)

    def cot_row(t, h, keep=True):
        sides = three_ways(cr[t, h], keep)
        for shift in range(3):
            c3[shift, t, h] = sides[shift].astype(BF16)
        return sides

    def put_turned(chip_half, k, sides):
        for shift in range(3):
            turned = sides[2 - shift].T.astype(BF16)
            for core in range(nc):
                ct[chip_half, core, shift * half_o : (shift + 1) * half_o, k * WP : (k + 1) * WP] = (
                    turned[core * half_o : (core + 1) * half_o]
                )

    for k in range(frames * band):
        put_turned(c, k, cot_row(k // band, 1 + k % band))
    for h in (0, band + 1):
        c3[:, :, h] = jnp.zeros((3, 2 * frames, WP, chans), BF16)
    load_w.wait()
    load_gn.wait()
    load_sh.wait()
    partner_cot.wait_recv()
    for k in range(frames * band):
        put_turned(1 - c, k, three_ways(cpart[k // band, k % band]))

    spread(st2, z, st1, (*column(1), *column(0)), 1)

    row_low, row_high = row > 0, row < n_rows - 1
    before = xr.at[0:frames]
    passed_low = remote(before.at[:, 0], before.at[:, 0], ps.at[5], pq.at[5], other)
    passed_high = remote(before.at[:, band + 1], before.at[:, band + 1], ps.at[6], pq.at[6], other)
    body_before = before.at[:, 1 : band + 1]
    passed_body = remote(body_before, body_before, ps.at[4], pq.at[4], other)
    mine_all = xr.at[pl.ds(own, frames)]
    gave_low = remote(mine_all.at[:, 0], mine_all.at[:, 0], ps.at[2], pq.at[2], other)
    gave_high = remote(mine_all.at[:, band + 1], mine_all.at[:, band + 1], ps.at[3], pq.at[3], other)
    for copy, _, gets in x_margins[:2]:
        received(copy, gets)
    started(gave_low, row_low)
    started(gave_high, row_high)

    taps = [(b, s) for b in range(3) for s in range(3)]

    def frame(refs, t):
        rows = [refs[s][t, b : b + band].reshape(band * WP, chans) for b, s in taps]
        return jnp.concatenate(rows, axis=1)

    def back_taps(a):
        return jnp.concatenate([wv[9 * (2 - a) + 3 * (2 - b) + 2 - s] for b, s in taps], axis=1)

    def back(lhs, rhs):
        return lax.dot_general(lhs, rhs, (((1,), (1,)), ((), ())), preferred_element_type=F32)

    half = band * WP
    c3s = [c3.at[s] for s in range(3)]
    both = back(frame(c3s, 1), jnp.concatenate([back_taps(1), back_taps(0)], axis=0))
    ga[0:half] = back(frame(c3s, 0), back_taps(0)) + both[:, :chans]
    ga[half:] = both[:, chans:]

    def cot_corner(h, k):
        landing = cr.at[frames : 2 * frames, h]
        return remote(cr.at[0:frames, h], landing, ps.at[k], pq.at[k], other)

    cot_low, cot_high = cot_corner(0, 5), cot_corner(band + 1, 6)
    for copy, _, gets in cot_margins[:2]:
        received(copy, gets)
    started(cot_low, follow & row_low)
    started(cot_high, follow & row_high)

    received(cot_margins[2][0], cot_margins[2][2])
    has_next = tm < n_tm - 1
    for t in range(frames, 2 * frames):
        for h in range(1, band + 1):
            cot_row(t, h, has_next)
    both = back(frame(c3s, 2), jnp.concatenate([back_taps(2), back_taps(1)], axis=0))
    ga[0:half] += both[:, :chans]
    ga[half:] += back(frame(c3s, 3), back_taps(2)) + both[:, chans:]

    def edge(t_in):
        keep = has_next if t_in >= frames else True
        for side, b, exists in ((0, 0, row_low), (1, 2, row_high)):
            sides = three_ways(cr[t_in, side * (band + 1)], exists & keep)
            lhs = jnp.concatenate([v.astype(BF16) for v in sides], axis=1)
            gets = [(t, t_in - t) for t in range(frames) if 0 <= t_in - t < 3]
            rhs = jnp.concatenate(
                [
                    jnp.concatenate(
                        [wv[9 * (2 - a) + 3 * (2 - b) + 2 - s] for s in range(3)], axis=1
                    )
                    for _, a in gets
                ],
                axis=0,
            )
            given = back(lhs, rhs)
            for j, (t, _) in enumerate(gets):
                at_t = t * half + side * (band - 1) * WP
                ga[at_t : at_t + WP] += given[:, j * chans : (j + 1) * chans]

    for t in range(frames):
        edge(t)

    finished(st2, 1)
    stats = summed(st2)
    wide = lambda v: jnp.broadcast_to(v, (8, chans))
    mean = group_total(wide(stats[0:1]), chans // G) / cells
    variance = group_total(wide(stats[1:2]), chans // G) / cells - mean * mean
    inverse = lax.rsqrt(variance + EPSILON)
    gain, shift_ = wide(gain_ref[...]), wide(bias_ref[...])
    mean, inverse, gain, shift_ = (v[0:1] for v in (mean, inverse, gain, shift_))

    swapped_x.wait_recv()
    received(gave_low, row_low)
    received(gave_high, row_high)

    for copy, _, gets in x_margins[2:]:
        received(copy, gets)
    started(passed_body, lead & has_before)
    started(passed_low, lead & has_before & row_low)
    started(passed_high, lead & has_before & row_high)


    def sigmoid(v):
        return 0.5 + 0.5 * jnp.tanh(0.5 * v)

    def act_frames(low, high, rows=range(band + 2)):
        for t in range(low, high):
            for h in rows:
                v = xr[t, h].astype(F32)
                pre = (v - mean) * inverse * gain + shift_
                act = pre * sigmoid(pre)
                keep = True
                if t < frames:
                    keep = has_before
                if h == 0:
                    keep = keep & row_low
                if h == band + 1:
                    keep = keep & row_high
                if keep is not True:
                    act = jnp.where(keep, act, 0.0)
                a0[t, h] = padded_row(act).astype(BF16)

    chip_frames = frames * nc
    turned = lambda: jnp.concatenate([ct[h, c] for h in range(nc)], axis=1)
    in_first_half = row // dests == 0
    place = lax.rem(row, dests)

    def blocks_of(p):
        low, high = PIECES[p]
        return slice(3 * low, 3 * high)

    def weight_piece(p):
        low, high = PIECES[p]
        rhs = jnp.concatenate(
            [
                a0[a : a + chip_frames, b : b + band].reshape(chip_frames * half, chans)
                for a, b in PAIRS[low:high]
            ],
            axis=1,
        )
        part = jnp.dot(turned(), rhs, preferred_element_type=F32)
        for j in range(high - low):
            for s in range(3):
                block = part[s * half_o : (s + 1) * half_o, j * chans : (j + 1) * chans]
                bsend[:, 3 * (low + j) + s] = block.reshape(dests, own_o, chans).astype(BF16)

    ys = dests // nx
    from_first = lax.rem(y - ys * c + ny, ny)

    def band_dests():
        near_first = (from_first == 0) | (from_first == ny - 1)
        start = jnp.where(near_first, ys - 1, 0)
        for ((dx, _),) in farthest_first([((k, nx),) for k in range(nx)]):
            for j in range(ys):
                yield ys * c + lax.rem(start + j, ys), lax.rem(x + dx, nx), dx != 0

    def send_rows(p):
        blocks = blocks_of(p)

        @pl.when(follow & jnp.logical_not(in_first_half))
        def _():
            brecv[row, blocks] = bsend[place, blocks]

        for ty, tx, is_other in band_dests():
            q = (ty - ys * c) * nx + tx
            device = {"z": z, "c": 1, "y": ty, "x": tx}
            copy = remote(
                bsend.at[q, blocks], brecv.at[row, blocks], bs.at[0], br.at[p], device
            )
            if is_other:
                copy.start()
            else:
                started(copy, lead | (ty != y))

    act_frames(frames, frames + chip_frames, range(band))
    weight_piece(0)
    send_rows(0)
    act_frames(frames, frames + chip_frames, range(band, band + 2))
    weight_piece(1)
    send_rows(1)
    received(passed_body, follow & has_before)
    received(passed_low, follow & has_before & row_low)
    received(passed_high, follow & has_before & row_high)
    act_frames(1, 2)

    weight_piece(2)
    send_rows(2)
    act_frames(0, 1)
    weight_piece(3)
    send_rows(3)
    for copy, _, gets in cot_margins[3:]:
        received(copy, gets)
    received(cot_low, lead & row_low)
    received(cot_high, lead & row_high)
    for t in range(frames, 2 * frames):
        edge(t)

    def pre_row(k):
        v = xr[own + k // band, 1 + k % band].astype(F32)
        return (v - mean) * inverse

    gains, biases = zero8, zero8
    for k in range(frames * band):
        normed = pre_row(k)
        pre = normed * gain + shift_
        sig = sigmoid(pre)
        at_k = slice(k * WP, k * WP + width)
        grad = ga[at_k] * sig * (1.0 + pre * (1.0 - sig))
        ga[at_k] = grad
        gains = gains + folded(grad * normed)
        biases = biases + folded(grad)
    gs1[tm, 0:1] = gains.sum(axis=0, keepdims=True)
    gs1[tm, 1:2] = biases.sum(axis=0, keepdims=True)
    collect(gs1, tm, column(1), 2)

    weight_piece(4)
    send_rows(4)

    def of_piece(buf, count, p, recv_sem):
        return several(buf.at[:, blocks_of(p)], count, bs.at[0], recv_sem.at[p])

    def send_z(p):
        blocks = blocks_of(p)

        @pl.when(follow)
        def _():
            received(of_piece(brecv, n_rows, p, br), in_first_half)
            received(of_piece(brecv, n_rows - 1, p, br), jnp.logical_not(in_first_half))
            value = brecv[0, blocks].astype(F32)
            for k in range(1, n_rows):
                value = value + brecv[k, blocks].astype(F32)
            crecv[z, blocks] = value.astype(BF16)
            mine = crecv.at[z, blocks]
            for device in column(1):
                remote(mine, mine, zs.at[0], zr.at[p], device).start()

    send_z(0)

    def shift_row(k, carry):
        t, h = k // high_rows, lax.rem(k, high_rows)
        v = a0[frames * c + t, h].astype(F32)
        a3[0, t, h] = pltpu.roll(v, 1, 0).astype(BF16)
        a3[1, t, h] = pltpu.roll(v, WP - 1, 0).astype(BF16)
        return carry

    lax.fori_loop(0, 2 * frames * high_rows, shift_row, 0)
    send_z(1)
    sides = (a3.at[0], a0.at[pl.ds(frames * c, 2 * frames)], a3.at[1])

    def front_taps(a):
        return jnp.concatenate([wv[9 * a + 3 * b + s] for b, s in taps], axis=0)

    def front(lhs, rhs):
        return jnp.dot(lhs, rhs, preferred_element_type=F32)

    one = front(frame(sides, 1), jnp.concatenate([front_taps(1), front_taps(0)], axis=1))
    cv[0:half] = front(frame(sides, 0), front_taps(0)) + one[:, :chans]
    cv[half:] = one[:, chans:]
    send_z(2)
    two = front(frame(sides, 2), jnp.concatenate([front_taps(2), front_taps(1)], axis=1))
    cv[0:half] += two[:, :chans]
    cv[half:] += front(frame(sides, 3), front_taps(2)) + two[:, chans:]
    for k in range(frames * band):
        v = xr[own + k // band, 1 + k % band].astype(F32)
        ofv[k // band, k % band] = (v + cv[k * WP : k * WP + width]).astype(BF16)
    spread(gs2, row, gs1, (*plane(1), *plane(0)), 3)
    send_z(3)

    send_z(4)

    finished(gs2, 3)
    sums = summed(gs2)
    gain_grad, bias_grad = wide(sums[0:1]), wide(sums[1:2])
    gv[...] = sums[0:1]
    bv[...] = sums[1:2]
    mean_dn = (group_total(gain * bias_grad, chans // G) / cells)[0:1]
    mean_dnn = (group_total(gain * gain_grad, chans // G) / cells)[0:1]
    for k in range(frames * band):
        t, h = k // band, k % band
        normed = pre_row(k)
        grad = ga[k * WP : k * WP + width]
        cot = cr[t, 1 + h].astype(F32)
        igv[t, h] = (inverse * (grad * gain - mean_dn - normed * mean_dnn) + cot).astype(BF16)

    for p in range(N_PIECES):
        blocks = blocks_of(p)

        @pl.when(follow)
        def _():
            of_piece(crecv, nz - 1, p, zr).wait_recv()
            value = crecv[0, blocks].astype(F32)
            for k in range(1, nz):
                value = value + crecv[k, blocks].astype(F32)
            fin[blocks] = value
            remote(fin.at[blocks], fin.at[blocks], fs.at[0], fr.at[0], other).start()

    whole = remote(fin, fin, fs.at[0], fr.at[0], other)
    received(whole, lead)
    scale = 1.0 / math.sqrt(all_pixels)
    for m in range(27):
        a, b = PAIRS[m // 3]
        at_m = (9 * a + 3 * b + m % 3) * chans
        wgv[:, at_m : at_m + chans] = fin[m] * scale

    def parts_left(count, k, sends):
        left(several(st1, count, st_s.at[k], st_r.at[k]), sends)

    for k, chips in ((0, n_rows), (2, nz)):
        parts_left(chips, k, lead)
        parts_left(chips - 1, k, follow)
    parts_left(2 * nz - 1, 1, follow)
    parts_left(2 * n_rows - 1, 3, follow)
    partner_cot.wait_send()
    swapped_x.wait_send()
    for copy, sends, _ in (*cot_margins, *x_margins):
        left(copy, sends)
    left(gave_low, row_low)
    left(gave_high, row_high)
    left(cot_low, follow & row_low)
    left(cot_high, follow & row_high)
    left(passed_body, lead & has_before)
    left(passed_low, lead & has_before & row_low)
    left(passed_high, lead & has_before & row_high)

    own_half = follow & jnp.logical_not(in_first_half)
    left(several(bsend, dests - 1, bs.at[0], br.at[0]), own_half)
    left(several(bsend, dests, bs.at[0], br.at[0]), jnp.logical_not(own_half))
    left(several(crecv, nz - 1, zs.at[0], zr.at[0]), follow)
    left(whole, follow)


def put_out(*refs):
    sources, places, sem = refs[:5], refs[5:10], refs[10]
    copies = [pltpu.make_async_copy(s, d, sem.at[k]) for k, (s, d) in enumerate(zip(sources, places))]
    for copy in copies:
        copy.start()
    for copy in copies:
        copy.wait()


def per_device(sizes, frames_in, norm_gain, norm_bias, conv_weight, cotangent):
    nz, nc, ny, nx = sizes
    n_tm, n_rows = nz * nc, ny * nx
    frames, band, width, chans = frames_in.shape
    own_o, dests = chans // n_rows, n_rows // nc
    rows = (2 * frames, band + 2)
    chip = (frames + frames * nc, band + 2)
    vmem, dma = pltpu.VMEM, pltpu.SemaphoreType.DMA
    scratch = [
        vmem((1, chans), F32),
        vmem((1, chans), F32),
        vmem((*chip, width, chans), BF16),
        vmem((*rows, width, chans), BF16),
        vmem((frames, band, width, chans), BF16),
        vmem((27, chans, chans), BF16),
        vmem((*chip, WP, chans), BF16),
        vmem((2, *rows, WP, chans), BF16),
        vmem((3, *rows, WP, chans), BF16),
        vmem((nc, nc, 3 * chans // nc, frames * band * WP), BF16),
        vmem((frames * band * WP, chans), F32),
        vmem((frames * band * WP, chans), F32),
        vmem((dests, 27, own_o, chans), BF16),
        vmem((n_rows, 27, own_o, chans), BF16),
        vmem((nz, 27, own_o, chans), BF16),
        vmem((27, own_o, chans), F32),
        vmem((n_rows * nc, 2, chans), F32),
        vmem((nz, 2, chans), F32),
        vmem((n_tm, 2, chans), F32),
        vmem((n_rows, 2, chans), F32),
        dma((5,)),
        dma((3,)), dma((3,)), dma((3,)), dma((3,)), dma((2,)), dma((2,)), dma((7,)), dma((7,)), dma((4,)), dma((4,)),
        dma((1,)), dma((N_PIECES,)), dma((1,)), dma((N_PIECES,)), dma((1,)), dma((1,)),
    ]
    anywhere = pl.BlockSpec(memory_space=pl.ANY)
    stays = pl.BlockSpec(memory_space=pltpu.HBM)
    inside = pl.BlockSpec(memory_space=pltpu.VMEM)
    out = jax.ShapeDtypeStruct
    operands = (
        frames_in,
        norm_gain.reshape(1, chans),
        norm_bias.reshape(1, chans),
        conv_weight.reshape(27, chans, chans),
        cotangent,
    )
    made = pl.pallas_call(
        functools.partial(kernel, sizes),
        out_shape=(
            out(frames_in.shape, BF16),
            out(frames_in.shape, BF16),
            out((own_o, 27 * chans), F32),
            out((1, chans), F32),
            out((1, chans), F32),
        ),
        in_specs=[stays] * 5,
        out_specs=[inside] * 5,
        scratch_shapes=scratch,
        compiler_params=pltpu.CompilerParams(
            collective_id=0, has_side_effects=True, vmem_limit_bytes=48 << 20
        ),
        name="block",
    )(*(pltpu.with_memory_space_constraint(a, pltpu.HBM) for a in operands))
    of, ig, wg, gg, bg = pl.pallas_call(
        put_out,
        out_shape=[out(a.shape, a.dtype) for a in made],
        in_specs=[anywhere] * 5,
        out_specs=[stays] * 5,
        scratch_shapes=[dma((5,))],
        compiler_params=pltpu.CompilerParams(vmem_limit_bytes=1 << 20),
        name="put_out",
    )(*made)
    return of, ig, wg, gg.reshape(chans), bg.reshape(chans)


def program(devices):
    torus = Mesh(devices, ("z", "c", "y", "x"))
    placed = (P(TM, ROWS, None, None), P(), P(), P(), P(TM, ROWS, None, None))
    return jax.shard_map(
        functools.partial(per_device, devices.shape),
        mesh=torus,
        in_specs=placed,
        out_specs=(P(TM, ROWS, None, None), P(TM, ROWS, None, None), P(ROWS, None), P(), P()),
        check_vma=False,
    )


def solution(mesh):
    return program(mesh.devices.reshape(8, 2, 4, 4))
```
